8 devices in a mesh: dp: 2 (over y, z), tp: 4 (over x, core).
Axes of the slice: x: 2, y: 2, z: 1, core: 2. Of those that a mesh axis runs over, the one named last changes fastest.
Arguments:
- x: bfloat16 [2048, 6144], P(('dp', 'tp')), parts along dimension 0
- dy: bfloat16 [2048, 6144], P(('dp', 'tp')), parts along dimension 0
- gain: bfloat16 [6144], replicated
- wq: bfloat16 [6144, 6144], P(None, 'tp')
- wk: bfloat16 [6144, 512], P(None, 'tp')
- wv: bfloat16 [6144, 512], P(None, 'tp')
- wo: bfloat16 [6144, 6144], P('tp')
Outputs:
- output 1: bfloat16 [2048, 6144], P(('dp', 'tp')), parts along dimension 0
- output 2: float32 [2, 6144], P('dp'), parts along dimension 0
- output 3: bfloat16 [12288, 6144], P('dp', 'tp'), parts along dimension 0
- output 4: bfloat16 [12288, 512], P('dp', 'tp'), parts along dimension 0
- output 5: bfloat16 [12288, 512], P('dp', 'tp'), parts along dimension 0
- output 6: bfloat16 [12288, 6144], P(('dp', 'tp')), parts along dimension 0
There are 2 independent parts. The reference program is written for one: setup_inputs(seed, part) draws one part's arguments, and reference() takes and returns one part's arrays. A program takes and returns all parts, laid end to end along the dimension named above; an argument that names none is the same for every part.
All inputs are finite; a program needn't handle non-finite values.
Results may differ from the reference program's by a relative error of at most 0.018.
Values are sent between devices in bfloat16 or wider.
A program may use at most 2 GiB of HBM per device.

```python
import jax
import jax.numpy as jnp
from jax import lax

ROWS = 1024
D = 6144
HEADS = 48
KV_HEADS = 4
HEAD = 128
THETA = 10000


def setup_inputs(seed: int = 0, part: int = 0) -> dict:
    kx, ky, kn, kq, kk, kv, ko = jax.random.split(jax.random.key(seed), 7)

    def weights(key, rows, columns):
        return jax.random.normal(key, (rows, columns), jnp.float32) * rows**-0.5

    drawn = {
        "x": jax.random.normal(jax.random.fold_in(kx, part), (ROWS, D), jnp.float32),
        "dy": jax.random.normal(jax.random.fold_in(ky, part), (ROWS, D), jnp.float32) * ROWS**-0.5,
        "gain": 1 + 0.1 * jax.random.normal(kn, (D,), jnp.float32),
        "wq": 2 * weights(kq, D, HEADS * HEAD),
        "wk": 2 * weights(kk, D, KV_HEADS * HEAD),
        "wv": 4 * weights(kv, D, KV_HEADS * HEAD),
        "wo": weights(ko, HEADS * HEAD, D),
    }
    return {k: v.astype(jnp.bfloat16) for k, v in drawn.items()}


def normed(x, gain):
    wide = x.astype(jnp.float32)
    scale = lax.rsqrt(jnp.mean(wide * wide, -1, keepdims=True) + 1e-6)
    return (wide * scale * gain.astype(jnp.float32)).astype(jnp.bfloat16)


def turned(t, place, theta):
    half = t.shape[-1] // 2
    angle = place.astype(jnp.float32)[:, None] * theta ** (-jnp.arange(half, dtype=jnp.float32) / half)
    cos, sin = jnp.cos(angle)[:, None], jnp.sin(angle)[:, None]
    a, b = t[..., :half].astype(jnp.float32), t[..., half:].astype(jnp.float32)
    return jnp.concatenate([a * cos - b * sin, b * cos + a * sin], -1).astype(jnp.bfloat16)


def matmul(a, w):
    return jnp.dot(a, w, preferred_element_type=jnp.float32).astype(jnp.bfloat16)


def einsum(form, a, b):
    return jnp.einsum(form, a.astype(jnp.float32), b.astype(jnp.float32))


def attention(q, k, v):
    scores = einsum("tgsd,ugd->gstu", q, k) * q.shape[-1] ** -0.5
    token = jnp.arange(q.shape[0])
    scores = jnp.where(token[:, None] >= token, scores, -jnp.inf)
    weights = jax.nn.softmax(scores, -1).astype(jnp.bfloat16)
    return einsum("gstu,ugd->tgsd", weights, v).astype(jnp.bfloat16)


def forward(x, gain, wq, wk, wv, wo):
    rows = x.shape[0]
    a, place = normed(x, gain), jnp.arange(rows)
    k = turned(matmul(a, wk).reshape(rows, -1, HEAD), place, THETA)
    q = turned(matmul(a, wq).reshape(rows, -1, HEAD), place, THETA).reshape(rows, k.shape[1], -1, HEAD)
    v = matmul(a, wv).reshape(rows, -1, HEAD)
    seen = attention(q, k, v).reshape(rows, -1)
    return (x.astype(jnp.float32) + jnp.dot(seen, wo, preferred_element_type=jnp.float32)).astype(jnp.bfloat16)


def reference(x, dy, gain, wq, wk, wv, wo):
    _, back = jax.vjp(forward, x, gain.astype(jnp.float32), wq, wk, wv, wo)
    by_x, by_gain, *by_weights = back(dy)
    return (by_x, by_gain[None], *by_weights)
```

```python
import functools

import jax
import jax.numpy as jnp
from jax import lax
from jax.experimental import pallas as pl
from jax.experimental.pallas import tpu as pltpu
from jax.sharding import PartitionSpec as P


HEAD = 128
THETA = 10000
HIDDEN = -2e30
LOG2E = 1.4426950408889634
VMEM = 56 * 2**20
HALF = 128
BLOCK = 256
F32, BF16 = jnp.float32, jnp.bfloat16
ANY = pl.BlockSpec(memory_space=pl.ANY)


def _dot(a, b, ca, cb):
    return lax.dot_general(a, b, (((ca,), (cb,)), ((), ())), preferred_element_type=F32)


def _call(kernel, name, grid, in_specs, out_specs, out_shape, scratch, flops, moved, args, scalars=1):
    return pl.pallas_call(
        kernel,
        name=name,
        grid_spec=pltpu.PrefetchScalarGridSpec(
            num_scalar_prefetch=scalars, grid=grid, in_specs=in_specs, out_specs=out_specs, scratch_shapes=scratch),
        out_shape=out_shape,
        compiler_params=pltpu.CompilerParams(dimension_semantics=("arbitrary",) * len(grid), vmem_limit_bytes=VMEM),
        cost_estimate=pl.CostEstimate(flops=int(flops), bytes_accessed=int(moved), transcendentals=0),
    )(*args)


def _fetch(pairs, sem):
    copies = [pltpu.make_async_copy(src, dst, sem.at[n]) for n, (src, dst) in enumerate(pairs)]
    for copy in copies:
        copy.start()
    for copy in copies:
        copy.wait()


def _sds(shape, dtype=BF16):
    return jax.ShapeDtypeStruct(shape, dtype)


def _table(ref, pos_ref, first, n):
    return jnp.concatenate([ref[pl.ds(pl.multiple_of(pos_ref[first + m], HALF), HALF), :] for m in range(n)], axis=0)


def _norm(x_ref, gain_ref, a0_ref, a1_ref):
    i = pl.program_id(0)
    x = x_ref[...].astype(F32)
    scale = lax.rsqrt(jnp.mean(x * x, -1, keepdims=True) + 1e-6)
    a = (x * scale * gain_ref[...].astype(F32)).astype(BF16)
    half = pl.num_programs(0) // 2

    @pl.when(i < half)
    def _():
        a0_ref[...] = a

    @pl.when(i >= half)
    def _():
        a1_ref[...] = a


def norm(x, gain):
    rows, d = x.shape
    return pl.pallas_call(
        _norm,
        name="norm",
        grid=(8,),
        in_specs=[pl.BlockSpec((32, d), lambda i: (i, 0)), pl.BlockSpec((1, d), lambda i: (0, 0))],
        out_specs=[pl.BlockSpec((32, d), lambda i: (jnp.minimum(i, 3), 0)), pl.BlockSpec((32, d), lambda i: (jnp.maximum(i - 4, 0), 0))],
        out_shape=[_sds((HALF, d)), _sds((HALF, d))],
        compiler_params=pltpu.CompilerParams(dimension_semantics=("arbitrary",), vmem_limit_bytes=VMEM),
        cost_estimate=pl.CostEstimate(flops=10**9, bytes_accessed=4 * rows * d, transcendentals=0),
    )(x, gain)


def _project(pos_ref, *refs, n, first):
    pieces, (wq_ref, wk_ref, wv_ref, c_ref, s_ref, q_ref, k_ref, v_ref, a_s, w_s, sem) = refs[:n], refs[n:]
    i = pl.program_id(0)
    last = pl.num_programs(0) - 1
    kv = [pltpu.make_async_copy(w, w_s.at[:, pl.ds(m * HEAD, HEAD)], sem.at[n + m]) for m, w in enumerate((wk_ref, wv_ref))]
    rows = a_s.shape[0] // n

    @pl.when(i == 0)
    def _():
        _fetch([(p, a_s.at[pl.ds(m * rows, rows), :]) for m, p in enumerate(pieces)], sem)
        for copy in kv:
            copy.start()

    def turn(t, cos, sin):
        t = t.astype(BF16).astype(F32)
        return (t * cos + pltpu.roll(t, HEAD // 2, 1) * sin).astype(BF16)

    cos, sin = _table(c_ref, pos_ref, first, a_s.shape[0] // HALF), _table(s_ref, pos_ref, first, a_s.shape[0] // HALF)

    @pl.when(i < last)
    def _():
        t = _dot(a_s[...], wq_ref[...], 1, 0)
        for m in range(t.shape[1] // HEAD):
            q_ref[:, m * HEAD : (m + 1) * HEAD] = turn(t[:, m * HEAD : (m + 1) * HEAD], cos, sin)

    @pl.when(i == last)
    def _():
        for copy in kv:
            copy.wait()
        t = _dot(a_s[...], w_s[...], 1, 0)
        k_ref[...] = turn(t[:, :HEAD], cos, sin)
        v_ref[...] = t[:, HEAD:].astype(BF16)


def project(pos, first, pieces, wq, wk, wv, cos, sin):
    d, width = wq.shape
    n, rows = len(pieces), sum(p.shape[0] for p in pieces)
    wide = 256
    steps = width // wide
    whole = lambda i, _: (0, 0)
    tile = lambda i, _: (0, jnp.minimum(i, steps - 1))
    return _call(
        functools.partial(_project, n=n, first=first), "project", (steps + 1,),
        [ANY] * n + [pl.BlockSpec((d, wide), tile), ANY, ANY, pl.BlockSpec(cos.shape, whole), pl.BlockSpec(sin.shape, whole)],
        [pl.BlockSpec((rows, wide), tile), pl.BlockSpec((rows, HEAD), whole), pl.BlockSpec((rows, HEAD), whole)],
        [_sds((rows, width)), _sds((rows, HEAD)), _sds((rows, HEAD))],
        [pltpu.VMEM((rows, d), BF16), pltpu.VMEM((d, 2 * HEAD), BF16), pltpu.SemaphoreType.DMA((n + 2,))],
        2 * rows * d * (width + 2 * HEAD), 2 * (d * (width + 256) + rows * (d + width)), (pos, *pieces, wq, wk, wv, cos, sin))


def _into(_, *refs, n):
    pieces, (w_ref, o_ref, a_s, sem) = refs[:n], refs[n:]
    rows = a_s.shape[0] // n

    @pl.when(pl.program_id(0) == 0)
    def _():
        _fetch([(p, a_s.at[pl.ds(m * rows, rows), :]) for m, p in enumerate(pieces)], sem)

    o_ref[...] = _dot(a_s[...], w_ref[...], 1, 1).astype(BF16)


def into(pos, pieces, wo):
    width, d = wo.shape
    n, rows = len(pieces), sum(p.shape[0] for p in pieces)
    wide = 256
    return _call(
        functools.partial(_into, n=n), "into", (width // wide,),
        [ANY] * n + [pl.BlockSpec((wide, d), lambda i, _: (i, 0))],
        pl.BlockSpec((rows, wide), lambda i, _: (0, i)), _sds((rows, width)),
        [pltpu.VMEM((rows, d), BF16), pltpu.SemaphoreType.DMA((n,))],
        2 * rows * d * width, 2 * (d * width + rows * (d + width)), (pos, *pieces, wo))


def _attend(pos_ref, q_ref, do_ref, kl_ref, kh_ref, kr_ref, vl_ref, vh_ref, vr_ref, c_ref, s_ref, *rest, first, hp, added):
    dk_in, dv_in = rest[:2] if added else (None, None)
    seen_ref, dq_ref, dk_ref, dv_ref, k_s, v_s, kt_s, vt_s, s_s, dp_s, o_s, dq_s, dk_s, dv_s = rest[-14:]
    iq, ih = pl.program_id(0), pl.program_id(1)
    wide = hp * BLOCK
    e = HEAD**-0.5 * LOG2E

    @pl.when((iq == 0) & (ih == 0))
    def _():
        at = 0
        for kc, vc in ((kl_ref, vl_ref), (kh_ref, vh_ref), (kr_ref, vr_ref)):
            for m in range(kc.shape[0] // HALF):
                here = pl.ds(pl.multiple_of(pos_ref[at], HALF), HALF)
                k_s[here, :] = kc[m * HALF : (m + 1) * HALF, :]
                v_s[here, :] = vc[m * HALF : (m + 1) * HALF, :]
                at += 1
        kt_s[...] = k_s[...].T
        vt_s[...] = v_s[...].T
        dk_s[...] = dk_in[...] if added else jnp.zeros_like(dk_s)
        dv_s[...] = dv_in[...] if added else jnp.zeros_like(dv_s)

    place = pos_ref[first + 2 * iq]
    own = lax.div(place, BLOCK)
    turned = lax.rem(place, BLOCK)
    q2 = jnp.concatenate([q_ref[:, m * HEAD : (m + 1) * HEAD] for m in range(hp)], axis=0)
    do2 = jnp.concatenate([do_ref[:, m * HEAD : (m + 1) * HEAD] for m in range(hp)], axis=0)

    def rows(j):
        return pl.ds(pl.multiple_of(j * BLOCK, BLOCK), BLOCK)

    here = rows(own)
    s = _dot(k_s[here, :], q2, 1, 1)
    query = lax.rem(lax.broadcasted_iota(jnp.int32, s.shape, 1) + turned, BLOCK)
    s = jnp.where(lax.broadcasted_iota(jnp.int32, s.shape, 0) <= query, s, HIDDEN)
    s_s[here, :] = s

    def scores(j, top):
        s = _dot(k_s[rows(j), :], q2, 1, 1)
        s_s[rows(j), :] = s
        return jnp.maximum(top, s.max(axis=0, keepdims=True))

    top = lax.fori_loop(0, own, scores, s.max(axis=0, keepdims=True))
    o_s[...] = jnp.zeros_like(o_s)
    dq_s[...] = jnp.zeros_like(dq_s)

    def weigh(j, sums):
        total, delta = sums
        dp = _dot(v_s[rows(j), :], do2, 1, 1)
        dp_s[rows(j), :] = dp
        p = jnp.exp2((s_s[rows(j), :] - top) * e)
        s_s[rows(j), :] = p
        o_s[...] += _dot(vt_s[:, rows(j)], p.astype(BF16), 1, 0)
        return total + p.sum(axis=0, keepdims=True), delta + (p * dp).sum(axis=0, keepdims=True)

    zero = jnp.zeros((1, wide), F32)
    total, delta = lax.fori_loop(0, own + 1, weigh, (zero, zero))
    inv = 1 / total
    delta = delta * inv

    def grads(j, _):
        p = s_s[rows(j), :] * inv
        ds = (p * (dp_s[rows(j), :] - delta)).astype(BF16)
        dv_s[rows(j), :] += _dot(p.astype(BF16), do2, 1, 0)
        dk_s[rows(j), :] += _dot(ds, q2, 1, 0)
        dq_s[...] += _dot(kt_s[:, rows(j)], ds, 1, 0)

    lax.fori_loop(0, own + 1, grads, None)
    cos, sin = _table(c_ref, pos_ref, first + 2 * iq, 2), _table(s_ref, pos_ref, first + 2 * iq, 2)
    o = (o_s[...] * inv).astype(BF16)
    for m in range(hp):
        seen_ref[m * HEAD : (m + 1) * HEAD, :] = o[:, m * BLOCK : (m + 1) * BLOCK]
        g = (dq_s[:, m * BLOCK : (m + 1) * BLOCK] * HEAD**-0.5).T.astype(BF16).astype(F32)
        dq_ref[:, m * HEAD : (m + 1) * HEAD] = (g * cos - pltpu.roll(g, HEAD // 2, 1) * sin).astype(BF16)

    @pl.when((iq == pl.num_programs(0) - 1) & (ih == pl.num_programs(1) - 1))
    def _():
        dk_ref[...] = dk_s[...]
        dv_ref[...] = dv_s[...]


def attend(pos, first, q, do, ks, vs, cos, sin, sums=None):
    rows, width = q.shape
    hp = 4
    sk = sum(k.shape[0] for k in ks)
    tile = pl.BlockSpec((BLOCK, hp * HEAD), lambda i, h, _: (i, h))
    whole = lambda a: pl.BlockSpec(a.shape, lambda i, h, _: (0, 0))
    keys = _sds((sk, HEAD), F32)
    given = (*ks, *vs, cos, sin, *(sums or ()))
    wide = hp * BLOCK
    vmem = lambda *shape, t=F32: pltpu.VMEM(shape, t)
    return _call(
        functools.partial(_attend, first=first, hp=hp, added=sums is not None), "attend", (rows // BLOCK, width // (hp * HEAD)),
        [tile, tile, *map(whole, given)],
        [pl.BlockSpec((hp * HEAD, BLOCK), lambda i, h, _: (h, i)), tile, whole(keys), whole(keys)],
        [_sds((width, rows)), _sds((rows, width)), keys, keys],
        [vmem(sk, HEAD, t=BF16), vmem(sk, HEAD, t=BF16), vmem(HEAD, sk, t=BF16), vmem(HEAD, sk, t=BF16), vmem(sk, wide), vmem(sk, wide),
         vmem(HEAD, wide), vmem(HEAD, wide), vmem(sk, HEAD), vmem(sk, HEAD)],
        2 * 6 * 2 * rows * sk * width * 0.6, 8 * rows * width, (pos, q, do, *given))


def _back(pos_ref, dq_ref, dk_ref, dv_ref, c_ref, s_ref, wq_ref, wk_ref, wv_ref, keep_ref, send_ref, g_ref, *, first):
    width = dq_ref.shape[1]
    half = keep_ref.shape[0]

    @pl.when(pl.program_id(0) == 0)
    def _():
        n = dq_ref.shape[0] // HALF
        cos, sin = _table(c_ref, pos_ref, first, n), _table(s_ref, pos_ref, first, n)
        g = (_table(dk_ref, pos_ref, first, n) * HEAD**-0.5).astype(BF16).astype(F32)
        g_ref[:, :width] = dq_ref[...]
        g_ref[:, width : width + HEAD] = (g * cos - pltpu.roll(g, HEAD // 2, 1) * sin).astype(BF16)
        g_ref[:, width + HEAD :] = _table(dv_ref, pos_ref, first, n).astype(BF16)

    w = jnp.concatenate([wq_ref[...], wk_ref[...], wv_ref[...]], axis=1)
    t = _dot(g_ref[...], w, 1, 1)
    keep_ref[...] = t[:half]
    send_ref[...] = t[half:].astype(BF16)


def back(pos, first, dq, dk, dv, wq, wk, wv, cos, sin):
    d, width = wq.shape
    rows = dq.shape[0]
    wide = 512
    whole = lambda a: pl.BlockSpec(a.shape, lambda i, _: (0, 0))
    g = _sds((rows, width + 2 * HEAD))
    tile = lambda n: pl.BlockSpec((wide, n), lambda i, _: (i, 0))
    out = pl.BlockSpec((rows // 2, wide), lambda i, _: (0, i))
    return _call(
        functools.partial(_back, first=first), "back", (d // wide,),
        [*map(whole, (dq, dk, dv, cos, sin)), tile(width), tile(HEAD), tile(HEAD)],
        [out, out, whole(g)], [_sds((rows // 2, d), F32), _sds((rows // 2, d)), g], [],
        2 * rows * d * (width + 2 * HEAD), 2 * (d * (width + 256) + rows * (2 * d + width)), (pos, dq, dk, dv, cos, sin, wq, wk, wv))


def _weights(_, *refs, n, ng):
    pieces, gs, (wq_ref, wk_ref, wv_ref, g_s, sem) = refs[:n], refs[n : n + ng], refs[n + ng :]

    @pl.when(pl.program_id(0) == 0)
    def _():
        at, pairs = 0, []
        for g in gs:
            pairs.append((g, g_s.at[pl.ds(at, g.shape[0]), :]))
            at += g.shape[0]
        _fetch(pairs, sem)

    a = jnp.concatenate([p[...] for p in pieces], axis=0)
    t = _dot(a, g_s[...], 0, 0).astype(BF16)
    width = wq_ref.shape[1]
    wq_ref[...] = t[:, :width]
    wk_ref[...] = t[:, width : width + HEAD]
    wv_ref[...] = t[:, width + HEAD :]


def weights(pos, pieces, gs):
    d = pieces[0].shape[1]
    full = gs[0].shape[1]
    width = full - 2 * HEAD
    rows = sum(g.shape[0] for g in gs)
    wide = 512
    tile = lambda n: pl.BlockSpec((wide, n), lambda i, _: (i, 0))
    return _call(
        functools.partial(_weights, n=len(pieces), ng=len(gs)), "weights", (d // wide,),
        [pl.BlockSpec((p.shape[0], wide), lambda i, _: (0, i)) for p in pieces] + [ANY] * len(gs),
        [tile(width), tile(HEAD), tile(HEAD)], [_sds((d, width)), _sds((d, HEAD)), _sds((d, HEAD))],
        [pltpu.VMEM((rows, full), BF16), pltpu.SemaphoreType.DMA((len(gs),))],
        2 * rows * d * full, 2 * (rows * (d + full) + d * full), (pos, *pieces, *gs))


def _out_weights(_, *refs, n, ns):
    pieces, seen, (o_ref, s_s, sem) = refs[:n], refs[n : n + ns], refs[n + ns :]

    @pl.when(pl.program_id(0) == 0)
    def _():
        at, pairs = 0, []
        for s in seen:
            pairs.append((s, s_s.at[:, pl.ds(at, s.shape[1])]))
            at += s.shape[1]
        _fetch(pairs, sem)

    o_ref[...] = _dot(s_s[...], jnp.concatenate([p[...] for p in pieces], axis=0), 1, 0).astype(BF16)


def out_weights(pos, pieces, seen):
    d = pieces[0].shape[1]
    width = seen[0].shape[0]
    rows = sum(s.shape[1] for s in seen)
    wide = 512
    return _call(
        functools.partial(_out_weights, n=len(pieces), ns=len(seen)), "out_weights", (d // wide,),
        [pl.BlockSpec((p.shape[0], wide), lambda i, _: (0, i)) for p in pieces] + [ANY] * len(seen),
        pl.BlockSpec((width, wide), lambda i, _: (0, i)), _sds((width, d)),
        [pltpu.VMEM((width, rows), BF16), pltpu.SemaphoreType.DMA((len(seen),))],
        2 * rows * d * width, 2 * (rows * (d + width) + d * width), (pos, *pieces, *seen))


def _finish(own_ref, sib_ref, r0_ref, r1_ref, x_ref, dy_ref, gain_ref, dx_ref, dg_ref):
    i = pl.program_id(0)
    far = jnp.where(i < pl.num_programs(0) // 2, r0_ref[...].astype(F32), r1_ref[...].astype(F32))
    da = own_ref[...] + sib_ref[...].astype(F32) + far
    x = x_ref[...].astype(F32)
    scale = lax.rsqrt(jnp.mean(x * x, -1, keepdims=True) + 1e-6)
    h = x * scale
    dh = da * gain_ref[...].astype(F32)
    part = jnp.sum(da * h, axis=0, keepdims=True)
    dx = scale * (dh - h * jnp.mean(dh * h, -1, keepdims=True))
    dx_ref[...] = (dy_ref[...].astype(F32) + dx).astype(BF16)

    @pl.when(i == 0)
    def _():
        dg_ref[...] = part

    @pl.when(i > 0)
    def _():
        dg_ref[...] += part


def finish(own, sib, r0, r1, x, dy, gain):
    rows, d = x.shape
    n = 64
    tile = pl.BlockSpec((n, d), lambda i: (i, 0))
    half = rows // n // 2
    line = pl.BlockSpec((1, d), lambda i: (0, 0))
    return pl.pallas_call(
        _finish,
        name="finish",
        grid=(rows // n,),
        in_specs=[tile, tile, pl.BlockSpec((n, d), lambda i: (jnp.minimum(i, half - 1), 0)),
                  pl.BlockSpec((n, d), lambda i: (jnp.maximum(i - half, 0), 0)), tile, tile, line],
        out_specs=[tile, line],
        out_shape=[_sds((rows, d)), _sds((1, d), F32)],
        compiler_params=pltpu.CompilerParams(dimension_semantics=("arbitrary",), vmem_limit_bytes=VMEM),
        cost_estimate=pl.CostEstimate(flops=3 * 10**9, bytes_accessed=14 * rows * d, transcendentals=0),
    )(own, sib, r0, r1, x, dy, gain)


def tables(rows):
    half = HEAD // 2
    angle = jnp.arange(rows).astype(F32)[:, None] * THETA ** (-jnp.arange(half, dtype=F32) / half)
    cos, sin = jnp.cos(angle), jnp.sin(angle)
    return jnp.concatenate([cos, cos], -1), jnp.concatenate([-sin, sin], -1)


SIBLING = [(0, 1), (1, 0), (2, 3), (3, 2)]
PARTNER = [(0, 2), (2, 0), (1, 3), (3, 1)]
ACROSS = [(0, 3), (3, 0), (1, 2), (2, 1)]


def solution(mesh):
    def move(t, pairs):
        return lax.ppermute(t, "tp", pairs)

    def step(x, dy, gain, wq, wk, wv, wo):
        me = lax.axis_index("tp")
        core = lax.rem(me, 2)
        upper = core == 1
        gain = gain[None]
        start = lambda block, half: block * BLOCK + half * HALF
        sib, far = me + 1 - 2 * core, 2 * (1 - lax.div(me, 2))
        pos = jnp.stack([start(me, 0), start(me, 1), start(sib, 0), start(sib, 1), start(far + 1, core), start(far + 1, 1 - core),
                         start(far, core), start(far, 1 - core)]).astype(jnp.int32)
        cos, sin = tables(4 * BLOCK)

        def spread(own0, own1):
            sib0, sib1 = move(own0, SIBLING), move(own1, SIBLING)
            return sib0, sib1, jnp.where(upper, own1, sib0), jnp.where(upper, sib1, own0)

        a0, a1 = norm(x, gain)
        d0, d1 = dy[:HALF], dy[HALF:]
        b0, b1, a_high, a_low = spread(a0, a1)
        e0, e1, d_high, d_low = spread(d0, d1)
        ah = move(a_high, PARTNER)
        al = move(a_low, PARTNER)
        d_high, d_low, _ = lax.optimization_barrier((d_high, d_low, a_low))
        dh = move(d_high, PARTNER)
        dl = move(d_low, PARTNER)
        ah2, al2 = move(ah, SIBLING), move(al, SIBLING)
        dh2, dl2 = move(dh, SIBLING), move(dl, SIBLING)

        w = (wq, wk, wv)
        q_n, k_n, v_n = project(pos, 0, (a0, a1, b0, b1), *w, cos, sin)
        do_n = into(pos, (d0, d1, e0, e1), wo)
        q_h, k_h, v_h = project(pos, 4, (ah, ah2), *w, cos, sin)
        q_l, k_l, v_l = project(pos, 6, (al, al2), *w, cos, sin)
        keys = ((k_n, k_h, k_l), (v_n, v_h, v_l), cos, sin)
        seen_n, dq_n, dk, dv = attend(pos, 0, q_n, do_n, *keys)
        do_h = into(pos, (dh, dh2), wo)
        seen_h, dq_h, dk, dv = attend(pos, 4, q_h, do_h, *keys, sums=(dk, dv))
        keep_h, send_h, g_h = back(pos, 4, dq_h, dk, dv, *w, cos, sin)
        do_l = into(pos, (dl, dl2), wo)
        seen_l, dq_l, dk, dv = attend(pos, 6, q_l, do_l, *keys, sums=(dk, dv))
        keep_l, send_l, g_l = back(pos, 6, dq_l, dk, dv, *w, cos, sin)
        keep_n, send_n, g_n = back(pos, 0, dq_n, dk, dv, *w, cos, sin)

        add = lambda keep, came: (keep + came.astype(F32)).astype(BF16)
        r_h = move(add(keep_h, move(send_h, SIBLING)), PARTNER)
        r_l = move(add(keep_l, move(send_l, SIBLING)), PARTNER)
        s_n = move(send_n, SIBLING)
        mine = jnp.where(upper, r_h, r_l)
        other = move(jnp.where(upper, r_l, r_h), SIBLING)
        by_wo = out_weights(pos, (d0, d1, e0, e1, dh, dh2, dl, dl2), (seen_n, seen_h, seen_l))
        by_wq, by_wk, by_wv = weights(pos, (a0, a1, b0, b1, ah, ah2, al, al2), (g_n, g_h, g_l))
        by_x, part = finish(keep_n, s_n, jnp.where(upper, other, mine), jnp.where(upper, mine, other), x, dy, gain)
        by_gain = (part + move(part, SIBLING)) + (move(part, PARTNER) + move(part, ACROSS))
        return by_x, by_gain, by_wq, by_wk, by_wv, by_wo

    tokens, columns = P(("dp", "tp"), None), P(None, "tp")
    return jax.shard_map(
        step,
        mesh=mesh,
        in_specs=(tokens, tokens, P(None), columns, columns, columns, P("tp", None)),
        out_specs=(tokens, P("dp", None), P("dp", "tp"), P("dp", "tp"), P("dp", "tp"), P(("dp", "tp"), None)),
        check_vma=False,
    )
```

```python
import functools

import jax
import jax.numpy as jnp
from jax import lax
from jax.experimental import pallas as pl
from jax.experimental.pallas import tpu as pltpu
from jax.sharding import PartitionSpec as P


HEAD = 128
THETA = 10000
HIDDEN = -2e30
LOG2E = 1.4426950408889634
VMEM = 56 * 2**20
HALF = 128
BLOCK = 256
F32, BF16 = jnp.float32, jnp.bfloat16
ANY = pl.BlockSpec(memory_space=pl.ANY)


def _dot(a, b, ca, cb):
    return lax.dot_general(a, b, (((ca,), (cb,)), ((), ())), preferred_element_type=F32)


def _call(kernel, grid, in_specs, out_specs, out_shape, scratch, flops, moved, args, scalars=1):
    return pl.pallas_call(
        kernel,
        grid_spec=pltpu.PrefetchScalarGridSpec(
            num_scalar_prefetch=scalars, grid=grid, in_specs=in_specs, out_specs=out_specs, scratch_shapes=scratch),
        out_shape=out_shape,
        compiler_params=pltpu.CompilerParams(dimension_semantics=("arbitrary",) * len(grid), vmem_limit_bytes=VMEM),
        cost_estimate=pl.CostEstimate(flops=int(flops), bytes_accessed=int(moved), transcendentals=0),
    )(*args)


def _fetch(pairs, sem):
    copies = [pltpu.make_async_copy(src, dst, sem.at[n]) for n, (src, dst) in enumerate(pairs)]
    for copy in copies:
        copy.start()
    for copy in copies:
        copy.wait()


def _sds(shape, dtype=BF16):
    return jax.ShapeDtypeStruct(shape, dtype)


def _table(ref, pos_ref, first, n):
    return jnp.concatenate([ref[pl.ds(pl.multiple_of(pos_ref[first + m], HALF), HALF), :] for m in range(n)], axis=0)


def _copies(pairs, sem, base=0):
    return [pltpu.make_async_copy(src, dst, sem.at[base + n]) for n, (src, dst) in enumerate(pairs)]


def _norm(x_ref, gain_ref, a_ref, x_s, a_s, sem, out_sem):
    n = x_s.shape[0]
    rows = x_s.shape[1]
    part = lambda ref, i: ref.at[pl.ds(pl.multiple_of(i * rows, rows), rows), :]
    for copy in _copies([(part(x_ref, i), x_s.at[i]) for i in range(n)], sem):
        copy.start()

    def step(i, _):
        pltpu.make_async_copy(part(x_ref, i), x_s.at[i], sem.at[i]).wait()
        x = x_s[i].astype(F32)
        scale = lax.rsqrt(jnp.mean(x * x, -1, keepdims=True) + 1e-6)
        a_s[i] = (x * scale * gain_ref[...].astype(F32)).astype(BF16)
        pltpu.make_async_copy(a_s.at[i], part(a_ref, i), out_sem.at[i]).start()

    lax.fori_loop(0, n, step, None)
    for copy in _copies([(a_s.at[i], part(a_ref, i)) for i in range(n)], out_sem):
        copy.wait()


def norm(x, gain):
    rows, d = x.shape
    n = 8
    return pl.pallas_call(
        _norm,
        name="norm",
        in_specs=[ANY, pl.BlockSpec(memory_space=pltpu.VMEM)],
        out_specs=ANY,
        out_shape=_sds((rows, d)),
        scratch_shapes=[pltpu.VMEM((n, rows // n, d), BF16)] * 2 + [pltpu.SemaphoreType.DMA((n,))] * 2,
        compiler_params=pltpu.CompilerParams(vmem_limit_bytes=VMEM),
        cost_estimate=pl.CostEstimate(flops=10**9, bytes_accessed=4 * rows * d, transcendentals=0),
    )(x, gain)


def _all(kernel, n_in, out_shape, scratch, flops, moved, pos, *args):
    many = isinstance(out_shape, list)
    return pl.pallas_call(
        kernel,
        in_specs=[pl.BlockSpec(memory_space=pltpu.SMEM)] + [ANY] * n_in,
        out_specs=[ANY] * len(out_shape) if many else ANY,
        out_shape=out_shape,
        scratch_shapes=scratch,
        compiler_params=pltpu.CompilerParams(vmem_limit_bytes=VMEM),
        cost_estimate=pl.CostEstimate(flops=int(flops), bytes_accessed=int(moved), transcendentals=0),
    )(pos, *args)


def _pieces(pieces, a_s):
    at, pairs = 0, []
    for p in pieces:
        pairs.append((p, a_s.at[pl.ds(at, p.shape[0]), :]))
        at += p.shape[0]
    return pairs


def _places(pos_ref, ref, s, first):
    return [(ref.at[pl.ds(pl.multiple_of(pos_ref[first + m], HALF), HALF), :], s.at[pl.ds(m * HALF, HALF), :]) for m in range(s.shape[0] // HALF)]


def _project(pos_ref, *refs, n, first):
    pieces, (wq_ref, wk_ref, wv_ref, c_ref, s_ref, q_ref, k_ref, v_ref) = refs[:n], refs[n : n + 8]
    a_s, w_s, c_s, s_s, q_s, k_s, v_s, sem, w_sem, out_sem, kv_sem = refs[n + 8 :]
    steps, wide = w_s.shape[0] - 1, w_s.shape[2]
    pairs = _pieces(pieces, a_s) + _places(pos_ref, c_ref, c_s, first) + _places(pos_ref, s_ref, s_s, first)
    ready = _copies(pairs, sem)
    columns = lambda ref, i: ref.at[:, pl.ds(pl.multiple_of(i * wide, wide), wide)]
    tile = lambda i: pltpu.make_async_copy(columns(wq_ref, i), w_s.at[i], w_sem.at[i])
    kv = [pltpu.make_async_copy(w, w_s.at[steps, :, pl.ds(m * HEAD, HEAD)], kv_sem.at[m]) for m, w in enumerate((wk_ref, wv_ref))]
    for copy in ready + [tile(i) for i in range(steps)] + kv:
        copy.start()
    for copy in ready:
        copy.wait()

    def turn(t):
        t = t.astype(BF16).astype(F32)
        return (t * c_s[...] + pltpu.roll(t, HEAD // 2, 1) * s_s[...]).astype(BF16)

    out = lambda i, slot: pltpu.make_async_copy(q_s.at[slot], columns(q_ref, i), out_sem.at[slot])

    def step(i, _):
        slot = lax.rem(i, 2)
        tile(i).wait()
        t = _dot(a_s[...], w_s[i], 1, 0)

        @pl.when(i >= 2)
        def _():
            out(i - 2, slot).wait()

        for m in range(wide // HEAD):
            q_s[slot, :, m * HEAD : (m + 1) * HEAD] = turn(t[:, m * HEAD : (m + 1) * HEAD])
        out(i, slot).start()

    lax.fori_loop(0, steps, step, None)
    for copy in kv:
        copy.wait()
    t = _dot(a_s[...], w_s[steps], 1, 0)
    k_s[...] = turn(t[:, :HEAD])
    v_s[...] = t[:, HEAD:].astype(BF16)
    last = _copies([(k_s, k_ref), (v_s, v_ref)], kv_sem)
    for copy in last:
        copy.start()
    for copy in last + [out(steps - 2 + m, (steps + m) % 2) for m in range(2)]:
        copy.wait()


def project(pos, first, pieces, wq, wk, wv, cos, sin):
    d, width = wq.shape
    n, rows = len(pieces), sum(p.shape[0] for p in pieces)
    wide = 256
    steps = width // wide
    vmem, dma = pltpu.VMEM, pltpu.SemaphoreType.DMA
    return _all(
        functools.partial(_project, n=n, first=first), n + 5,
        [_sds((rows, width)), _sds((rows, HEAD)), _sds((rows, HEAD))],
        [vmem((rows, d), BF16), vmem((steps + 1, d, wide), BF16), vmem((rows, HEAD), F32), vmem((rows, HEAD), F32), vmem((2, rows, wide), BF16),
         vmem((rows, HEAD), BF16), vmem((rows, HEAD), BF16), dma((n + 2 * rows // HALF,)), dma((steps,)), dma((2,)), dma((2,))],
        2 * rows * d * (width + 2 * HEAD), 2 * (d * (width + 256) + rows * (d + width)), pos, *pieces, wq, wk, wv, cos, sin)


def _into(_, *refs, n):
    pieces, (w_ref, o_ref, a_s, w_s, o_s, sem, w_sem, out_sem) = refs[:n], refs[n:]
    steps, wide = w_s.shape[:2]
    ready = _copies(_pieces(pieces, a_s), sem)
    tile = lambda i: pltpu.make_async_copy(w_ref.at[pl.ds(pl.multiple_of(i * wide, wide), wide), :], w_s.at[i], w_sem.at[i])
    for copy in ready + [tile(i) for i in range(steps)]:
        copy.start()
    for copy in ready:
        copy.wait()
    out = lambda i, slot: pltpu.make_async_copy(o_s.at[slot], o_ref.at[:, pl.ds(pl.multiple_of(i * wide, wide), wide)], out_sem.at[slot])

    def step(i, _):
        slot = lax.rem(i, 2)
        tile(i).wait()
        t = _dot(a_s[...], w_s[i], 1, 1).astype(BF16)

        @pl.when(i >= 2)
        def _():
            out(i - 2, slot).wait()

        o_s[slot] = t
        out(i, slot).start()

    lax.fori_loop(0, steps, step, None)
    for m in range(2):
        out(steps - 2 + m, (steps + m) % 2).wait()


def into(pos, pieces, wo):
    width, d = wo.shape
    n, rows = len(pieces), sum(p.shape[0] for p in pieces)
    wide = 256
    steps = width // wide
    vmem, dma = pltpu.VMEM, pltpu.SemaphoreType.DMA
    return _all(
        functools.partial(_into, n=n), n + 1, _sds((rows, width)),
        [vmem((rows, d), BF16), vmem((steps, wide, d), BF16), vmem((2, rows, wide), BF16), dma((n,)), dma((steps,)), dma((2,))],
        2 * rows * d * width, 2 * (d * width + rows * (d + width)), pos, *pieces, wo)


def _attend(pos_ref, q_ref, do_ref, kl_ref, kh_ref, kr_ref, vl_ref, vh_ref, vr_ref, c_ref, s_ref, *rest, first, hp, added):
    dk_in, dv_in = rest[:2] if added else (None, None)
    seen_ref, dq_ref, dk_ref, dv_ref, k_s, v_s, kt_s, vt_s, s_s, dp_s, o_s, dq_s, dk_s, dv_s = rest[-14:]
    iq, ih = pl.program_id(0), pl.program_id(1)
    wide = hp * BLOCK
    e = HEAD**-0.5 * LOG2E

    @pl.when((iq == 0) & (ih == 0))
    def _():
        at = 0
        for kc, vc in ((kl_ref, vl_ref), (kh_ref, vh_ref), (kr_ref, vr_ref)):
            for m in range(kc.shape[0] // HALF):
                here = pl.ds(pl.multiple_of(pos_ref[at], HALF), HALF)
                k_s[here, :] = kc[m * HALF : (m + 1) * HALF, :]
                v_s[here, :] = vc[m * HALF : (m + 1) * HALF, :]
                at += 1
        kt_s[...] = k_s[...].T
        vt_s[...] = v_s[...].T
        dk_s[...] = dk_in[...] if added else jnp.zeros_like(dk_s)
        dv_s[...] = dv_in[...] if added else jnp.zeros_like(dv_s)

    place = pos_ref[first + 2 * iq]
    own = lax.div(place, BLOCK)
    turned = lax.rem(place, BLOCK)
    q2 = jnp.concatenate([q_ref[:, m * HEAD : (m + 1) * HEAD] for m in range(hp)], axis=0)
    do2 = jnp.concatenate([do_ref[:, m * HEAD : (m + 1) * HEAD] for m in range(hp)], axis=0)

    def rows(j):
        return pl.ds(pl.multiple_of(j * BLOCK, BLOCK), BLOCK)

    here = rows(own)
    s = _dot(k_s[here, :], q2, 1, 1)
    query = lax.rem(lax.broadcasted_iota(jnp.int32, s.shape, 1) + turned, BLOCK)
    s = jnp.where(lax.broadcasted_iota(jnp.int32, s.shape, 0) <= query, s, HIDDEN)
    s_s[here, :] = s

    def scores(j, top):
        s = _dot(k_s[rows(j), :], q2, 1, 1)
        s_s[rows(j), :] = s
        return jnp.maximum(top, s.max(axis=0, keepdims=True))

    top = lax.fori_loop(0, own, scores, s.max(axis=0, keepdims=True))
    o_s[...] = jnp.zeros_like(o_s)
    dq_s[...] = jnp.zeros_like(dq_s)

    def weigh(j, sums):
        total, delta = sums
        dp = _dot(v_s[rows(j), :], do2, 1, 1)
        dp_s[rows(j), :] = dp
        p = jnp.exp2((s_s[rows(j), :] - top) * e)
        s_s[rows(j), :] = p
        o_s[...] += _dot(vt_s[:, rows(j)], p.astype(BF16), 1, 0)
        return total + p.sum(axis=0, keepdims=True), delta + (p * dp).sum(axis=0, keepdims=True)

    zero = jnp.zeros((1, wide), F32)
    total, delta = lax.fori_loop(0, own + 1, weigh, (zero, zero))
    inv = 1 / total
    delta = delta * inv

    def grads(j, _):
        p = s_s[rows(j), :] * inv
        ds = (p * (dp_s[rows(j), :] - delta)).astype(BF16)
        dv_s[rows(j), :] += _dot(p.astype(BF16), do2, 1, 0)
        dk_s[rows(j), :] += _dot(ds, q2, 1, 0)
        dq_s[...] += _dot(kt_s[:, rows(j)], ds, 1, 0)

    lax.fori_loop(0, own + 1, grads, None)
    cos, sin = _table(c_ref, pos_ref, first + 2 * iq, 2), _table(s_ref, pos_ref, first + 2 * iq, 2)
    o = (o_s[...] * inv).astype(BF16)
    for m in range(hp):
        seen_ref[m * HEAD : (m + 1) * HEAD, :] = o[:, m * BLOCK : (m + 1) * BLOCK]
        g = (dq_s[:, m * BLOCK : (m + 1) * BLOCK] * HEAD**-0.5).T.astype(BF16).astype(F32)
        dq_ref[:, m * HEAD : (m + 1) * HEAD] = (g * cos - pltpu.roll(g, HEAD // 2, 1) * sin).astype(BF16)

    @pl.when((iq == pl.num_programs(0) - 1) & (ih == pl.num_programs(1) - 1))
    def _():
        dk_ref[...] = dk_s[...]
        dv_ref[...] = dv_s[...]


def attend(pos, first, q, do, ks, vs, cos, sin, sums=None):
    rows, width = q.shape
    hp = 4
    sk = sum(k.shape[0] for k in ks)
    tile = pl.BlockSpec((BLOCK, hp * HEAD), lambda i, h, _: (i, h))
    whole = lambda a: pl.BlockSpec(a.shape, lambda i, h, _: (0, 0))
    keys = _sds((sk, HEAD), F32)
    given = (*ks, *vs, cos, sin, *(sums or ()))
    wide = hp * BLOCK
    vmem = lambda *shape, t=F32: pltpu.VMEM(shape, t)
    return _call(
        functools.partial(_attend, first=first, hp=hp, added=sums is not None), (rows // BLOCK, width // (hp * HEAD)),
        [tile, tile, *map(whole, given)],
        [pl.BlockSpec((hp * HEAD, BLOCK), lambda i, h, _: (h, i)), tile, whole(keys), whole(keys)],
        [_sds((width, rows)), _sds((rows, width)), keys, keys],
        [vmem(sk, HEAD, t=BF16), vmem(sk, HEAD, t=BF16), vmem(HEAD, sk, t=BF16), vmem(HEAD, sk, t=BF16), vmem(sk, wide), vmem(sk, wide),
         vmem(HEAD, wide), vmem(HEAD, wide), vmem(sk, HEAD), vmem(sk, HEAD)],
        2 * 6 * 2 * rows * sk * width * 0.6, 8 * rows * width, (pos, q, do, *given))


def _back(pos_ref, dq_ref, dk_ref, dv_ref, c_ref, s_ref, wq_ref, wk_ref, wv_ref, keep_ref, send_ref, g_ref,
          g_s, dk_s, dv_s, c_s, s_s, w_s, keep_s, send_s, sem, w_sem, out_sem, g_sem, *, first):
    rows, width = dq_ref.shape
    half = rows // 2
    steps, wide = w_s.shape[:2]
    pairs = [(dq_ref, g_s.at[:, pl.ds(0, width)])]
    for ref, s in ((dk_ref, dk_s), (dv_ref, dv_s), (c_ref, c_s), (s_ref, s_s)):
        pairs += _places(pos_ref, ref, s, first)
    ready = _copies(pairs, sem)
    lines = lambda ref, i: ref.at[pl.ds(pl.multiple_of(i * wide, wide), wide), :]
    parts = ((wq_ref, 0, width), (wk_ref, width, HEAD), (wv_ref, width + HEAD, HEAD))
    tile = lambda i: [pltpu.make_async_copy(lines(w, i), w_s.at[i, :, pl.ds(at, size)], w_sem.at[i, m]) for m, (w, at, size) in enumerate(parts)]
    for copy in ready + sum((tile(i) for i in range(steps)), []):
        copy.start()
    for copy in ready:
        copy.wait()
    g = (dk_s[...] * HEAD**-0.5).astype(BF16).astype(F32)
    g_s[:, width : width + HEAD] = (g * c_s[...] - pltpu.roll(g, HEAD // 2, 1) * s_s[...]).astype(BF16)
    g_s[:, width + HEAD :] = dv_s[...].astype(BF16)
    g_out = pltpu.make_async_copy(g_s, g_ref, g_sem.at[0])
    g_out.start()

    def out(i, slot):
        columns = pl.ds(pl.multiple_of(i * wide, wide), wide)
        return _copies([(keep_s.at[slot], keep_ref.at[:, columns]), (send_s.at[slot], send_ref.at[:, columns])], out_sem.at[slot])

    def step(i, _):
        slot = lax.rem(i, 2)
        for copy in tile(i):
            copy.wait()
        t = _dot(g_s[...], w_s[i], 1, 1)

        @pl.when(i >= 2)
        def _():
            for copy in out(i - 2, slot):
                copy.wait()

        keep_s[slot] = t[:half]
        send_s[slot] = t[half:].astype(BF16)
        for copy in out(i, slot):
            copy.start()

    lax.fori_loop(0, steps, step, None)
    for m in range(2):
        for copy in out(steps - 2 + m, (steps + m) % 2):
            copy.wait()
    g_out.wait()


def back(pos, first, dq, dk, dv, wq, wk, wv, cos, sin):
    d, width = wq.shape
    rows = dq.shape[0]
    wide = 512
    steps = d // wide
    full = width + 2 * HEAD
    vmem, dma = pltpu.VMEM, pltpu.SemaphoreType.DMA
    line = vmem((rows, HEAD), F32)
    return _all(
        functools.partial(_back, first=first), 8, [_sds((rows // 2, d), F32), _sds((rows // 2, d)), _sds((rows, full))],
        [vmem((rows, full), BF16), line, line, line, line, vmem((steps, wide, full), BF16), vmem((2, rows // 2, wide), F32),
         vmem((2, rows // 2, wide), BF16), dma((1 + 4 * rows // HALF,)), dma((steps, 3)), dma((2, 2)), dma((1,))],
        2 * rows * d * full, 2 * (d * full + rows * (2 * d + width)), pos, dq, dk, dv, cos, sin, wq, wk, wv)


def _weights(_, *refs, n, ng):
    pieces, gs, (wq_ref, wk_ref, wv_ref, g_s, sem) = refs[:n], refs[n : n + ng], refs[n + ng :]

    @pl.when(pl.program_id(0) == 0)
    def _():
        at, pairs = 0, []
        for g in gs:
            pairs.append((g, g_s.at[pl.ds(at, g.shape[0]), :]))
            at += g.shape[0]
        _fetch(pairs, sem)

    a = jnp.concatenate([p[...] for p in pieces], axis=0)
    t = _dot(a, g_s[...], 0, 0).astype(BF16)
    width = wq_ref.shape[1]
    wq_ref[...] = t[:, :width]
    wk_ref[...] = t[:, width : width + HEAD]
    wv_ref[...] = t[:, width + HEAD :]


def weights(pos, pieces, gs):
    d = pieces[0].shape[1]
    full = gs[0].shape[1]
    width = full - 2 * HEAD
    rows = sum(g.shape[0] for g in gs)
    wide = 512
    tile = lambda n: pl.BlockSpec((wide, n), lambda i, _: (i, 0))
    return _call(
        functools.partial(_weights, n=len(pieces), ng=len(gs)), (d // wide,),
        [pl.BlockSpec((p.shape[0], wide), lambda i, _: (0, i)) for p in pieces] + [ANY] * len(gs),
        [tile(width), tile(HEAD), tile(HEAD)], [_sds((d, width)), _sds((d, HEAD)), _sds((d, HEAD))],
        [pltpu.VMEM((rows, full), BF16), pltpu.SemaphoreType.DMA((len(gs),))],
        2 * rows * d * full, 2 * (rows * (d + full) + d * full), (pos, *pieces, *gs))


def _out_weights(_, *refs, n, ns):
    pieces, seen, (o_ref, s_s, sem) = refs[:n], refs[n : n + ns], refs[n + ns :]

    @pl.when(pl.program_id(0) == 0)
    def _():
        at, pairs = 0, []
        for s in seen:
            pairs.append((s, s_s.at[:, pl.ds(at, s.shape[1])]))
            at += s.shape[1]
        _fetch(pairs, sem)

    o_ref[...] = _dot(s_s[...], jnp.concatenate([p[...] for p in pieces], axis=0), 1, 0).astype(BF16)


def out_weights(pos, pieces, seen):
    d = pieces[0].shape[1]
    width = seen[0].shape[0]
    rows = sum(s.shape[1] for s in seen)
    wide = 512
    return _call(
        functools.partial(_out_weights, n=len(pieces), ns=len(seen)), (d // wide,),
        [pl.BlockSpec((p.shape[0], wide), lambda i, _: (0, i)) for p in pieces] + [ANY] * len(seen),
        pl.BlockSpec((width, wide), lambda i, _: (0, i)), _sds((width, d)),
        [pltpu.VMEM((width, rows), BF16), pltpu.SemaphoreType.DMA((len(seen),))],
        2 * rows * d * width, 2 * (rows * (d + width) + d * width), (pos, *pieces, *seen))


def _finish(pos_ref, own_ref, sib_ref, rh_ref, oh_ref, rl_ref, ol_ref, x_ref, dy_ref, gain_ref, dx_ref, dg_ref,
            own_s, sib_s, far_s, x_s, dy_s, gain_s, dx_s, dg_s, sem, out_sem):
    n, rows = x_s.shape[:2]
    part = lambda ref, i: ref.at[pl.ds(pl.multiple_of(i * rows, rows), rows), :]
    upper = lax.rem(lax.div(pos_ref[0], BLOCK), 2) == 1
    half = n // 2
    far = lambda i, low: (ol_ref if i >= half else rl_ref) if low else (rh_ref if i >= half else oh_ref)
    for i in range(n):
        for k, (ref, s) in enumerate(((own_ref, own_s), (sib_ref, sib_s), (x_ref, x_s), (dy_ref, dy_s))):
            pltpu.make_async_copy(part(ref, i), s.at[i], sem.at[i, k]).start()
        for low in (False, True):

            @pl.when(upper != low)
            def _():
                pltpu.make_async_copy(part(far(i, low), i % half), far_s.at[i], sem.at[i, 4]).start()

    get_gain = pltpu.make_async_copy(gain_ref, gain_s, out_sem.at[n])
    get_gain.start()
    get_gain.wait()
    dg_s[...] = jnp.zeros_like(dg_s)

    def step(i, _):
        for k, (ref, s) in enumerate(((own_ref, own_s), (sib_ref, sib_s), (x_ref, x_s), (dy_ref, dy_s))):
            pltpu.make_async_copy(part(ref, i), s.at[i], sem.at[i, k]).wait()
        pltpu.make_async_copy(part(rh_ref, 0), far_s.at[i], sem.at[i, 4]).wait()
        da = own_s[i] + sib_s[i].astype(F32) + far_s[i].astype(F32)
        x = x_s[i].astype(F32)
        scale = lax.rsqrt(jnp.mean(x * x, -1, keepdims=True) + 1e-6)
        h = x * scale
        dg_s[...] += jnp.sum(da * h, axis=0, keepdims=True)
        dh = da * gain_s[...].astype(F32)
        dx = scale * (dh - h * jnp.mean(dh * h, -1, keepdims=True))
        dx_s[i] = (dy_s[i].astype(F32) + dx).astype(BF16)
        pltpu.make_async_copy(dx_s.at[i], part(dx_ref, i), out_sem.at[i]).start()

    lax.fori_loop(0, n, step, None)
    last = pltpu.make_async_copy(dg_s, dg_ref, out_sem.at[n])
    last.start()
    for copy in _copies([(dx_s.at[i], part(dx_ref, i)) for i in range(n)], out_sem) + [last]:
        copy.wait()


def finish(pos, own, sib, rh, oh, rl, ol, x, dy, gain):
    rows, d = x.shape
    n = 8
    block = (n, rows // n, d)
    vmem, dma = pltpu.VMEM, pltpu.SemaphoreType.DMA
    return _all(
        _finish, 9, [_sds((rows, d)), _sds((1, d), F32)],
        [vmem(block, F32), vmem(block, BF16), vmem(block, BF16), vmem(block, BF16), vmem(block, BF16), vmem((1, d), BF16), vmem(block, BF16),
         vmem((1, d), F32), dma((n, 5)), dma((n + 1,))],
        3 * 10**9, 14 * rows * d, pos, own, sib, rh, oh, rl, ol, x, dy, gain)


def tables(rows):
    half = HEAD // 2
    angle = jnp.arange(rows).astype(F32)[:, None] * THETA ** (-jnp.arange(half, dtype=F32) / half)
    cos, sin = jnp.cos(angle), jnp.sin(angle)
    return jnp.concatenate([cos, cos], -1), jnp.concatenate([-sin, sin], -1)


SIBLING = [(0, 1), (1, 0), (2, 3), (3, 2)]
PARTNER = [(0, 2), (2, 0), (1, 3), (3, 1)]
ACROSS = [(0, 3), (3, 0), (1, 2), (2, 1)]


def solution(mesh):
    def move(t, pairs):
        return lax.ppermute(t, "tp", pairs)

    def work(x, dy, gain, wq, wk, wv, wo):
        me = lax.axis_index("tp")
        core = lax.rem(me, 2)
        upper = core == 1
        gain = gain[None]
        start = lambda block, half: block * BLOCK + half * HALF
        sib, far = me + 1 - 2 * core, 2 * (1 - lax.div(me, 2))
        pos = jnp.stack([start(me, 0), start(me, 1), start(sib, 0), start(sib, 1), start(far + 1, core), start(far + 1, 1 - core),
                         start(far, core), start(far, 1 - core)]).astype(jnp.int32)
        cos, sin = tables(4 * BLOCK)

        def after(t, *others):
            return lax.optimization_barrier((t, *others))[0]

        def halves(own, sib):
            return jnp.where(upper, own[HALF:], sib[:HALF]), jnp.where(upper, sib[HALF:], own[:HALF])

        e = move(dy, SIBLING)
        a = norm(x, gain)
        b = move(a, SIBLING)
        a_high, a_low = halves(a, b)
        ah = move(a_high, PARTNER)
        al = move(a_low, PARTNER)
        d_high, d_low = halves(*after((dy, e), a_low))
        dh = move(d_high, PARTNER)
        dl = move(d_low, PARTNER)

        w = (wq, wk, wv)
        q_n, k_n, v_n = project(pos, 0, (a, after(b, d_high, d_low)), *w, cos, sin)
        do_n = into(pos, (dy, after(e, q_n)), wo)
        ah = after(ah, do_n)
        ah2 = move(ah, SIBLING)
        q_h, k_h, v_h = project(pos, 4, (ah, ah2), *w, cos, sin)
        al = after(al, q_h)
        al2 = move(al, SIBLING)
        q_l, k_l, v_l = project(pos, 6, (al, al2), *w, cos, sin)
        keys = ((k_n, k_h, k_l), (v_n, v_h, v_l), cos, sin)
        seen_n, dq_n, dk, dv = attend(pos, 0, q_n, do_n, *keys)
        dh = after(dh, dq_n)
        dh2 = move(dh, SIBLING)
        do_h = into(pos, (dh, dh2), wo)
        seen_h, dq_h, dk, dv = attend(pos, 4, q_h, do_h, *keys, sums=(dk, dv))
        keep_h, send_h, g_h = back(pos, 4, dq_h, dk, dv, *w, cos, sin)
        add = lambda keep, came: (keep + came.astype(F32)).astype(BF16)
        dl = after(dl, send_h)
        dl2 = move(dl, SIBLING)
        sum_h = add(keep_h, move(send_h, SIBLING))
        r_h = move(sum_h, PARTNER)
        do_l = into(pos, (dl, after(dl2, sum_h)), wo)
        seen_l, dq_l, dk, dv = attend(pos, 6, q_l, do_l, *keys, sums=(dk, dv))
        keep_l, send_l, g_l = back(pos, 6, dq_l, dk, dv, *w, cos, sin)
        sum_l = add(keep_l, move(send_l, SIBLING))
        r_l = move(sum_l, PARTNER)
        keep_n, send_n, g_n = back(pos, 0, after(dq_n, sum_l), dk, dv, *w, cos, sin)
        s_n = move(send_n, SIBLING)
        by_wo = out_weights(pos, (dy, e, dh, dh2, dl, dl2), (seen_n, seen_h, after(seen_l, send_n)))
        r_h = after(r_h, by_wo)
        o_h = move(r_h, SIBLING)
        r_l = after(r_l, by_wo)
        o_l = move(r_l, SIBLING)
        by_x, part = finish(pos, keep_n, s_n, r_h, o_h, r_l, o_l, x, dy, gain)
        by_wq, by_wk, by_wv = weights(pos, (a, b, ah, ah2, al, al2), (after(g_n, part), g_h, g_l))
        by_gain = (part + move(part, SIBLING)) + (move(part, PARTNER) + move(part, ACROSS))
        return by_x, by_gain, by_wq, by_wk, by_wv, by_wo

    tokens, columns = P(("dp", "tp"), None), P(None, "tp")
    return jax.shard_map(
        work,
        mesh=mesh,
        in_specs=(tokens, tokens, P(None), columns, columns, columns, P("tp", None)),
        out_specs=(tokens, P("dp", None), P("dp", "tp"), P("dp", "tp"), P("dp", "tp"), P(("dp", "tp"), None)),
        check_vma=False,
    )
```

```python
import functools

import jax
import jax.numpy as jnp
from jax import lax
from jax.experimental import pallas as pl
from jax.experimental.pallas import tpu as pltpu
from jax.sharding import PartitionSpec as P


HEAD = 128
THETA = 10000
HIDDEN = -2e30
LOG2E = 1.4426950408889634
VMEM = 56 * 2**20
HALF = 128
BLOCK = 256
AHEAD = 2
F32, BF16 = jnp.float32, jnp.bfloat16
ANY = pl.BlockSpec(memory_space=pl.ANY)


def _dot(a, b, ca, cb):
    return lax.dot_general(a, b, (((ca,), (cb,)), ((), ())), preferred_element_type=F32)


def _call(kernel, grid, in_specs, out_specs, out_shape, scratch, flops, moved, args, scalars=1):
    return pl.pallas_call(
        kernel,
        grid_spec=pltpu.PrefetchScalarGridSpec(
            num_scalar_prefetch=scalars, grid=grid, in_specs=in_specs, out_specs=out_specs, scratch_shapes=scratch),
        out_shape=out_shape,
        compiler_params=pltpu.CompilerParams(dimension_semantics=("arbitrary",) * len(grid), vmem_limit_bytes=VMEM),
        cost_estimate=pl.CostEstimate(flops=int(flops), bytes_accessed=int(moved), transcendentals=0),
    )(*args)


def _fetch(pairs, sem):
    copies = [pltpu.make_async_copy(src, dst, sem.at[n]) for n, (src, dst) in enumerate(pairs)]
    for copy in copies:
        copy.start()
    for copy in copies:
        copy.wait()


def _sds(shape, dtype=BF16):
    return jax.ShapeDtypeStruct(shape, dtype)


def _table(ref, pos_ref, first, n):
    return jnp.concatenate([ref[pl.ds(pl.multiple_of(pos_ref[first + m], HALF), HALF), :] for m in range(n)], axis=0)


def _copies(pairs, sem, base=0):
    return [pltpu.make_async_copy(src, dst, sem.at[base + n]) for n, (src, dst) in enumerate(pairs)]


def _norm(x_ref, gain_ref, a_ref, x_s, a_s, sem, out_sem):
    n = x_s.shape[0]
    rows = x_s.shape[1]
    part = lambda ref, i: ref.at[pl.ds(pl.multiple_of(i * rows, rows), rows), :]
    get = lambda i: pltpu.make_async_copy(part(x_ref, i), x_s.at[i], sem.at[i])
    for i in range(AHEAD + 1):
        get(i).start()

    def step(i, _):
        get(i).wait()

        @pl.when(i + AHEAD + 1 < n)
        def _():
            get(i + AHEAD + 1).start()

        x = x_s[i].astype(F32)
        scale = lax.rsqrt(jnp.mean(x * x, -1, keepdims=True) + 1e-6)
        a_s[i] = (x * scale * gain_ref[...].astype(F32)).astype(BF16)
        pltpu.make_async_copy(a_s.at[i], part(a_ref, i), out_sem.at[i]).start()

    lax.fori_loop(0, n, step, None)
    for copy in _copies([(a_s.at[i], part(a_ref, i)) for i in range(n)], out_sem):
        copy.wait()


def norm(x, gain):
    rows, d = x.shape
    n = 8
    return pl.pallas_call(
        _norm,
        name="norm",
        in_specs=[ANY, pl.BlockSpec(memory_space=pltpu.VMEM)],
        out_specs=ANY,
        out_shape=_sds((rows, d)),
        scratch_shapes=[pltpu.VMEM((n, rows // n, d), BF16)] * 2 + [pltpu.SemaphoreType.DMA((n,))] * 2,
        compiler_params=pltpu.CompilerParams(vmem_limit_bytes=VMEM),
        cost_estimate=pl.CostEstimate(flops=10**9, bytes_accessed=4 * rows * d, transcendentals=0),
    )(x, gain)


def _all(kernel, n_in, out_shape, scratch, flops, moved, pos, *args):
    many = isinstance(out_shape, list)
    return pl.pallas_call(
        kernel,
        in_specs=[pl.BlockSpec(memory_space=pltpu.SMEM)] + [ANY] * n_in,
        out_specs=[ANY] * len(out_shape) if many else ANY,
        out_shape=out_shape,
        scratch_shapes=scratch,
        compiler_params=pltpu.CompilerParams(vmem_limit_bytes=VMEM),
        cost_estimate=pl.CostEstimate(flops=int(flops), bytes_accessed=int(moved), transcendentals=0),
    )(pos, *args)


def _pieces(pieces, a_s):
    at, pairs = 0, []
    for p in pieces:
        pairs.append((p, a_s.at[pl.ds(at, p.shape[0]), :]))
        at += p.shape[0]
    return pairs


def _places(pos_ref, ref, s, first):
    return [(ref.at[pl.ds(pl.multiple_of(pos_ref[first + m], HALF), HALF), :], s.at[pl.ds(m * HALF, HALF), :]) for m in range(s.shape[0] // HALF)]


def _project(pos_ref, *refs, n, first):
    pieces, (wq_ref, wk_ref, wv_ref, c_ref, s_ref, q_ref, k_ref, v_ref) = refs[:n], refs[n : n + 8]
    a_s, w_s, c_s, s_s, q_s, k_s, v_s, sem, w_sem, out_sem, kv_sem = refs[n + 8 :]
    steps, wide = w_s.shape[0] - 1, w_s.shape[2]
    pairs = _pieces(pieces, a_s) + _places(pos_ref, c_ref, c_s, first) + _places(pos_ref, s_ref, s_s, first)
    ready = _copies(pairs, sem)
    columns = lambda ref, i: ref.at[:, pl.ds(pl.multiple_of(i * wide, wide), wide)]
    tile = lambda i: pltpu.make_async_copy(columns(wq_ref, i), w_s.at[i], w_sem.at[i])
    kv = [pltpu.make_async_copy(w, w_s.at[steps, :, pl.ds(m * HEAD, HEAD)], kv_sem.at[m]) for m, w in enumerate((wk_ref, wv_ref))]
    for copy in ready + [tile(0)]:
        copy.start()
    for copy in ready:
        copy.wait()
    for i in range(1, AHEAD):
        tile(i).start()

    def turn(t):
        t = t.astype(BF16).astype(F32)
        return (t * c_s[...] + pltpu.roll(t, HEAD // 2, 1) * s_s[...]).astype(BF16)

    out = lambda i, slot: pltpu.make_async_copy(q_s.at[slot], columns(q_ref, i), out_sem.at[slot])

    def step(i, _):
        slot = lax.rem(i, 2)
        tile(i).wait()

        @pl.when(i + AHEAD < steps)
        def _():
            tile(i + AHEAD).start()

        @pl.when(i + AHEAD == steps)
        def _():
            for copy in kv:
                copy.start()

        t = _dot(a_s[...], w_s[i], 1, 0)

        @pl.when(i >= 2)
        def _():
            out(i - 2, slot).wait()

        for m in range(wide // HEAD):
            q_s[slot, :, m * HEAD : (m + 1) * HEAD] = turn(t[:, m * HEAD : (m + 1) * HEAD])
        out(i, slot).start()

    lax.fori_loop(0, steps, step, None)
    for copy in kv:
        copy.wait()
    t = _dot(a_s[...], w_s[steps], 1, 0)
    k_s[...] = turn(t[:, :HEAD])
    v_s[...] = t[:, HEAD:].astype(BF16)
    last = _copies([(k_s, k_ref), (v_s, v_ref)], kv_sem)
    for copy in last:
        copy.start()
    for copy in last + [out(steps - 2 + m, (steps + m) % 2) for m in range(2)]:
        copy.wait()


def project(pos, first, pieces, wq, wk, wv, cos, sin):
    d, width = wq.shape
    n, rows = len(pieces), sum(p.shape[0] for p in pieces)
    wide = 256
    steps = width // wide
    vmem, dma = pltpu.VMEM, pltpu.SemaphoreType.DMA
    return _all(
        functools.partial(_project, n=n, first=first), n + 5,
        [_sds((rows, width)), _sds((rows, HEAD)), _sds((rows, HEAD))],
        [vmem((rows, d), BF16), vmem((steps + 1, d, wide), BF16), vmem((rows, HEAD), F32), vmem((rows, HEAD), F32), vmem((2, rows, wide), BF16),
         vmem((rows, HEAD), BF16), vmem((rows, HEAD), BF16), dma((n + 2 * rows // HALF,)), dma((steps,)), dma((2,)), dma((2,))],
        2 * rows * d * (width + 2 * HEAD), 2 * (d * (width + 256) + rows * (d + width)), pos, *pieces, wq, wk, wv, cos, sin)


def _into(_, *refs, n):
    pieces, (w_ref, o_ref, a_s, w_s, o_s, sem, w_sem, out_sem) = refs[:n], refs[n:]
    steps, wide = w_s.shape[:2]
    ready = _copies(_pieces(pieces, a_s), sem)
    tile = lambda i: pltpu.make_async_copy(w_ref.at[pl.ds(pl.multiple_of(i * wide, wide), wide), :], w_s.at[i], w_sem.at[i])
    for copy in ready + [tile(0)]:
        copy.start()
    for copy in ready:
        copy.wait()
    for i in range(1, AHEAD):
        tile(i).start()
    out = lambda i, slot: pltpu.make_async_copy(o_s.at[slot], o_ref.at[:, pl.ds(pl.multiple_of(i * wide, wide), wide)], out_sem.at[slot])

    def step(i, _):
        slot = lax.rem(i, 2)
        tile(i).wait()

        @pl.when(i + AHEAD < steps)
        def _():
            tile(i + AHEAD).start()

        t = _dot(a_s[...], w_s[i], 1, 1).astype(BF16)

        @pl.when(i >= 2)
        def _():
            out(i - 2, slot).wait()

        o_s[slot] = t
        out(i, slot).start()

    lax.fori_loop(0, steps, step, None)
    for m in range(2):
        out(steps - 2 + m, (steps + m) % 2).wait()


def into(pos, pieces, wo):
    width, d = wo.shape
    n, rows = len(pieces), sum(p.shape[0] for p in pieces)
    wide = 256
    steps = width // wide
    vmem, dma = pltpu.VMEM, pltpu.SemaphoreType.DMA
    return _all(
        functools.partial(_into, n=n), n + 1, _sds((rows, width)),
        [vmem((rows, d), BF16), vmem((steps, wide, d), BF16), vmem((2, rows, wide), BF16), dma((n,)), dma((steps,)), dma((2,))],
        2 * rows * d * width, 2 * (d * width + rows * (d + width)), pos, *pieces, wo)


def _attend(pos_ref, q_ref, do_ref, kl_ref, kh_ref, kr_ref, vl_ref, vh_ref, vr_ref, c_ref, s_ref, *rest, first, hp, added):
    dk_in, dv_in = rest[:2] if added else (None, None)
    seen_ref, dq_ref, dk_ref, dv_ref, k_s, v_s, kt_s, vt_s, s_s, dp_s, o_s, dq_s, dk_s, dv_s = rest[-14:]
    iq, ih = pl.program_id(0), pl.program_id(1)
    wide = hp * BLOCK
    e = HEAD**-0.5 * LOG2E

    @pl.when((iq == 0) & (ih == 0))
    def _():
        at = 0
        for kc, vc in ((kl_ref, vl_ref), (kh_ref, vh_ref), (kr_ref, vr_ref)):
            for m in range(kc.shape[0] // HALF):
                here = pl.ds(pl.multiple_of(pos_ref[at], HALF), HALF)
                k_s[here, :] = kc[m * HALF : (m + 1) * HALF, :]
                v_s[here, :] = vc[m * HALF : (m + 1) * HALF, :]
                at += 1
        kt_s[...] = k_s[...].T
        vt_s[...] = v_s[...].T
        dk_s[...] = dk_in[...] if added else jnp.zeros_like(dk_s)
        dv_s[...] = dv_in[...] if added else jnp.zeros_like(dv_s)

    place = pos_ref[first + 2 * iq]
    own = lax.div(place, BLOCK)
    turned = lax.rem(place, BLOCK)
    q2 = jnp.concatenate([q_ref[:, m * HEAD : (m + 1) * HEAD] for m in range(hp)], axis=0)
    do2 = jnp.concatenate([do_ref[:, m * HEAD : (m + 1) * HEAD] for m in range(hp)], axis=0)

    def rows(j):
        return pl.ds(pl.multiple_of(j * BLOCK, BLOCK), BLOCK)

    here = rows(own)
    s = _dot(k_s[here, :], q2, 1, 1)
    query = lax.rem(lax.broadcasted_iota(jnp.int32, s.shape, 1) + turned, BLOCK)
    s = jnp.where(lax.broadcasted_iota(jnp.int32, s.shape, 0) <= query, s, HIDDEN)
    s_s[here, :] = s

    def scores(j, top):
        s = _dot(k_s[rows(j), :], q2, 1, 1)
        s_s[rows(j), :] = s
        return jnp.maximum(top, s.max(axis=0, keepdims=True))

    top = lax.fori_loop(0, own, scores, s.max(axis=0, keepdims=True))
    o_s[...] = jnp.zeros_like(o_s)
    dq_s[...] = jnp.zeros_like(dq_s)

    def weigh(j, sums):
        total, delta = sums
        dp = _dot(v_s[rows(j), :], do2, 1, 1)
        dp_s[rows(j), :] = dp
        p = jnp.exp2((s_s[rows(j), :] - top) * e)
        s_s[rows(j), :] = p
        o_s[...] += _dot(vt_s[:, rows(j)], p.astype(BF16), 1, 0)
        return total + p.sum(axis=0, keepdims=True), delta + (p * dp).sum(axis=0, keepdims=True)

    zero = jnp.zeros((1, wide), F32)
    total, delta = lax.fori_loop(0, own + 1, weigh, (zero, zero))
    inv = 1 / total
    delta = delta * inv

    def grads(j, _):
        p = s_s[rows(j), :] * inv
        ds = (p * (dp_s[rows(j), :] - delta)).astype(BF16)
        dv_s[rows(j), :] += _dot(p.astype(BF16), do2, 1, 0)
        dk_s[rows(j), :] += _dot(ds, q2, 1, 0)
        dq_s[...] += _dot(kt_s[:, rows(j)], ds, 1, 0)

    lax.fori_loop(0, own + 1, grads, None)
    cos, sin = _table(c_ref, pos_ref, first + 2 * iq, 2), _table(s_ref, pos_ref, first + 2 * iq, 2)
    o = (o_s[...] * inv).astype(BF16)
    for m in range(hp):
        seen_ref[m * HEAD : (m + 1) * HEAD, :] = o[:, m * BLOCK : (m + 1) * BLOCK]
        g = (dq_s[:, m * BLOCK : (m + 1) * BLOCK] * HEAD**-0.5).T.astype(BF16).astype(F32)
        dq_ref[:, m * HEAD : (m + 1) * HEAD] = (g * cos - pltpu.roll(g, HEAD // 2, 1) * sin).astype(BF16)

    @pl.when((iq == pl.num_programs(0) - 1) & (ih == pl.num_programs(1) - 1))
    def _():
        dk_ref[...] = dk_s[...]
        dv_ref[...] = dv_s[...]


def attend(pos, first, q, do, ks, vs, cos, sin, sums=None):
    rows, width = q.shape
    hp = 4
    sk = sum(k.shape[0] for k in ks)
    tile = pl.BlockSpec((BLOCK, hp * HEAD), lambda i, h, _: (i, h))
    whole = lambda a: pl.BlockSpec(a.shape, lambda i, h, _: (0, 0))
    keys = _sds((sk, HEAD), F32)
    given = (*ks, *vs, cos, sin, *(sums or ()))
    wide = hp * BLOCK
    vmem = lambda *shape, t=F32: pltpu.VMEM(shape, t)
    return _call(
        functools.partial(_attend, first=first, hp=hp, added=sums is not None), (rows // BLOCK, width // (hp * HEAD)),
        [tile, tile, *map(whole, given)],
        [pl.BlockSpec((hp * HEAD, BLOCK), lambda i, h, _: (h, i)), tile, whole(keys), whole(keys)],
        [_sds((width, rows)), _sds((rows, width)), keys, keys],
        [vmem(sk, HEAD, t=BF16), vmem(sk, HEAD, t=BF16), vmem(HEAD, sk, t=BF16), vmem(HEAD, sk, t=BF16), vmem(sk, wide), vmem(sk, wide),
         vmem(HEAD, wide), vmem(HEAD, wide), vmem(sk, HEAD), vmem(sk, HEAD)],
        2 * 6 * 2 * rows * sk * width * 0.6, 8 * rows * width, (pos, q, do, *given))


def _back(pos_ref, dq_ref, dk_ref, dv_ref, c_ref, s_ref, wq_ref, wk_ref, wv_ref, keep_ref, send_ref, g_ref,
          g_s, dk_s, dv_s, c_s, s_s, w_s, keep_s, send_s, sem, w_sem, out_sem, g_sem, *, first):
    rows, width = dq_ref.shape
    half = rows // 2
    steps, wide = w_s.shape[:2]
    pairs = [(dq_ref, g_s.at[:, pl.ds(0, width)])]
    for ref, s in ((dk_ref, dk_s), (dv_ref, dv_s), (c_ref, c_s), (s_ref, s_s)):
        pairs += _places(pos_ref, ref, s, first)
    ready = _copies(pairs, sem)
    lines = lambda ref, i: ref.at[pl.ds(pl.multiple_of(i * wide, wide), wide), :]
    parts = ((wq_ref, 0, width), (wk_ref, width, HEAD), (wv_ref, width + HEAD, HEAD))
    tile = lambda i: [pltpu.make_async_copy(lines(w, i), w_s.at[i, :, pl.ds(at, size)], w_sem.at[i, m]) for m, (w, at, size) in enumerate(parts)]
    for copy in ready + tile(0) + tile(1):
        copy.start()
    for copy in ready:
        copy.wait()
    for copy in tile(2):
        copy.start()
    g = (dk_s[...] * HEAD**-0.5).astype(BF16).astype(F32)
    g_s[:, width : width + HEAD] = (g * c_s[...] - pltpu.roll(g, HEAD // 2, 1) * s_s[...]).astype(BF16)
    g_s[:, width + HEAD :] = dv_s[...].astype(BF16)
    g_out = pltpu.make_async_copy(g_s, g_ref, g_sem.at[0])
    g_out.start()

    def out(i, slot):
        columns = pl.ds(pl.multiple_of(i * wide, wide), wide)
        return _copies([(keep_s.at[slot], keep_ref.at[:, columns]), (send_s.at[slot], send_ref.at[:, columns])], out_sem.at[slot])

    def step(i, _):
        slot = lax.rem(i, 2)
        for copy in tile(i):
            copy.wait()

        @pl.when(i + 3 < steps)
        def _():
            for copy in tile(i + 3):
                copy.start()

        t = _dot(g_s[...], w_s[i], 1, 1)

        @pl.when(i >= 2)
        def _():
            for copy in out(i - 2, slot):
                copy.wait()

        keep_s[slot] = t[:half]
        send_s[slot] = t[half:].astype(BF16)
        for copy in out(i, slot):
            copy.start()

    lax.fori_loop(0, steps, step, None)
    for m in range(2):
        for copy in out(steps - 2 + m, (steps + m) % 2):
            copy.wait()
    g_out.wait()


def back(pos, first, dq, dk, dv, wq, wk, wv, cos, sin):
    d, width = wq.shape
    rows = dq.shape[0]
    wide = 512
    steps = d // wide
    full = width + 2 * HEAD
    vmem, dma = pltpu.VMEM, pltpu.SemaphoreType.DMA
    line = vmem((rows, HEAD), F32)
    return _all(
        functools.partial(_back, first=first), 8, [_sds((rows // 2, d), F32), _sds((rows // 2, d)), _sds((rows, full))],
        [vmem((rows, full), BF16), line, line, line, line, vmem((steps, wide, full), BF16), vmem((2, rows // 2, wide), F32),
         vmem((2, rows // 2, wide), BF16), dma((1 + 4 * rows // HALF,)), dma((steps, 3)), dma((2, 2)), dma((1,))],
        2 * rows * d * full, 2 * (d * full + rows * (2 * d + width)), pos, dq, dk, dv, cos, sin, wq, wk, wv)


def _weights(_, *refs, n, ng):
    pieces, gs, (wq_ref, wk_ref, wv_ref, g_s, sem) = refs[:n], refs[n : n + ng], refs[n + ng :]

    @pl.when(pl.program_id(0) == 0)
    def _():
        at, pairs = 0, []
        for g in gs:
            pairs.append((g, g_s.at[pl.ds(at, g.shape[0]), :]))
            at += g.shape[0]
        _fetch(pairs, sem)

    a = jnp.concatenate([p[...] for p in pieces], axis=0)
    t = _dot(a, g_s[...], 0, 0).astype(BF16)
    width = wq_ref.shape[1]
    wq_ref[...] = t[:, :width]
    wk_ref[...] = t[:, width : width + HEAD]
    wv_ref[...] = t[:, width + HEAD :]


def weights(pos, pieces, gs):
    d = pieces[0].shape[1]
    full = gs[0].shape[1]
    width = full - 2 * HEAD
    rows = sum(g.shape[0] for g in gs)
    wide = 512
    tile = lambda n: pl.BlockSpec((wide, n), lambda i, _: (i, 0))
    return _call(
        functools.partial(_weights, n=len(pieces), ng=len(gs)), (d // wide,),
        [pl.BlockSpec((p.shape[0], wide), lambda i, _: (0, i)) for p in pieces] + [ANY] * len(gs),
        [tile(width), tile(HEAD), tile(HEAD)], [_sds((d, width)), _sds((d, HEAD)), _sds((d, HEAD))],
        [pltpu.VMEM((rows, full), BF16), pltpu.SemaphoreType.DMA((len(gs),))],
        2 * rows * d * full, 2 * (rows * (d + full) + d * full), (pos, *pieces, *gs))


def _out_weights(_, *refs, n, ns):
    pieces, seen, (o_ref, s_s, sem) = refs[:n], refs[n : n + ns], refs[n + ns :]

    @pl.when(pl.program_id(0) == 0)
    def _():
        at, pairs = 0, []
        for s in seen:
            pairs.append((s, s_s.at[:, pl.ds(at, s.shape[1])]))
            at += s.shape[1]
        _fetch(pairs, sem)

    o_ref[...] = _dot(s_s[...], jnp.concatenate([p[...] for p in pieces], axis=0), 1, 0).astype(BF16)


def out_weights(pos, pieces, seen):
    d = pieces[0].shape[1]
    width = seen[0].shape[0]
    rows = sum(s.shape[1] for s in seen)
    wide = 512
    return _call(
        functools.partial(_out_weights, n=len(pieces), ns=len(seen)), (d // wide,),
        [pl.BlockSpec((p.shape[0], wide), lambda i, _: (0, i)) for p in pieces] + [ANY] * len(seen),
        pl.BlockSpec((width, wide), lambda i, _: (0, i)), _sds((width, d)),
        [pltpu.VMEM((width, rows), BF16), pltpu.SemaphoreType.DMA((len(seen),))],
        2 * rows * d * width, 2 * (rows * (d + width) + d * width), (pos, *pieces, *seen))


def _finish(pos_ref, own_ref, sib_ref, rh_ref, oh_ref, rl_ref, ol_ref, x_ref, dy_ref, gain_ref, dx_ref, dg_ref,
            own_s, sib_s, far_s, x_s, dy_s, gain_s, dx_s, dg_s, sem, out_sem):
    n, rows = x_s.shape[:2]
    part = lambda ref, i: ref.at[pl.ds(pl.multiple_of(i * rows, rows), rows), :]
    upper = lax.rem(lax.div(pos_ref[0], BLOCK), 2) == 1
    half = n // 2
    far = lambda late, low: (ol_ref if late else rl_ref) if low else (rh_ref if late else oh_ref)
    rest = ((own_ref, own_s), (sib_ref, sib_s), (x_ref, x_s), (dy_ref, dy_s))

    def get(i):
        for k, (ref, s) in enumerate(rest):
            pltpu.make_async_copy(part(ref, i), s.at[i], sem.at[i, k]).start()
        for low in (False, True):
            for late in (False, True):

                @pl.when((upper != low) & ((i >= half) == late))
                def _():
                    pltpu.make_async_copy(part(far(late, low), lax.rem(i, half)), far_s.at[i], sem.at[i, 4]).start()

    get_gain = pltpu.make_async_copy(gain_ref, gain_s, out_sem.at[n])
    get_gain.start()
    for i in range(AHEAD):
        get(jnp.int32(i))
    get_gain.wait()
    dg_s[...] = jnp.zeros_like(dg_s)

    def step(i, _):
        @pl.when(i + AHEAD < n)
        def _():
            get(i + AHEAD)

        for k, (ref, s) in enumerate(rest):
            pltpu.make_async_copy(part(ref, i), s.at[i], sem.at[i, k]).wait()
        pltpu.make_async_copy(part(rh_ref, 0), far_s.at[i], sem.at[i, 4]).wait()
        da = own_s[i] + sib_s[i].astype(F32) + far_s[i].astype(F32)
        x = x_s[i].astype(F32)
        scale = lax.rsqrt(jnp.mean(x * x, -1, keepdims=True) + 1e-6)
        h = x * scale
        dg_s[...] += jnp.sum(da * h, axis=0, keepdims=True)
        dh = da * gain_s[...].astype(F32)
        dx = scale * (dh - h * jnp.mean(dh * h, -1, keepdims=True))
        dx_s[i] = (dy_s[i].astype(F32) + dx).astype(BF16)
        pltpu.make_async_copy(dx_s.at[i], part(dx_ref, i), out_sem.at[i]).start()

    lax.fori_loop(0, n, step, None)
    last = pltpu.make_async_copy(dg_s, dg_ref, out_sem.at[n])
    last.start()
    for copy in _copies([(dx_s.at[i], part(dx_ref, i)) for i in range(n)], out_sem) + [last]:
        copy.wait()


def finish(pos, own, sib, rh, oh, rl, ol, x, dy, gain):
    rows, d = x.shape
    n = 8
    block = (n, rows // n, d)
    vmem, dma = pltpu.VMEM, pltpu.SemaphoreType.DMA
    return _all(
        _finish, 9, [_sds((rows, d)), _sds((1, d), F32)],
        [vmem(block, F32), vmem(block, BF16), vmem(block, BF16), vmem(block, BF16), vmem(block, BF16), vmem((1, d), BF16), vmem(block, BF16),
         vmem((1, d), F32), dma((n, 5)), dma((n + 1,))],
        3 * 10**9, 14 * rows * d, pos, own, sib, rh, oh, rl, ol, x, dy, gain)


def tables(rows):
    half = HEAD // 2
    angle = jnp.arange(rows).astype(F32)[:, None] * THETA ** (-jnp.arange(half, dtype=F32) / half)
    cos, sin = jnp.cos(angle), jnp.sin(angle)
    return jnp.concatenate([cos, cos], -1), jnp.concatenate([-sin, sin], -1)


SIBLING = [(0, 1), (1, 0), (2, 3), (3, 2)]
PARTNER = [(0, 2), (2, 0), (1, 3), (3, 1)]
ACROSS = [(0, 3), (3, 0), (1, 2), (2, 1)]


def solution(mesh):
    def move(t, pairs):
        return lax.ppermute(t, "tp", pairs)

    def work(x, dy, gain, wq, wk, wv, wo):
        me = lax.axis_index("tp")
        core = lax.rem(me, 2)
        upper = core == 1
        gain = gain[None]
        start = lambda block, half: block * BLOCK + half * HALF
        sib, far = me + 1 - 2 * core, 2 * (1 - lax.div(me, 2))
        pos = jnp.stack([start(me, 0), start(me, 1), start(sib, 0), start(sib, 1), start(far + 1, core), start(far + 1, 1 - core),
                         start(far, core), start(far, 1 - core)]).astype(jnp.int32)
        cos, sin = tables(4 * BLOCK)

        def after(t, *others):
            return lax.optimization_barrier((t, *others))[0]

        def halves(own, sib):
            return jnp.where(upper, own[HALF:], sib[:HALF]), jnp.where(upper, sib[HALF:], own[:HALF])

        e = move(dy, SIBLING)
        a = norm(x, gain)
        b = move(a, SIBLING)
        a_high, a_low = halves(a, b)
        ah = move(a_high, PARTNER)
        al = move(a_low, PARTNER)
        d_high, d_low = halves(*after((dy, e), a_low))
        dh = move(d_high, PARTNER)
        dl = move(d_low, PARTNER)

        w = (wq, wk, wv)
        q_n, k_n, v_n = project(pos, 0, (a, after(b, d_high, d_low)), *w, cos, sin)
        do_n = into(pos, (dy, after(e, q_n)), wo)
        ah = after(ah, do_n)
        ah2 = move(ah, SIBLING)
        q_h, k_h, v_h = project(pos, 4, (ah, ah2), *w, cos, sin)
        al = after(al, q_h)
        al2 = move(al, SIBLING)
        q_l, k_l, v_l = project(pos, 6, (al, al2), *w, cos, sin)
        keys = ((k_n, k_h, k_l), (v_n, v_h, v_l), cos, sin)
        seen_n, dq_n, dk, dv = attend(pos, 0, q_n, do_n, *keys)
        dh = after(dh, dq_n)
        dh2 = move(dh, SIBLING)
        do_h = into(pos, (dh, dh2), wo)
        seen_h, dq_h, dk, dv = attend(pos, 4, q_h, do_h, *keys, sums=(dk, dv))
        keep_h, send_h, g_h = back(pos, 4, dq_h, dk, dv, *w, cos, sin)
        add = lambda keep, came: (keep + came.astype(F32)).astype(BF16)
        dl = after(dl, send_h)
        dl2 = move(dl, SIBLING)
        sum_h = add(keep_h, move(send_h, SIBLING))
        r_h = move(sum_h, PARTNER)
        do_l = into(pos, (dl, after(dl2, sum_h)), wo)
        seen_l, dq_l, dk, dv = attend(pos, 6, q_l, do_l, *keys, sums=(dk, dv))
        keep_l, send_l, g_l = back(pos, 6, dq_l, dk, dv, *w, cos, sin)
        sum_l = add(keep_l, move(send_l, SIBLING))
        r_l = move(sum_l, PARTNER)
        keep_n, send_n, g_n = back(pos, 0, after(dq_n, sum_l), dk, dv, *w, cos, sin)
        s_n = move(send_n, SIBLING)
        by_wo = out_weights(pos, (dy, e, dh, dh2, dl, dl2), (seen_n, seen_h, after(seen_l, send_n)))
        r_h = after(r_h, by_wo)
        o_h = move(r_h, SIBLING)
        r_l = after(r_l, by_wo)
        o_l = move(r_l, SIBLING)
        by_x, part = finish(pos, keep_n, s_n, r_h, o_h, r_l, o_l, x, dy, gain)
        by_wq, by_wk, by_wv = weights(pos, (a, b, ah, ah2, al, al2), (after(g_n, part), g_h, g_l))
        by_gain = (part + move(part, SIBLING)) + (move(part, PARTNER) + move(part, ACROSS))
        return by_x, by_gain, by_wq, by_wk, by_wv, by_wo

    tokens, columns = P(("dp", "tp"), None), P(None, "tp")
    return jax.shard_map(
        work,
        mesh=mesh,
        in_specs=(tokens, tokens, P(None), columns, columns, columns, P("tp", None)),
        out_specs=(tokens, P("dp", None), P("dp", "tp"), P("dp", "tp"), P("dp", "tp"), P(("dp", "tp"), None)),
        check_vma=False,
    )
```

```python
import functools

import jax
import jax.numpy as jnp
from jax import lax
from jax.experimental import pallas as pl
from jax.experimental.pallas import tpu as pltpu
from jax.sharding import PartitionSpec as P


HEAD = 128
THETA = 10000
HIDDEN = -2e30
LOG2E = 1.4426950408889634
VMEM = 56 * 2**20
HALF = 128
BLOCK = 256
LAG = 3
AHEAD = 2
F32, BF16 = jnp.float32, jnp.bfloat16
ANY = pl.BlockSpec(memory_space=pl.ANY)


def _dot(a, b, ca, cb):
    return lax.dot_general(a, b, (((ca,), (cb,)), ((), ())), preferred_element_type=F32)


def _call(kernel, grid, in_specs, out_specs, out_shape, scratch, flops, moved, args, scalars=1):
    return pl.pallas_call(
        kernel,
        grid_spec=pltpu.PrefetchScalarGridSpec(
            num_scalar_prefetch=scalars, grid=grid, in_specs=in_specs, out_specs=out_specs, scratch_shapes=scratch),
        out_shape=out_shape,
        compiler_params=pltpu.CompilerParams(dimension_semantics=("arbitrary",) * len(grid), vmem_limit_bytes=VMEM),
        cost_estimate=pl.CostEstimate(flops=int(flops), bytes_accessed=int(moved), transcendentals=0),
    )(*args)


def _fetch(pairs, sem):
    copies = [pltpu.make_async_copy(src, dst, sem.at[n]) for n, (src, dst) in enumerate(pairs)]
    for copy in copies:
        copy.start()
    for copy in copies:
        copy.wait()


def _here():
    me = lax.axis_index("tp")
    core = lax.rem(me, 2)
    return me, core, me + 1 - 2 * core, 2 * (1 - lax.div(me, 2))


def _starts(chunk):
    me, core, sib, far = _here()
    at = lambda block, half: block * BLOCK + half * HALF
    if chunk == "near":
        return [at(me, 0), at(me, 1), at(sib, 0), at(sib, 1)]
    block = far + (chunk == "high")
    return [at(block, core), at(block, 1 - core)]


def _meet():
    barrier = pltpu.get_barrier_semaphore()
    pl.semaphore_signal(barrier, inc=1, device_id={"tp": _here()[2]}, device_id_type=pl.DeviceIdType.MESH)
    pl.semaphore_wait(barrier, 1)


def _to_sibling(src, dst, send_sem, recv_sem):
    return pltpu.make_async_remote_copy(src_ref=src, dst_ref=dst, send_sem=send_sem, recv_sem=recv_sem, device_id={"tp": _here()[2]},
                                        device_id_type=pl.DeviceIdType.MESH)


def _sds(shape, dtype=BF16):
    return jax.ShapeDtypeStruct(shape, dtype)


def _table(ref, pos_ref, first, n):
    return jnp.concatenate([ref[pl.ds(pl.multiple_of(pos_ref[first + m], HALF), HALF), :] for m in range(n)], axis=0)


def _copies(pairs, sem, base=0):
    return [pltpu.make_async_copy(src, dst, sem.at[base + n]) for n, (src, dst) in enumerate(pairs)]


def _norm(x_ref, gain_ref, a_ref, x_s, a_s, sem, out_sem):
    n = x_s.shape[0]
    rows = x_s.shape[1]
    part = lambda ref, i: ref.at[pl.ds(pl.multiple_of(i * rows, rows), rows), :]
    get = lambda i: pltpu.make_async_copy(part(x_ref, i), x_s.at[i], sem.at[i])
    for i in range(AHEAD + 1):
        get(i).start()

    def step(i, _):
        get(i).wait()

        @pl.when(i + AHEAD + 1 < n)
        def _():
            get(i + AHEAD + 1).start()

        x = x_s[i].astype(F32)
        scale = lax.rsqrt(jnp.mean(x * x, -1, keepdims=True) + 1e-6)
        a_s[i] = (x * scale * gain_ref[...].astype(F32)).astype(BF16)
        pltpu.make_async_copy(a_s.at[i], part(a_ref, i), out_sem.at[i]).start()

    lax.fori_loop(0, n, step, None)
    for copy in _copies([(a_s.at[i], part(a_ref, i)) for i in range(n)], out_sem):
        copy.wait()


def norm(x, gain):
    rows, d = x.shape
    n = 8
    return pl.pallas_call(
        _norm,
        name="norm",
        in_specs=[ANY, pl.BlockSpec(memory_space=pltpu.VMEM)],
        out_specs=ANY,
        out_shape=_sds((rows, d)),
        scratch_shapes=[pltpu.VMEM((n, rows // n, d), BF16)] * 2 + [pltpu.SemaphoreType.DMA((n,))] * 2,
        compiler_params=pltpu.CompilerParams(vmem_limit_bytes=VMEM),
        cost_estimate=pl.CostEstimate(flops=10**9, bytes_accessed=4 * rows * d, transcendentals=0),
    )(x, gain)


def _all(kernel, out_shape, scratch, flops, moved, *args, meeting=None):
    many = isinstance(out_shape, list)
    extra = {} if meeting is None else dict(collective_id=meeting, has_side_effects=True)
    return pl.pallas_call(
        kernel,
        in_specs=[ANY] * len(args),
        out_specs=[ANY] * len(out_shape) if many else ANY,
        out_shape=out_shape,
        scratch_shapes=scratch,
        compiler_params=pltpu.CompilerParams(vmem_limit_bytes=VMEM, **extra),
        cost_estimate=pl.CostEstimate(flops=int(flops), bytes_accessed=int(moved), transcendentals=0),
    )(*args)


def _pieces(pieces, a_s):
    at, pairs = 0, []
    for p in pieces:
        pairs.append((p, a_s.at[pl.ds(at, p.shape[0]), :]))
        at += p.shape[0]
    return pairs


def _places(chunk, ref, s):
    return [(ref.at[pl.ds(pl.multiple_of(at, HALF), HALF), :], s.at[pl.ds(m * HALF, HALF), :]) for m, at in enumerate(_starts(chunk))]


def _forward(piece, a_s, f_ref, sems):
    rows = piece.shape[0]
    under = a_s.at[pl.ds(rows, rows), :]
    return _to_sibling(piece, under, sems.at[0], sems.at[1]), pltpu.make_async_copy(under, f_ref, sems.at[2])


def _project(*refs, n, chunk):
    pieces, (wq_ref, wk_ref, wv_ref, c_ref, s_ref, q_ref, k_ref, v_ref), refs = refs[:n], refs[n : n + 8], refs[n + 8 :]
    f_ref, refs = (None, refs) if chunk == "near" else (refs[0], refs[1:])
    a_s, w_s, c_s, s_s, q_s, k_s, v_s, sem, w_sem, out_sem, kv_sem, f_sem = refs
    steps, wide = w_s.shape[0] - 1, w_s.shape[2]
    pairs = _pieces(pieces, a_s) + _places(chunk, c_ref, c_s) + _places(chunk, s_ref, s_s)
    ready = _copies(pairs, sem)
    columns = lambda ref, i: ref.at[:, pl.ds(pl.multiple_of(i * wide, wide), wide)]
    tile = lambda i: pltpu.make_async_copy(columns(wq_ref, i), w_s.at[i], w_sem.at[i])
    kv = [pltpu.make_async_copy(w, w_s.at[steps, :, pl.ds(m * HEAD, HEAD)], kv_sem.at[m]) for m, w in enumerate((wk_ref, wv_ref))]
    for copy in ready + [tile(0)]:
        copy.start()
    if f_ref is not None:
        _meet()
        forward, keep = _forward(pieces[0], a_s, f_ref, f_sem)
        forward.start()
    for copy in ready:
        copy.wait()
    for i in range(1, AHEAD):
        tile(i).start()
    if f_ref is not None:
        forward.wait()
        keep.start()

    def turn(t):
        t = t.astype(BF16).astype(F32)
        return (t * c_s[...] + pltpu.roll(t, HEAD // 2, 1) * s_s[...]).astype(BF16)

    out = lambda i, slot: pltpu.make_async_copy(q_s.at[slot], columns(q_ref, i), out_sem.at[slot])

    def step(i, _):
        slot = lax.rem(i, 2)
        tile(i).wait()

        @pl.when(i + AHEAD < steps)
        def _():
            tile(i + AHEAD).start()

        @pl.when(i + AHEAD == steps)
        def _():
            for copy in kv:
                copy.start()

        t = _dot(a_s[...], w_s[i], 1, 0)

        @pl.when(i >= 2)
        def _():
            out(i - 2, slot).wait()

        for m in range(wide // HEAD):
            q_s[slot, :, m * HEAD : (m + 1) * HEAD] = turn(t[:, m * HEAD : (m + 1) * HEAD])
        out(i, slot).start()

    lax.fori_loop(0, steps, step, None)
    for copy in kv:
        copy.wait()
    t = _dot(a_s[...], w_s[steps], 1, 0)
    k_s[...] = turn(t[:, :HEAD])
    v_s[...] = t[:, HEAD:].astype(BF16)
    last = _copies([(k_s, k_ref), (v_s, v_ref)], kv_sem)
    for copy in last:
        copy.start()
    for copy in last + [out(steps - 2 + m, (steps + m) % 2) for m in range(2)]:
        copy.wait()
    if f_ref is not None:
        keep.wait()


def project(chunk, pieces, wq, wk, wv, cos, sin, meeting=None):
    d, width = wq.shape
    n, rows = len(pieces), sum(p.shape[0] for p in pieces)
    more = [] if meeting is None else [_sds((rows, d))]
    rows *= 1 + len(more)
    wide = 256
    steps = width // wide
    vmem, dma = pltpu.VMEM, pltpu.SemaphoreType.DMA
    return _all(
        functools.partial(_project, n=n, chunk=chunk),
        [_sds((rows, width)), _sds((rows, HEAD)), _sds((rows, HEAD)), *more],
        [vmem((rows, d), BF16), vmem((steps + 1, d, wide), BF16), vmem((rows, HEAD), F32), vmem((rows, HEAD), F32), vmem((2, rows, wide), BF16),
         vmem((rows, HEAD), BF16), vmem((rows, HEAD), BF16), dma((n + 2 * rows // HALF,)), dma((steps,)), dma((2,)), dma((2,)), dma((3,))],
        2 * rows * d * (width + 2 * HEAD), 2 * (d * (width + 256) + rows * (d + width)), *pieces, wq, wk, wv, cos, sin, meeting=meeting)


def _into(*refs, n, forwards):
    pieces, w_ref, o_ref, refs = refs[:n], refs[n], refs[n + 1], refs[n + 2 :]
    f_ref, refs = (refs[0], refs[1:]) if forwards else (None, refs)
    a_s, w_s, o_s, sem, w_sem, out_sem, f_sem = refs
    steps, wide = w_s.shape[:2]
    ready = _copies(_pieces(pieces, a_s), sem)
    tile = lambda i: pltpu.make_async_copy(w_ref.at[pl.ds(pl.multiple_of(i * wide, wide), wide), :], w_s.at[i], w_sem.at[i])
    for copy in ready + [tile(0)]:
        copy.start()
    if forwards:
        _meet()
        forward, keep = _forward(pieces[0], a_s, f_ref, f_sem)
        forward.start()
    for copy in ready:
        copy.wait()
    for i in range(1, AHEAD):
        tile(i).start()
    if forwards:
        forward.wait()
        keep.start()
    out = lambda i, slot: pltpu.make_async_copy(o_s.at[slot], o_ref.at[:, pl.ds(pl.multiple_of(i * wide, wide), wide)], out_sem.at[slot])

    def step(i, _):
        slot = lax.rem(i, 2)
        tile(i).wait()

        @pl.when(i + AHEAD < steps)
        def _():
            tile(i + AHEAD).start()

        t = _dot(a_s[...], w_s[i], 1, 1).astype(BF16)

        @pl.when(i >= 2)
        def _():
            out(i - 2, slot).wait()

        o_s[slot] = t
        out(i, slot).start()

    lax.fori_loop(0, steps, step, None)
    for m in range(2):
        out(steps - 2 + m, (steps + m) % 2).wait()
    if forwards:
        keep.wait()


def into(pieces, wo, meeting=None):
    width, d = wo.shape
    n, rows = len(pieces), sum(p.shape[0] for p in pieces)
    more = [] if meeting is None else [_sds((rows, d))]
    rows *= 1 + len(more)
    result = _sds((rows, width))
    wide = 256
    steps = width // wide
    vmem, dma = pltpu.VMEM, pltpu.SemaphoreType.DMA
    return _all(
        functools.partial(_into, n=n, forwards=bool(more)), [result, *more] if more else result,
        [vmem((rows, d), BF16), vmem((steps, wide, d), BF16), vmem((2, rows, wide), BF16), dma((n,)), dma((steps,)), dma((2,)), dma((3,))],
        2 * rows * d * width, 2 * (d * width + rows * (d + width)), *pieces, wo, meeting=meeting)


def _attend(pos_ref, q_ref, do_ref, kl_ref, kh_ref, kr_ref, vl_ref, vh_ref, vr_ref, c_ref, s_ref, *rest, first, hp, added):
    dk_in, dv_in = rest[:2] if added else (None, None)
    seen_ref, dq_ref, dk_ref, dv_ref, k_s, v_s, kt_s, vt_s, s_s, dp_s, o_s, dq_s, dk_s, dv_s = rest[-14:]
    iq, ih = pl.program_id(0), pl.program_id(1)
    wide = hp * BLOCK
    e = HEAD**-0.5 * LOG2E

    @pl.when((iq == 0) & (ih == 0))
    def _():
        at = 0
        for kc, vc in ((kl_ref, vl_ref), (kh_ref, vh_ref), (kr_ref, vr_ref)):
            for m in range(kc.shape[0] // HALF):
                here = pl.ds(pl.multiple_of(pos_ref[at], HALF), HALF)
                k_s[here, :] = kc[m * HALF : (m + 1) * HALF, :]
                v_s[here, :] = vc[m * HALF : (m + 1) * HALF, :]
                at += 1
        kt_s[...] = k_s[...].T
        vt_s[...] = v_s[...].T
        dk_s[...] = dk_in[...] if added else jnp.zeros_like(dk_s)
        dv_s[...] = dv_in[...] if added else jnp.zeros_like(dv_s)

    place = pos_ref[first + 2 * iq]
    own = lax.div(place, BLOCK)
    turned = lax.rem(place, BLOCK)
    q2 = jnp.concatenate([q_ref[:, m * HEAD : (m + 1) * HEAD] for m in range(hp)], axis=0)
    do2 = jnp.concatenate([do_ref[:, m * HEAD : (m + 1) * HEAD] for m in range(hp)], axis=0)

    def rows(j):
        return pl.ds(pl.multiple_of(j * BLOCK, BLOCK), BLOCK)

    here = rows(own)
    s = _dot(k_s[here, :], q2, 1, 1)
    query = lax.rem(lax.broadcasted_iota(jnp.int32, s.shape, 1) + turned, BLOCK)
    s = jnp.where(lax.broadcasted_iota(jnp.int32, s.shape, 0) <= query, s, HIDDEN)
    s_s[here, :] = s

    def scores(j, top):
        s = _dot(k_s[rows(j), :], q2, 1, 1)
        s_s[rows(j), :] = s
        return jnp.maximum(top, s.max(axis=0, keepdims=True))

    top = lax.fori_loop(0, own, scores, s.max(axis=0, keepdims=True))
    o_s[...] = jnp.zeros_like(o_s)
    dq_s[...] = jnp.zeros_like(dq_s)

    def weigh(j, sums):
        total, delta = sums
        dp = _dot(v_s[rows(j), :], do2, 1, 1)
        dp_s[rows(j), :] = dp.astype(BF16)
        p = jnp.exp2((s_s[rows(j), :] - top) * e)
        s_s[rows(j), :] = p
        o_s[...] += _dot(vt_s[:, rows(j)], p.astype(BF16), 1, 0)
        return total + p.sum(axis=0, keepdims=True), delta + (p * dp).sum(axis=0, keepdims=True)

    zero = jnp.zeros((1, wide), F32)
    total, delta = lax.fori_loop(0, own + 1, weigh, (zero, zero))
    inv = 1 / total
    delta = delta * inv

    def grads(j, _):
        p = s_s[rows(j), :] * inv
        ds = (p * (dp_s[rows(j), :] - delta)).astype(BF16)
        dv_s[rows(j), :] += _dot(p.astype(BF16), do2, 1, 0)
        dk_s[rows(j), :] += _dot(ds, q2, 1, 0)
        dq_s[...] += _dot(kt_s[:, rows(j)], ds, 1, 0)

    lax.fori_loop(0, own + 1, grads, None)
    cos, sin = _table(c_ref, pos_ref, first + 2 * iq, 2), _table(s_ref, pos_ref, first + 2 * iq, 2)
    o = (o_s[...] * inv).astype(BF16)
    for m in range(hp):
        seen_ref[m * HEAD : (m + 1) * HEAD, :] = o[:, m * BLOCK : (m + 1) * BLOCK]
        g = (dq_s[:, m * BLOCK : (m + 1) * BLOCK] * HEAD**-0.5).T.astype(BF16).astype(F32)
        dq_ref[:, m * HEAD : (m + 1) * HEAD] = (g * cos - pltpu.roll(g, HEAD // 2, 1) * sin).astype(BF16)

    @pl.when((iq == pl.num_programs(0) - 1) & (ih == pl.num_programs(1) - 1))
    def _():
        dk_ref[...] = dk_s[...]
        dv_ref[...] = dv_s[...]


def attend(pos, first, q, do, ks, vs, cos, sin, sums=None):
    rows, width = q.shape
    hp = 4
    sk = sum(k.shape[0] for k in ks)
    tile = pl.BlockSpec((BLOCK, hp * HEAD), lambda i, h, _: (i, h))
    whole = lambda a: pl.BlockSpec(a.shape, lambda i, h, _: (0, 0))
    keys = _sds((sk, HEAD), F32)
    given = (*ks, *vs, cos, sin, *(sums or ()))
    wide = hp * BLOCK
    vmem = lambda *shape, t=F32: pltpu.VMEM(shape, t)
    return _call(
        functools.partial(_attend, first=first, hp=hp, added=sums is not None), (rows // BLOCK, width // (hp * HEAD)),
        [tile, tile, *map(whole, given)],
        [pl.BlockSpec((hp * HEAD, BLOCK), lambda i, h, _: (h, i)), tile, whole(keys), whole(keys)],
        [_sds((width, rows)), _sds((rows, width)), keys, keys],
        [vmem(sk, HEAD, t=BF16), vmem(sk, HEAD, t=BF16), vmem(HEAD, sk, t=BF16), vmem(HEAD, sk, t=BF16), vmem(sk, wide), vmem(sk, wide, t=BF16),
         vmem(HEAD, wide), vmem(HEAD, wide), vmem(sk, HEAD), vmem(sk, HEAD)],
        2 * 6 * 2 * rows * sk * width * 0.6, 8 * rows * width, (pos, q, do, *given))


def _back(dq_ref, dk_ref, dv_ref, c_ref, s_ref, wq_ref, wk_ref, wv_ref, sum_ref, g_ref,
          g_s, dk_s, dv_s, c_s, s_s, w_s, keep_s, send_s, came_s, sum_s, sem, w_sem, out_sem, g_sem, send_sem, recv_sem, *, chunk):
    rows, width = dq_ref.shape
    half = rows // 2
    steps, wide = w_s.shape[:2]
    pairs = [(dq_ref, g_s.at[:, pl.ds(0, width)])]
    for ref, s in ((dk_ref, dk_s), (dv_ref, dv_s), (c_ref, c_s), (s_ref, s_s)):
        pairs += _places(chunk, ref, s)
    ready = _copies(pairs, sem)
    lines = lambda ref, i: ref.at[pl.ds(pl.multiple_of(i * wide, wide), wide), :]
    parts = ((wq_ref, 0, width), (wk_ref, width, HEAD), (wv_ref, width + HEAD, HEAD))
    tile = lambda i: [pltpu.make_async_copy(lines(w, i), w_s.at[i, :, pl.ds(at, size)], w_sem.at[i, m]) for m, (w, at, size) in enumerate(parts)]
    for copy in ready + tile(0) + tile(1):
        copy.start()
    _meet()
    for copy in ready:
        copy.wait()
    for copy in tile(2):
        copy.start()
    g = (dk_s[...] * HEAD**-0.5).astype(BF16).astype(F32)
    g_s[:, width : width + HEAD] = (g * c_s[...] - pltpu.roll(g, HEAD // 2, 1) * s_s[...]).astype(BF16)
    g_s[:, width + HEAD :] = dv_s[...].astype(BF16)
    g_out = pltpu.make_async_copy(g_s, g_ref, g_sem.at[0])
    g_out.start()
    swap = lambda i: _to_sibling(send_s.at[i], came_s.at[i], send_sem.at[i], recv_sem.at[i])
    out = lambda i: pltpu.make_async_copy(sum_s.at[i], sum_ref.at[:, pl.ds(pl.multiple_of(i * wide, wide), wide)], out_sem.at[i])

    def add(i):
        swap(i).wait_recv()
        sum_s[i] = (keep_s[i] + came_s[i].astype(F32)).astype(sum_s.dtype)
        out(i).start()

    def step(i, _):
        for copy in tile(i):
            copy.wait()

        @pl.when(i + 3 < steps)
        def _():
            for copy in tile(i + 3):
                copy.start()

        t = _dot(g_s[...], w_s[i], 1, 1)
        keep_s[i] = t[:half]
        send_s[i] = t[half:].astype(BF16)
        swap(i).start()

        @pl.when(i >= LAG)
        def _():
            add(i - LAG)

    lax.fori_loop(0, steps, step, None)
    lax.fori_loop(steps - LAG, steps, lambda i, _: add(i), None)

    def done(i, _):
        swap(i).wait_send()
        out(i).wait()

    lax.fori_loop(0, steps, done, None)
    g_out.wait()


def back(chunk, dtype, dq, dk, dv, wq, wk, wv, cos, sin, meeting):
    d, width = wq.shape
    rows = dq.shape[0]
    wide = 512
    steps = d // wide
    full = width + 2 * HEAD
    vmem, dma = pltpu.VMEM, pltpu.SemaphoreType.DMA
    line = vmem((rows, HEAD), F32)
    tiles = lambda t: vmem((steps, rows // 2, wide), t)
    return _all(
        functools.partial(_back, chunk=chunk), [_sds((rows // 2, d), dtype), _sds((rows, full))],
        [vmem((rows, full), BF16), line, line, line, line, vmem((steps, wide, full), BF16), tiles(F32), tiles(BF16), tiles(BF16), tiles(dtype),
         dma((1 + 4 * rows // HALF,)), dma((steps, 3)), dma((steps,)), dma((1,)), dma((steps,)), dma((steps,))],
        2 * rows * d * full, 2 * (d * full + rows * (2 * d + width)), dq, dk, dv, cos, sin, wq, wk, wv, meeting=meeting)


def _weights(_, *refs, n, ng):
    pieces, gs, (wq_ref, wk_ref, wv_ref, g_s, sem) = refs[:n], refs[n : n + ng], refs[n + ng :]

    @pl.when(pl.program_id(0) == 0)
    def _():
        at, pairs = 0, []
        for g in gs:
            pairs.append((g, g_s.at[pl.ds(at, g.shape[0]), :]))
            at += g.shape[0]
        _fetch(pairs, sem)

    a = jnp.concatenate([p[...] for p in pieces], axis=0)
    t = _dot(a, g_s[...], 0, 0).astype(BF16)
    width = wq_ref.shape[1]
    wq_ref[...] = t[:, :width]
    wk_ref[...] = t[:, width : width + HEAD]
    wv_ref[...] = t[:, width + HEAD :]


def weights(pos, pieces, gs):
    d = pieces[0].shape[1]
    full = gs[0].shape[1]
    width = full - 2 * HEAD
    rows = sum(g.shape[0] for g in gs)
    wide = 512
    tile = lambda n: pl.BlockSpec((wide, n), lambda i, _: (i, 0))
    return _call(
        functools.partial(_weights, n=len(pieces), ng=len(gs)), (d // wide,),
        [pl.BlockSpec((p.shape[0], wide), lambda i, _: (0, i)) for p in pieces] + [ANY] * len(gs),
        [tile(width), tile(HEAD), tile(HEAD)], [_sds((d, width)), _sds((d, HEAD)), _sds((d, HEAD))],
        [pltpu.VMEM((rows, full), BF16), pltpu.SemaphoreType.DMA((len(gs),))],
        2 * rows * d * full, 2 * (rows * (d + full) + d * full), (pos, *pieces, *gs))


def _out_weights(_, *refs, n, ns):
    pieces, seen, (o_ref, s_s, sem) = refs[:n], refs[n : n + ns], refs[n + ns :]

    @pl.when(pl.program_id(0) == 0)
    def _():
        at, pairs = 0, []
        for s in seen:
            pairs.append((s, s_s.at[:, pl.ds(at, s.shape[1])]))
            at += s.shape[1]
        _fetch(pairs, sem)

    o_ref[...] = _dot(s_s[...], jnp.concatenate([p[...] for p in pieces], axis=0), 1, 0).astype(BF16)


def out_weights(pos, pieces, seen):
    d = pieces[0].shape[1]
    width = seen[0].shape[0]
    rows = sum(s.shape[1] for s in seen)
    wide = 512
    return _call(
        functools.partial(_out_weights, n=len(pieces), ns=len(seen)), (d // wide,),
        [pl.BlockSpec((p.shape[0], wide), lambda i, _: (0, i)) for p in pieces] + [ANY] * len(seen),
        pl.BlockSpec((width, wide), lambda i, _: (0, i)), _sds((width, d)),
        [pltpu.VMEM((width, rows), BF16), pltpu.SemaphoreType.DMA((len(seen),))],
        2 * rows * d * width, 2 * (rows * (d + width) + d * width), (pos, *pieces, *seen))


def _finish(own_ref, rh_ref, oh_ref, rl_ref, ol_ref, x_ref, dy_ref, gain_ref, dx_ref, dg_ref,
            own_s, far_s, x_s, dy_s, gain_s, dx_s, dg_s, sem, out_sem):
    n, rows = x_s.shape[:2]
    part = lambda ref, i: ref.at[pl.ds(pl.multiple_of(i * rows, rows), rows), :]
    upper = _here()[1] == 1
    half = n // 2
    far = lambda late, low: (ol_ref if late else rl_ref) if low else (rh_ref if late else oh_ref)
    rest = ((own_ref, own_s), (x_ref, x_s), (dy_ref, dy_s))

    def get(i):
        for k, (ref, s) in enumerate(rest):
            pltpu.make_async_copy(part(ref, i), s.at[i], sem.at[i, k]).start()
        for low in (False, True):
            for late in (False, True):

                @pl.when((upper != low) & ((i >= half) == late))
                def _():
                    pltpu.make_async_copy(part(far(late, low), lax.rem(i, half)), far_s.at[i], sem.at[i, 3]).start()

    get_gain = pltpu.make_async_copy(gain_ref, gain_s, out_sem.at[n])
    get_gain.start()
    for i in range(AHEAD):
        get(jnp.int32(i))
    get_gain.wait()
    dg_s[...] = jnp.zeros_like(dg_s)

    def step(i, _):
        @pl.when(i + AHEAD < n)
        def _():
            get(i + AHEAD)

        for k, (ref, s) in enumerate(rest):
            pltpu.make_async_copy(part(ref, i), s.at[i], sem.at[i, k]).wait()
        pltpu.make_async_copy(part(rh_ref, 0), far_s.at[i], sem.at[i, 3]).wait()
        da = own_s[i] + far_s[i].astype(F32)
        x = x_s[i].astype(F32)
        scale = lax.rsqrt(jnp.mean(x * x, -1, keepdims=True) + 1e-6)
        h = x * scale
        dg_s[...] += jnp.sum(da * h, axis=0, keepdims=True)
        dh = da * gain_s[...].astype(F32)
        dx = scale * (dh - h * jnp.mean(dh * h, -1, keepdims=True))
        dx_s[i] = (dy_s[i].astype(F32) + dx).astype(BF16)
        pltpu.make_async_copy(dx_s.at[i], part(dx_ref, i), out_sem.at[i]).start()

    lax.fori_loop(0, n, step, None)
    last = pltpu.make_async_copy(dg_s, dg_ref, out_sem.at[n])
    last.start()
    for copy in _copies([(dx_s.at[i], part(dx_ref, i)) for i in range(n)], out_sem) + [last]:
        copy.wait()


def finish(own, rh, oh, rl, ol, x, dy, gain):
    rows, d = x.shape
    n = 8
    block = (n, rows // n, d)
    vmem, dma = pltpu.VMEM, pltpu.SemaphoreType.DMA
    return _all(
        _finish, [_sds((rows, d)), _sds((1, d), F32)],
        [vmem(block, F32), vmem(block, BF16), vmem(block, BF16), vmem(block, BF16), vmem((1, d), BF16), vmem(block, BF16),
         vmem((1, d), F32), dma((n, 4)), dma((n + 1,))],
        3 * 10**9, 12 * rows * d, own, rh, oh, rl, ol, x, dy, gain)


def tables(rows):
    half = HEAD // 2
    angle = jnp.arange(rows).astype(F32)[:, None] * THETA ** (-jnp.arange(half, dtype=F32) / half)
    cos, sin = jnp.cos(angle), jnp.sin(angle)
    return jnp.concatenate([cos, cos], -1), jnp.concatenate([-sin, sin], -1)


SIBLING = [(0, 1), (1, 0), (2, 3), (3, 2)]
PARTNER = [(0, 2), (2, 0), (1, 3), (3, 1)]
ACROSS = [(0, 3), (3, 0), (1, 2), (2, 1)]


def solution(mesh):
    def move(t, pairs):
        return lax.ppermute(t, "tp", pairs)

    def work(x, dy, gain, wq, wk, wv, wo):
        me = lax.axis_index("tp")
        core = lax.rem(me, 2)
        upper = core == 1
        gain = gain[None]
        start = lambda block, half: block * BLOCK + half * HALF
        sib, far = me + 1 - 2 * core, 2 * (1 - lax.div(me, 2))
        pos = jnp.stack([start(me, 0), start(me, 1), start(sib, 0), start(sib, 1), start(far + 1, core), start(far + 1, 1 - core),
                         start(far, core), start(far, 1 - core)]).astype(jnp.int32)
        cos, sin = tables(4 * BLOCK)

        def after(t, *others):
            return lax.optimization_barrier((t, *others))[0]

        def halves(own, sib):
            return jnp.where(upper, own[HALF:], sib[:HALF]), jnp.where(upper, sib[HALF:], own[:HALF])

        e = move(dy, SIBLING)
        a = norm(x, gain)
        b = move(a, SIBLING)
        a_high, a_low = halves(a, b)
        ah = move(a_high, PARTNER)
        al = move(a_low, PARTNER)
        d_high, d_low = halves(*after((dy, e), a_low))
        dh = move(d_high, PARTNER)
        dl = move(d_low, PARTNER)

        w = (wq, wk, wv)
        turns = (cos, sin)
        q_n, k_n, v_n = project("near", (a, after(b, d_high, d_low)), *w, *turns)
        do_n = into((dy, after(e, q_n)), wo)
        ah = after(ah, do_n)
        q_h, k_h, v_h, ah2 = project("high", (ah,), *w, *turns, meeting=0)
        al = after(al, q_h)
        q_l, k_l, v_l, al2 = project("low", (al,), *w, *turns, meeting=1)
        keys = ((k_n, k_h, k_l), (v_n, v_h, v_l), *turns)
        seen_n, dq_n, dk, dv = attend(pos, 0, q_n, do_n, *keys)
        dh = after(dh, dq_n)
        do_h, dh2 = into((dh,), wo, meeting=2)
        seen_h, dq_h, dk, dv = attend(pos, 4, q_h, do_h, *keys, sums=(dk, dv))
        sum_h, g_h = back("high", BF16, dq_h, dk, dv, *w, *turns, meeting=3)
        r_h = move(sum_h, PARTNER)
        dl = after(dl, sum_h)
        do_l, dl2 = into((dl,), wo, meeting=4)
        seen_l, dq_l, dk, dv = attend(pos, 6, q_l, do_l, *keys, sums=(dk, dv))
        sum_l, g_l = back("low", BF16, dq_l, dk, dv, *w, *turns, meeting=5)
        r_l = move(sum_l, PARTNER)
        own, g_n = back("near", F32, after(dq_n, sum_l), dk, dv, *w, *turns, meeting=6)
        by_wo = out_weights(pos, (dy, e, dh, dh2, dl, dl2), (seen_n, seen_h, after(seen_l, own)))
        r_h = after(r_h, by_wo)
        o_h = move(r_h, SIBLING)
        r_l = after(r_l, by_wo)
        o_l = move(r_l, SIBLING)
        by_x, part = finish(own, r_h, o_h, r_l, o_l, x, dy, gain)
        by_wq, by_wk, by_wv = weights(pos, (a, b, ah, ah2, al, al2), (after(g_n, part), g_h, g_l))
        by_gain = (part + move(part, SIBLING)) + (move(part, PARTNER) + move(part, ACROSS))
        return by_x, by_gain, by_wq, by_wk, by_wv, by_wo

    tokens, columns = P(("dp", "tp"), None), P(None, "tp")
    return jax.shard_map(
        work,
        mesh=mesh,
        in_specs=(tokens, tokens, P(None), columns, columns, columns, P("tp", None)),
        out_specs=(tokens, P("dp", None), P("dp", "tp"), P("dp", "tp"), P("dp", "tp"), P(("dp", "tp"), None)),
        check_vma=False,
    )
```

```python
import functools

import jax
import jax.numpy as jnp
from jax import lax
from jax.experimental import pallas as pl
from jax.experimental.pallas import tpu as pltpu
from jax.sharding import PartitionSpec as P


HEAD = 128
THETA = 10000
HIDDEN = -2e30
LOG2E = 1.4426950408889634
VMEM = 63 * 2**20
HALF = 128
BLOCK = 256
LAG = 3
AHEAD = 2
F32, BF16 = jnp.float32, jnp.bfloat16
ANY = pl.BlockSpec(memory_space=pl.ANY)


def _dot(a, b, ca, cb):
    return lax.dot_general(a, b, (((ca,), (cb,)), ((), ())), preferred_element_type=F32)


def _call(kernel, grid, in_specs, out_specs, out_shape, scratch, flops, moved, args, scalars=1):
    return pl.pallas_call(
        kernel,
        grid_spec=pltpu.PrefetchScalarGridSpec(
            num_scalar_prefetch=scalars, grid=grid, in_specs=in_specs, out_specs=out_specs, scratch_shapes=scratch),
        out_shape=out_shape,
        compiler_params=pltpu.CompilerParams(dimension_semantics=("arbitrary",) * len(grid), vmem_limit_bytes=VMEM),
        cost_estimate=pl.CostEstimate(flops=int(flops), bytes_accessed=int(moved), transcendentals=0),
    )(*args)


def _fetch(pairs, sem):
    copies = [pltpu.make_async_copy(src, dst, sem.at[n]) for n, (src, dst) in enumerate(pairs)]
    for copy in copies:
        copy.start()
    for copy in copies:
        copy.wait()


def _here():
    me = lax.axis_index("tp")
    core = lax.rem(me, 2)
    return me, core, me + 1 - 2 * core, 2 * (1 - lax.div(me, 2))


def _starts(chunk):
    me, core, sib, far = _here()
    at = lambda block, half: block * BLOCK + half * HALF
    if chunk == "near":
        return [at(me, 0), at(me, 1), at(sib, 0), at(sib, 1)]
    block = far + (chunk == "high")
    return [at(block, core), at(block, 1 - core)]


def _meet():
    barrier = pltpu.get_barrier_semaphore()
    pl.semaphore_signal(barrier, inc=1, device_id={"tp": _here()[2]}, device_id_type=pl.DeviceIdType.MESH)
    pl.semaphore_wait(barrier, 1)


def _to_sibling(src, dst, send_sem, recv_sem):
    return pltpu.make_async_remote_copy(src_ref=src, dst_ref=dst, send_sem=send_sem, recv_sem=recv_sem, device_id={"tp": _here()[2]},
                                        device_id_type=pl.DeviceIdType.MESH)


def _sds(shape, dtype=BF16):
    return jax.ShapeDtypeStruct(shape, dtype)


def _table(ref, pos_ref, first, n):
    return jnp.concatenate([ref[pl.ds(pl.multiple_of(pos_ref[first + m], HALF), HALF), :] for m in range(n)], axis=0)


def _head(x_ref, dy_ref, gain_ref, a_ref, b_ref, ah_ref, al_ref, e_ref, dh_ref, dl_ref,
          x_s, a_s, d_s, gain_s, sem, out_sem, part_sem, send_sem, recv_sem, far_send, far_recv, d_sem, d_send, d_recv):
    n, rows = x_s.shape[:2]
    half = n // 2
    core = _here()[1]
    part = lambda ref, i: ref.at[pl.ds(pl.multiple_of(i * rows, rows), rows), :]
    halves = lambda ref, i: ref.at[pl.ds(pl.multiple_of(i * HALF, HALF), HALF), :]
    get = lambda i: pltpu.make_async_copy(part(x_ref, i), x_s.at[i], sem.at[i])
    put = lambda i: pltpu.make_async_copy(a_s.at[i], part(a_ref, i), out_sem.at[i])
    give = lambda i: _to_sibling(a_s.at[i], part(b_ref, i), send_sem.at[i], recv_sem.at[i])
    keep = lambda to, i: pltpu.make_async_copy(a_s.at[i], part(to, lax.rem(i, half)), part_sem.at[i])
    hand = lambda to, i: _to_sibling(a_s.at[i], part(to, lax.rem(i, half)), far_send.at[i], far_recv.at[i])
    gain_copy = pltpu.make_async_copy(gain_ref, gain_s, d_sem.at[2])
    gain_copy.start()
    for i in range(AHEAD + 1):
        get(i).start()
    d_get = pltpu.make_async_copy(halves(dy_ref, core), d_s, d_sem.at[0])
    d_put = lambda to: pltpu.make_async_copy(d_s, to, d_sem.at[1])
    d_give = _to_sibling(dy_ref, e_ref, d_send.at[0], d_recv.at[0])
    d_hand = lambda to: _to_sibling(halves(dy_ref, 1 - core), to, d_send.at[1], d_recv.at[1])
    ways = ((0, al_ref, dl_ref, ah_ref, dh_ref), (1, ah_ref, dh_ref, al_ref, dl_ref))
    _meet()
    gain_copy.wait()

    def step(i, _):
        get(i).wait()

        @pl.when(i + AHEAD + 1 < n)
        def _():
            get(i + AHEAD + 1).start()

        x = x_s[i].astype(F32)
        scale = lax.rsqrt(jnp.mean(x * x, -1, keepdims=True) + 1e-6)
        a_s[i] = (x * scale * gain_s[...].astype(F32)).astype(BF16)
        put(i).start()
        give(i).start()
        for which, to, _, _, _ in ways:

            @pl.when((core == which) & (lax.div(i, half) == which))
            def _():
                keep(to, i).start()

            @pl.when((core == which) & (lax.div(i, half) != which))
            def _():
                hand(to, i).start()

    lax.fori_loop(0, n, step, None)
    d_get.start()
    d_give.start()
    for which, _, to, _, _ in ways:

        @pl.when(core == which)
        def _():
            d_hand(to).start()

    d_get.wait()
    for which, _, to, _, _ in ways:

        @pl.when(core == which)
        def _():
            d_put(to).start()

    def done(i, _):
        put(i).wait()
        give(i).wait()
        for which, to, _, other, _ in ways:

            @pl.when((core == which) & (lax.div(i, half) == which))
            def _():
                keep(to, i).wait()
                hand(other, i).wait_recv()

            @pl.when((core == which) & (lax.div(i, half) != which))
            def _():
                hand(to, i).wait_send()

    lax.fori_loop(0, n, done, None)
    d_give.wait()
    for which, _, to, _, other in ways:

        @pl.when(core == which)
        def _():
            d_put(to).wait()
            d_hand(to).wait_send()
            d_hand(other).wait_recv()


def head(x, dy, gain, meeting):
    rows, d = x.shape
    n = 8
    block = (n, rows // n, d)
    vmem, dma = pltpu.VMEM, pltpu.SemaphoreType.DMA
    full, half = _sds((rows, d)), _sds((rows // 2, d))
    return _all(
        _head, [full, full, half, half, full, half, half],
        [vmem(block, BF16), vmem(block, BF16), vmem((HALF, d), BF16), vmem((1, d), BF16), *[dma((n,))] * 7, dma((3,)), dma((2,)), dma((2,))],
        10**9, 24 * rows * d, x, dy, gain, meeting=meeting)


def _copies(pairs, sem, base=0):
    return [pltpu.make_async_copy(src, dst, sem.at[base + n]) for n, (src, dst) in enumerate(pairs)]


def _all(kernel, out_shape, scratch, flops, moved, *args, meeting=None):
    many = isinstance(out_shape, list)
    extra = {} if meeting is None else dict(collective_id=meeting, has_side_effects=True)
    return pl.pallas_call(
        kernel,
        in_specs=[ANY] * len(args),
        out_specs=[ANY] * len(out_shape) if many else ANY,
        out_shape=out_shape,
        scratch_shapes=scratch,
        compiler_params=pltpu.CompilerParams(vmem_limit_bytes=VMEM, **extra),
        cost_estimate=pl.CostEstimate(flops=int(flops), bytes_accessed=int(moved), transcendentals=0),
    )(*args)


def _pieces(pieces, a_s):
    at, pairs = 0, []
    for p in pieces:
        pairs.append((p, a_s.at[pl.ds(at, p.shape[0]), :]))
        at += p.shape[0]
    return pairs


def _places(chunk, ref, s):
    return [(ref.at[pl.ds(pl.multiple_of(at, HALF), HALF), :], s.at[pl.ds(m * HALF, HALF), :]) for m, at in enumerate(_starts(chunk))]


def _forward(piece, a_s, f_ref, sems):
    rows = piece.shape[0]
    under = a_s.at[pl.ds(rows, rows), :]
    return _to_sibling(piece, under, sems.at[0], sems.at[1]), pltpu.make_async_copy(under, f_ref, sems.at[2])


def _project(*refs, n, chunk):
    pieces, (wq_ref, wk_ref, wv_ref, c_ref, s_ref, q_ref, k_ref, v_ref), refs = refs[:n], refs[n : n + 8], refs[n + 8 :]
    f_ref, refs = (None, refs) if chunk == "near" else (refs[0], refs[1:])
    a_s, w_s, c_s, s_s, q_s, k_s, v_s, sem, w_sem, out_sem, kv_sem, f_sem = refs
    steps, wide = w_s.shape[0] - 1, w_s.shape[2]
    pairs = _pieces(pieces, a_s) + _places(chunk, c_ref, c_s) + _places(chunk, s_ref, s_s)
    ready = _copies(pairs, sem)
    columns = lambda ref, i: ref.at[:, pl.ds(pl.multiple_of(i * wide, wide), wide)]
    tile = lambda i: pltpu.make_async_copy(columns(wq_ref, i), w_s.at[i], w_sem.at[i])
    kv = [pltpu.make_async_copy(w, w_s.at[steps, :, pl.ds(m * HEAD, HEAD)], kv_sem.at[m]) for m, w in enumerate((wk_ref, wv_ref))]
    for copy in ready + [tile(0)]:
        copy.start()
    if f_ref is not None:
        _meet()
        forward, keep = _forward(pieces[0], a_s, f_ref, f_sem)
        forward.start()
    for copy in ready:
        copy.wait()
    for i in range(1, AHEAD):
        tile(i).start()
    if f_ref is not None:
        forward.wait()
        keep.start()

    def turn(t):
        t = t.astype(BF16).astype(F32)
        return (t * c_s[...] + pltpu.roll(t, HEAD // 2, 1) * s_s[...]).astype(BF16)

    out = lambda i, slot: pltpu.make_async_copy(q_s.at[slot], columns(q_ref, i), out_sem.at[slot])

    def step(i, _):
        slot = lax.rem(i, 2)
        tile(i).wait()

        @pl.when(i + AHEAD < steps)
        def _():
            tile(i + AHEAD).start()

        @pl.when(i + AHEAD == steps)
        def _():
            for copy in kv:
                copy.start()

        t = _dot(a_s[...], w_s[i], 1, 0)

        @pl.when(i >= 2)
        def _():
            out(i - 2, slot).wait()

        for m in range(wide // HEAD):
            q_s[slot, :, m * HEAD : (m + 1) * HEAD] = turn(t[:, m * HEAD : (m + 1) * HEAD])
        out(i, slot).start()

    lax.fori_loop(0, steps, step, None)
    for copy in kv:
        copy.wait()
    t = _dot(a_s[...], w_s[steps], 1, 0)
    k_s[...] = turn(t[:, :HEAD])
    v_s[...] = t[:, HEAD:].astype(BF16)
    last = _copies([(k_s, k_ref), (v_s, v_ref)], kv_sem)
    for copy in last:
        copy.start()
    for copy in last + [out(steps - 2 + m, (steps + m) % 2) for m in range(2)]:
        copy.wait()
    if f_ref is not None:
        keep.wait()


def project(chunk, pieces, wq, wk, wv, cos, sin, meeting=None):
    d, width = wq.shape
    n, rows = len(pieces), sum(p.shape[0] for p in pieces)
    more = [] if meeting is None else [_sds((rows, d))]
    rows *= 1 + len(more)
    wide = 256
    steps = width // wide
    vmem, dma = pltpu.VMEM, pltpu.SemaphoreType.DMA
    return _all(
        functools.partial(_project, n=n, chunk=chunk),
        [_sds((rows, width)), _sds((rows, HEAD)), _sds((rows, HEAD)), *more],
        [vmem((rows, d), BF16), vmem((steps + 1, d, wide), BF16), vmem((rows, HEAD), F32), vmem((rows, HEAD), F32), vmem((2, rows, wide), BF16),
         vmem((rows, HEAD), BF16), vmem((rows, HEAD), BF16), dma((n + 2 * rows // HALF,)), dma((steps,)), dma((2,)), dma((2,)), dma((3,))],
        2 * rows * d * (width + 2 * HEAD), 2 * (d * (width + 256) + rows * (d + width)), *pieces, wq, wk, wv, cos, sin, meeting=meeting)


def _into(*refs, n, forwards):
    pieces, w_ref, o_ref, refs = refs[:n], refs[n], refs[n + 1], refs[n + 2 :]
    f_ref, refs = (refs[0], refs[1:]) if forwards else (None, refs)
    a_s, w_s, o_s, sem, w_sem, out_sem, f_sem = refs
    steps, wide = w_s.shape[:2]
    ready = _copies(_pieces(pieces, a_s), sem)
    tile = lambda i: pltpu.make_async_copy(w_ref.at[pl.ds(pl.multiple_of(i * wide, wide), wide), :], w_s.at[i], w_sem.at[i])
    for copy in ready + [tile(0)]:
        copy.start()
    if forwards:
        _meet()
        forward, keep = _forward(pieces[0], a_s, f_ref, f_sem)
        forward.start()
    for copy in ready:
        copy.wait()
    for i in range(1, AHEAD):
        tile(i).start()
    if forwards:
        forward.wait()
        keep.start()
    out = lambda i, slot: pltpu.make_async_copy(o_s.at[slot], o_ref.at[:, pl.ds(pl.multiple_of(i * wide, wide), wide)], out_sem.at[slot])

    def step(i, _):
        slot = lax.rem(i, 2)
        tile(i).wait()

        @pl.when(i + AHEAD < steps)
        def _():
            tile(i + AHEAD).start()

        t = _dot(a_s[...], w_s[i], 1, 1).astype(BF16)

        @pl.when(i >= 2)
        def _():
            out(i - 2, slot).wait()

        o_s[slot] = t
        out(i, slot).start()

    lax.fori_loop(0, steps, step, None)
    for m in range(2):
        out(steps - 2 + m, (steps + m) % 2).wait()
    if forwards:
        keep.wait()


def into(pieces, wo, meeting=None):
    width, d = wo.shape
    n, rows = len(pieces), sum(p.shape[0] for p in pieces)
    more = [] if meeting is None else [_sds((rows, d))]
    rows *= 1 + len(more)
    result = _sds((rows, width))
    wide = 256
    steps = width // wide
    vmem, dma = pltpu.VMEM, pltpu.SemaphoreType.DMA
    return _all(
        functools.partial(_into, n=n, forwards=bool(more)), [result, *more] if more else result,
        [vmem((rows, d), BF16), vmem((steps, wide, d), BF16), vmem((2, rows, wide), BF16), dma((n,)), dma((steps,)), dma((2,)), dma((3,))],
        2 * rows * d * width, 2 * (d * width + rows * (d + width)), *pieces, wo, meeting=meeting)


def _attend(pos_ref, q_ref, do_ref, kl_ref, kh_ref, kr_ref, vl_ref, vh_ref, vr_ref, c_ref, s_ref, *rest, first, hp, added):
    dk_in, dv_in = rest[:2] if added else (None, None)
    seen_ref, dq_ref, dk_ref, dv_ref, k_s, v_s, kt_s, vt_s, s_s, dp_s, o_s, dq_s, dk_s, dv_s = rest[-14:]
    iq, ih = pl.program_id(0), pl.program_id(1)
    wide = hp * BLOCK
    e = HEAD**-0.5 * LOG2E

    @pl.when((iq == 0) & (ih == 0))
    def _():
        at = 0
        for kc, vc in ((kl_ref, vl_ref), (kh_ref, vh_ref), (kr_ref, vr_ref)):
            for m in range(kc.shape[0] // HALF):
                here = pl.ds(pl.multiple_of(pos_ref[at], HALF), HALF)
                k_s[here, :] = kc[m * HALF : (m + 1) * HALF, :]
                v_s[here, :] = vc[m * HALF : (m + 1) * HALF, :]
                at += 1
        kt_s[...] = k_s[...].T
        vt_s[...] = v_s[...].T
        dk_s[...] = dk_in[...] if added else jnp.zeros_like(dk_s)
        dv_s[...] = dv_in[...] if added else jnp.zeros_like(dv_s)

    place = pos_ref[first + 2 * iq]
    own = lax.div(place, BLOCK)
    turned = lax.rem(place, BLOCK)
    q2 = jnp.concatenate([q_ref[:, m * HEAD : (m + 1) * HEAD] for m in range(hp)], axis=0)
    do2 = jnp.concatenate([do_ref[:, m * HEAD : (m + 1) * HEAD] for m in range(hp)], axis=0)

    def rows(j):
        return pl.ds(pl.multiple_of(j * BLOCK, BLOCK), BLOCK)

    here = rows(own)
    s = _dot(k_s[here, :], q2, 1, 1)
    query = lax.rem(lax.broadcasted_iota(jnp.int32, s.shape, 1) + turned, BLOCK)
    s = jnp.where(lax.broadcasted_iota(jnp.int32, s.shape, 0) <= query, s, HIDDEN)
    s_s[here, :] = s

    def scores(j, top):
        s = _dot(k_s[rows(j), :], q2, 1, 1)
        s_s[rows(j), :] = s
        return jnp.maximum(top, s.max(axis=0, keepdims=True))

    top = lax.fori_loop(0, own, scores, s.max(axis=0, keepdims=True))
    o_s[...] = jnp.zeros_like(o_s)
    dq_s[...] = jnp.zeros_like(dq_s)

    def weigh(j, sums):
        total, delta = sums
        dp = _dot(v_s[rows(j), :], do2, 1, 1)
        dp_s[rows(j), :] = dp
        p = jnp.exp2((s_s[rows(j), :] - top) * e)
        s_s[rows(j), :] = p
        o_s[...] += _dot(vt_s[:, rows(j)], p.astype(BF16), 1, 0)
        return total + p.sum(axis=0, keepdims=True), delta + (p * dp).sum(axis=0, keepdims=True)

    zero = jnp.zeros((1, wide), F32)
    total, delta = lax.fori_loop(0, own + 1, weigh, (zero, zero))
    inv = 1 / total
    delta = delta * inv

    def grads(j, _):
        p = s_s[rows(j), :] * inv
        ds = (p * (dp_s[rows(j), :] - delta)).astype(BF16)
        dv_s[rows(j), :] += _dot(p.astype(BF16), do2, 1, 0)
        dk_s[rows(j), :] += _dot(ds, q2, 1, 0)
        dq_s[...] += _dot(kt_s[:, rows(j)], ds, 1, 0)

    lax.fori_loop(0, own + 1, grads, None)
    cos, sin = _table(c_ref, pos_ref, first + 2 * iq, 2), _table(s_ref, pos_ref, first + 2 * iq, 2)
    o = (o_s[...] * inv).astype(BF16)
    for m in range(hp):
        seen_ref[m * HEAD : (m + 1) * HEAD, :] = o[:, m * BLOCK : (m + 1) * BLOCK]
        g = (dq_s[:, m * BLOCK : (m + 1) * BLOCK] * HEAD**-0.5).T.astype(BF16).astype(F32)
        dq_ref[:, m * HEAD : (m + 1) * HEAD] = (g * cos - pltpu.roll(g, HEAD // 2, 1) * sin).astype(BF16)

    @pl.when((iq == pl.num_programs(0) - 1) & (ih == pl.num_programs(1) - 1))
    def _():
        dk_ref[...] = dk_s[...]
        dv_ref[...] = dv_s[...]


def attend(pos, first, q, do, ks, vs, cos, sin, sums=None):
    rows, width = q.shape
    hp = 4
    sk = sum(k.shape[0] for k in ks)
    tile = pl.BlockSpec((BLOCK, hp * HEAD), lambda i, h, _: (i, h))
    whole = lambda a: pl.BlockSpec(a.shape, lambda i, h, _: (0, 0))
    keys = _sds((sk, HEAD), F32)
    given = (*ks, *vs, cos, sin, *(sums or ()))
    wide = hp * BLOCK
    vmem = lambda *shape, t=F32: pltpu.VMEM(shape, t)
    return _call(
        functools.partial(_attend, first=first, hp=hp, added=sums is not None), (rows // BLOCK, width // (hp * HEAD)),
        [tile, tile, *map(whole, given)],
        [pl.BlockSpec((hp * HEAD, BLOCK), lambda i, h, _: (h, i)), tile, whole(keys), whole(keys)],
        [_sds((width, rows)), _sds((rows, width)), keys, keys],
        [vmem(sk, HEAD, t=BF16), vmem(sk, HEAD, t=BF16), vmem(HEAD, sk, t=BF16), vmem(HEAD, sk, t=BF16), vmem(sk, wide), vmem(sk, wide),
         vmem(HEAD, wide), vmem(HEAD, wide), vmem(sk, HEAD), vmem(sk, HEAD)],
        2 * 6 * 2 * rows * sk * width * 0.6, 8 * rows * width, (pos, q, do, *given))


def _back(dq_ref, dk_ref, dv_ref, c_ref, s_ref, wq_ref, wk_ref, wv_ref, sum_ref, g_ref,
          g_s, dk_s, dv_s, c_s, s_s, w_s, keep_s, send_s, came_s, sum_s, sem, w_sem, out_sem, g_sem, send_sem, recv_sem, *, chunk):
    rows, width = dq_ref.shape
    half = rows // 2
    steps, wide = w_s.shape[:2]
    pairs = [(dq_ref, g_s.at[:, pl.ds(0, width)])]
    for ref, s in ((dk_ref, dk_s), (dv_ref, dv_s), (c_ref, c_s), (s_ref, s_s)):
        pairs += _places(chunk, ref, s)
    ready = _copies(pairs, sem)
    lines = lambda ref, i: ref.at[pl.ds(pl.multiple_of(i * wide, wide), wide), :]
    parts = ((wq_ref, 0, width), (wk_ref, width, HEAD), (wv_ref, width + HEAD, HEAD))
    tile = lambda i: [pltpu.make_async_copy(lines(w, i), w_s.at[i, :, pl.ds(at, size)], w_sem.at[i, m]) for m, (w, at, size) in enumerate(parts)]
    for copy in ready + tile(0) + tile(1):
        copy.start()
    _meet()
    for copy in ready:
        copy.wait()
    for copy in tile(2):
        copy.start()
    g = (dk_s[...] * HEAD**-0.5).astype(BF16).astype(F32)
    g_s[:, width : width + HEAD] = (g * c_s[...] - pltpu.roll(g, HEAD // 2, 1) * s_s[...]).astype(BF16)
    g_s[:, width + HEAD :] = dv_s[...].astype(BF16)
    g_out = pltpu.make_async_copy(g_s, g_ref, g_sem.at[0])
    g_out.start()
    swap = lambda i: _to_sibling(send_s.at[i], came_s.at[i], send_sem.at[i], recv_sem.at[i])
    out = lambda i: pltpu.make_async_copy(sum_s.at[i], sum_ref.at[:, pl.ds(pl.multiple_of(i * wide, wide), wide)], out_sem.at[i])

    def add(i):
        swap(i).wait_recv()
        sum_s[i] = (keep_s[i] + came_s[i].astype(F32)).astype(sum_s.dtype)
        out(i).start()

    def step(i, _):
        for copy in tile(i):
            copy.wait()

        @pl.when(i + 3 < steps)
        def _():
            for copy in tile(i + 3):
                copy.start()

        t = _dot(g_s[...], w_s[i], 1, 1)
        keep_s[i] = t[:half]
        send_s[i] = t[half:].astype(BF16)
        swap(i).start()

        @pl.when(i >= LAG)
        def _():
            add(i - LAG)

    lax.fori_loop(0, steps, step, None)
    lax.fori_loop(steps - LAG, steps, lambda i, _: add(i), None)

    def done(i, _):
        swap(i).wait_send()
        out(i).wait()

    lax.fori_loop(0, steps, done, None)
    g_out.wait()


def back(chunk, dtype, dq, dk, dv, wq, wk, wv, cos, sin, meeting):
    d, width = wq.shape
    rows = dq.shape[0]
    wide = 512
    steps = d // wide
    full = width + 2 * HEAD
    vmem, dma = pltpu.VMEM, pltpu.SemaphoreType.DMA
    line = vmem((rows, HEAD), F32)
    tiles = lambda t: vmem((steps, rows // 2, wide), t)
    return _all(
        functools.partial(_back, chunk=chunk), [_sds((rows // 2, d), dtype), _sds((rows, full))],
        [vmem((rows, full), BF16), line, line, line, line, vmem((steps, wide, full), BF16), tiles(F32), tiles(BF16), tiles(BF16), tiles(dtype),
         dma((1 + 4 * rows // HALF,)), dma((steps, 3)), dma((steps,)), dma((1,)), dma((steps,)), dma((steps,))],
        2 * rows * d * full, 2 * (d * full + rows * (2 * d + width)), dq, dk, dv, cos, sin, wq, wk, wv, meeting=meeting)


def _weights(_, *refs, n, ng):
    pieces, gs, (wq_ref, wk_ref, wv_ref, g_s, sem) = refs[:n], refs[n : n + ng], refs[n + ng :]

    @pl.when(pl.program_id(0) == 0)
    def _():
        at, pairs = 0, []
        for g in gs:
            pairs.append((g, g_s.at[pl.ds(at, g.shape[0]), :]))
            at += g.shape[0]
        _fetch(pairs, sem)

    a = jnp.concatenate([p[...] for p in pieces], axis=0)
    t = _dot(a, g_s[...], 0, 0).astype(BF16)
    width = wq_ref.shape[1]
    wq_ref[...] = t[:, :width]
    wk_ref[...] = t[:, width : width + HEAD]
    wv_ref[...] = t[:, width + HEAD :]


def weights(pos, pieces, gs):
    d = pieces[0].shape[1]
    full = gs[0].shape[1]
    width = full - 2 * HEAD
    rows = sum(g.shape[0] for g in gs)
    wide = 1024
    tile = lambda n: pl.BlockSpec((wide, n), lambda i, _: (i, 0))
    return _call(
        functools.partial(_weights, n=len(pieces), ng=len(gs)), (d // wide,),
        [pl.BlockSpec((p.shape[0], wide), lambda i, _: (0, i)) for p in pieces] + [ANY] * len(gs),
        [tile(width), tile(HEAD), tile(HEAD)], [_sds((d, width)), _sds((d, HEAD)), _sds((d, HEAD))],
        [pltpu.VMEM((rows, full), BF16), pltpu.SemaphoreType.DMA((len(gs),))],
        2 * rows * d * full, 2 * (rows * (d + full) + d * full), (pos, *pieces, *gs))


def _out_weights(_, *refs, n, ns):
    pieces, seen, (o_ref, s_s, sem) = refs[:n], refs[n : n + ns], refs[n + ns :]

    @pl.when(pl.program_id(0) == 0)
    def _():
        at, pairs = 0, []
        for s in seen:
            pairs.append((s, s_s.at[:, pl.ds(at, s.shape[1])]))
            at += s.shape[1]
        _fetch(pairs, sem)

    o_ref[...] = _dot(s_s[...], jnp.concatenate([p[...] for p in pieces], axis=0), 1, 0).astype(BF16)


def out_weights(pos, pieces, seen):
    d = pieces[0].shape[1]
    width = seen[0].shape[0]
    rows = sum(s.shape[1] for s in seen)
    wide = 1024
    return _call(
        functools.partial(_out_weights, n=len(pieces), ns=len(seen)), (d // wide,),
        [pl.BlockSpec((p.shape[0], wide), lambda i, _: (0, i)) for p in pieces] + [ANY] * len(seen),
        pl.BlockSpec((width, wide), lambda i, _: (0, i)), _sds((width, d)),
        [pltpu.VMEM((width, rows), BF16), pltpu.SemaphoreType.DMA((len(seen),))],
        2 * rows * d * width, 2 * (rows * (d + width) + d * width), (pos, *pieces, *seen))


def _finish(own_ref, rh_ref, rl_ref, x_ref, dy_ref, gain_ref, dx_ref, dg_ref,
            own_s, far_s, x_s, dy_s, gain_s, dx_s, dg_s, sem, out_sem, far_sem):
    n, rows = x_s.shape[:2]
    part = lambda ref, i: ref.at[pl.ds(pl.multiple_of(i * rows, rows), rows), :]
    core = _here()[1]
    half = n // 2
    there = far_s.at[pl.ds(pl.multiple_of(core * HALF, HALF), HALF), :]
    mine = lambda ref: pltpu.make_async_copy(ref, there, far_sem.at[0])
    hand = lambda ref: _to_sibling(ref, there, far_sem.at[1], far_sem.at[2])
    rest = ((own_ref, own_s), (x_ref, x_s), (dy_ref, dy_s))
    row = lambda i: lax.rem(i + core * half, n)

    def get(i):
        return [pltpu.make_async_copy(part(ref, row(i)), s.at[i], sem.at[i, k]) for k, (ref, s) in enumerate(rest)]

    get_gain = pltpu.make_async_copy(gain_ref, gain_s, out_sem.at[n])
    get_gain.start()
    _meet()
    for which, here, give in ((0, rl_ref, rh_ref), (1, rh_ref, rl_ref)):

        @pl.when(core == which)
        def _():
            mine(here).start()
            hand(give).start()

    for i in range(AHEAD):
        for copy in get(i):
            copy.start()
    get_gain.wait()
    mine(rh_ref).wait()
    dg_s[...] = jnp.zeros_like(dg_s)

    def step(i, _):
        @pl.when(i + AHEAD < n)
        def _():
            for copy in get(i + AHEAD):
                copy.start()

        @pl.when(i == half)
        def _():
            hand(rh_ref).wait_recv()

        for copy in get(i):
            copy.wait()
        far = far_s[pl.ds(pl.multiple_of(row(i) * rows, rows), rows), :]
        da = own_s[i] + far.astype(F32)
        x = x_s[i].astype(F32)
        scale = lax.rsqrt(jnp.mean(x * x, -1, keepdims=True) + 1e-6)
        h = x * scale
        dg_s[...] += jnp.sum(da * h, axis=0, keepdims=True)
        dh = da * gain_s[...].astype(F32)
        dx = scale * (dh - h * jnp.mean(dh * h, -1, keepdims=True))
        dx_s[i] = (dy_s[i].astype(F32) + dx).astype(BF16)
        pltpu.make_async_copy(dx_s.at[i], part(dx_ref, row(i)), out_sem.at[i]).start()

    lax.fori_loop(0, n, step, None)
    last = pltpu.make_async_copy(dg_s, dg_ref, out_sem.at[n])
    last.start()
    for copy in _copies([(dx_s.at[i], part(dx_ref, i)) for i in range(n)], out_sem) + [last]:
        copy.wait()
    hand(rh_ref).wait_send()


def finish(own, rh, rl, x, dy, gain, meeting):
    rows, d = x.shape
    n = 8
    block = (n, rows // n, d)
    vmem, dma = pltpu.VMEM, pltpu.SemaphoreType.DMA
    return _all(
        _finish, [_sds((rows, d)), _sds((1, d), F32)],
        [vmem(block, F32), vmem((rows, d), BF16), vmem(block, BF16), vmem(block, BF16), vmem((1, d), BF16), vmem(block, BF16),
         vmem((1, d), F32), dma((n, 3)), dma((n + 1,)), dma((3,))],
        3 * 10**9, 12 * rows * d, own, rh, rl, x, dy, gain, meeting=meeting)


def tables(rows):
    half = HEAD // 2
    angle = jnp.arange(rows).astype(F32)[:, None] * THETA ** (-jnp.arange(half, dtype=F32) / half)
    cos, sin = jnp.cos(angle), jnp.sin(angle)
    return jnp.concatenate([cos, cos], -1), jnp.concatenate([-sin, sin], -1)


SIBLING = [(0, 1), (1, 0), (2, 3), (3, 2)]
PARTNER = [(0, 2), (2, 0), (1, 3), (3, 1)]
ACROSS = [(0, 3), (3, 0), (1, 2), (2, 1)]


def solution(mesh):
    def move(t, pairs):
        return lax.ppermute(t, "tp", pairs)

    def work(x, dy, gain, wq, wk, wv, wo):
        me = lax.axis_index("tp")
        core = lax.rem(me, 2)
        gain = gain[None]
        start = lambda block, half: block * BLOCK + half * HALF
        sib, far = me + 1 - 2 * core, 2 * (1 - lax.div(me, 2))
        pos = jnp.stack([start(me, 0), start(me, 1), start(sib, 0), start(sib, 1), start(far + 1, core), start(far + 1, 1 - core),
                         start(far, core), start(far, 1 - core)]).astype(jnp.int32)
        cos, sin = tables(4 * BLOCK)

        def after(t, *others):
            return lax.optimization_barrier((t, *others))[0]

        a, b, a_high, a_low, e, d_high, d_low = head(x, dy, gain, 7)
        ah = move(a_high, PARTNER)
        al = move(a_low, PARTNER)
        dh = move(d_high, PARTNER)
        dl = move(d_low, PARTNER)

        w = (wq, wk, wv)
        turns = (cos, sin)
        q_n, k_n, v_n = project("near", (a, b), *w, *turns)
        do_n = into((dy, after(e, q_n)), wo)
        ah = after(ah, do_n)
        q_h, k_h, v_h, ah2 = project("high", (ah,), *w, *turns, meeting=0)
        al = after(al, q_h)
        q_l, k_l, v_l, al2 = project("low", (al,), *w, *turns, meeting=1)
        keys = ((k_n, k_h, k_l), (v_n, v_h, v_l), *turns)
        seen_n, dq_n, dk, dv = attend(pos, 0, q_n, do_n, *keys)
        dh = after(dh, dq_n)
        do_h, dh2 = into((dh,), wo, meeting=2)
        seen_h, dq_h, dk, dv = attend(pos, 4, q_h, do_h, *keys, sums=(dk, dv))
        sum_h, g_h = back("high", BF16, dq_h, dk, dv, *w, *turns, meeting=3)
        r_h = move(sum_h, PARTNER)
        dl = after(dl, sum_h)
        do_l, dl2 = into((dl,), wo, meeting=4)
        seen_l, dq_l, dk, dv = attend(pos, 6, q_l, do_l, *keys, sums=(dk, dv))
        sum_l, g_l = back("low", BF16, dq_l, dk, dv, *w, *turns, meeting=5)
        r_l = move(sum_l, PARTNER)
        own, g_n = back("near", F32, after(dq_n, sum_l), dk, dv, *w, *turns, meeting=6)
        by_wo = out_weights(pos, (dy, e, dh, dh2, dl, dl2), (seen_n, seen_h, after(seen_l, own)))
        by_x, part = finish(own, after(r_h, by_wo), after(r_l, by_wo), x, dy, gain, 8)
        by_wq, by_wk, by_wv = weights(pos, (a, b, ah, ah2, al, al2), (after(g_n, part), g_h, g_l))
        by_gain = (part + move(part, SIBLING)) + (move(part, PARTNER) + move(part, ACROSS))
        return by_x, by_gain, by_wq, by_wk, by_wv, by_wo

    tokens, columns = P(("dp", "tp"), None), P(None, "tp")
    return jax.shard_map(
        work,
        mesh=mesh,
        in_specs=(tokens, tokens, P(None), columns, columns, columns, P("tp", None)),
        out_specs=(tokens, P("dp", None), P("dp", "tp"), P("dp", "tp"), P("dp", "tp"), P(("dp", "tp"), None)),
        check_vma=False,
    )
```

```python
import functools

import jax
import jax.numpy as jnp
from jax import lax
from jax.experimental import pallas as pl
from jax.experimental.pallas import tpu as pltpu
from jax.sharding import PartitionSpec as P


HEAD = 128
THETA = 10000
HIDDEN = -2e30
LOG2E = 1.4426950408889634
VMEM = 63 * 2**20
HALF = 128
BLOCK = 256
LAG = 3
AHEAD = 2
F32, BF16 = jnp.float32, jnp.bfloat16
ANY = pl.BlockSpec(memory_space=pl.ANY)


def _dot(a, b, ca, cb):
    return lax.dot_general(a, b, (((ca,), (cb,)), ((), ())), preferred_element_type=F32)


def _call(kernel, grid, in_specs, out_specs, out_shape, scratch, flops, moved, args, scalars=1):
    return pl.pallas_call(
        kernel,
        grid_spec=pltpu.PrefetchScalarGridSpec(
            num_scalar_prefetch=scalars, grid=grid, in_specs=in_specs, out_specs=out_specs, scratch_shapes=scratch),
        out_shape=out_shape,
        compiler_params=pltpu.CompilerParams(dimension_semantics=("arbitrary",) * len(grid), vmem_limit_bytes=VMEM),
        cost_estimate=pl.CostEstimate(flops=int(flops), bytes_accessed=int(moved), transcendentals=0),
    )(*args)


def _fetch(pairs, sem):
    copies = [pltpu.make_async_copy(src, dst, sem.at[n]) for n, (src, dst) in enumerate(pairs)]
    for copy in copies:
        copy.start()
    for copy in copies:
        copy.wait()


def _here():
    me = lax.axis_index("tp")
    core = lax.rem(me, 2)
    return me, core, me + 1 - 2 * core, 2 * (1 - lax.div(me, 2))


def _starts(chunk):
    me, core, sib, far = _here()
    at = lambda block, half: block * BLOCK + half * HALF
    if chunk == "near":
        return [at(me, 0), at(me, 1), at(sib, 0), at(sib, 1)]
    block = far + (chunk == "high")
    return [at(block, core), at(block, 1 - core)]


def _meet():
    barrier = pltpu.get_barrier_semaphore()
    pl.semaphore_signal(barrier, inc=1, device_id={"tp": _here()[2]}, device_id_type=pl.DeviceIdType.MESH)
    pl.semaphore_wait(barrier, 1)


def _to_sibling(src, dst, send_sem, recv_sem):
    return pltpu.make_async_remote_copy(src_ref=src, dst_ref=dst, send_sem=send_sem, recv_sem=recv_sem, device_id={"tp": _here()[2]},
                                        device_id_type=pl.DeviceIdType.MESH)


def _sds(shape, dtype=BF16):
    return jax.ShapeDtypeStruct(shape, dtype)


def _table(ref, pos_ref, first, n):
    return jnp.concatenate([ref[pl.ds(pl.multiple_of(pos_ref[first + m], HALF), HALF), :] for m in range(n)], axis=0)


def _head(x_ref, gain_ref, a_ref, b_ref, ah_ref, al_ref, x_s, a_s, b_s, gain_s, sem, out_sem, part_sem, send_sem, recv_sem, b_sem, far_sem, gain_sem):
    n, rows = x_s.shape[:2]
    half = n // 2
    core = _here()[1]
    part = lambda ref, i: ref.at[pl.ds(pl.multiple_of(i * rows, rows), rows), :]
    get = lambda i: pltpu.make_async_copy(part(x_ref, i), x_s.at[i], sem.at[i])
    put = lambda i: pltpu.make_async_copy(a_s.at[i], part(a_ref, i), out_sem.at[i])
    give = lambda i: _to_sibling(a_s.at[i], b_s.at[i], send_sem.at[i], recv_sem.at[i])
    b_put = lambda i: pltpu.make_async_copy(b_s.at[i], part(b_ref, i), b_sem.at[i])
    keep = lambda to, i: pltpu.make_async_copy(a_s.at[i], part(to, lax.rem(i, half)), part_sem.at[i])
    b_keep = lambda to, i: pltpu.make_async_copy(b_s.at[i], part(to, lax.rem(i, half)), far_sem.at[i])
    ways = ((0, al_ref, ah_ref), (1, ah_ref, al_ref))
    gain_copy = pltpu.make_async_copy(gain_ref, gain_s, gain_sem.at[0])
    gain_copy.start()
    for i in range(AHEAD + 1):
        get(i).start()
    _meet()
    gain_copy.wait()

    def parts(i, do):
        for which, own, sib in ways:

            @pl.when((core == which) & (lax.div(i, half) == which))
            def _():
                do(own, sib)

    def step(i, _):
        get(i).wait()

        @pl.when(i + AHEAD + 1 < n)
        def _():
            get(i + AHEAD + 1).start()

        x = x_s[i].astype(F32)
        scale = lax.rsqrt(jnp.mean(x * x, -1, keepdims=True) + 1e-6)
        a_s[i] = (x * scale * gain_s[...].astype(F32)).astype(BF16)
        give(i).start()
        put(i).start()
        parts(i, lambda own, sib: keep(own, i).start())

    lax.fori_loop(0, n, step, None)

    def came(i, _):
        give(i).wait_recv()
        b_put(i).start()
        parts(i, lambda own, sib: b_keep(sib, i).start())

    lax.fori_loop(0, n, came, None)

    def done(i, _):
        put(i).wait()
        give(i).wait_send()
        b_put(i).wait()

        def both(own, sib):
            keep(own, i).wait()
            b_keep(sib, i).wait()

        parts(i, both)

    lax.fori_loop(0, n, done, None)


def head(x, gain, meeting):
    rows, d = x.shape
    n = 8
    block = (n, rows // n, d)
    vmem, dma = pltpu.VMEM, pltpu.SemaphoreType.DMA
    full, half = _sds((rows, d)), _sds((rows // 2, d))
    return _all(
        _head, [full, full, half, half],
        [vmem(block, BF16), vmem(block, BF16), vmem(block, BF16), vmem((1, d), BF16), *[dma((n,))] * 7, dma((1,))],
        10**9, 12 * rows * d, x, gain, meeting=meeting)


def _copies(pairs, sem, base=0):
    return [pltpu.make_async_copy(src, dst, sem.at[base + n]) for n, (src, dst) in enumerate(pairs)]


def _all(kernel, out_shape, scratch, flops, moved, *args, meeting=None):
    many = isinstance(out_shape, list)
    extra = {} if meeting is None else dict(collective_id=meeting, has_side_effects=True)
    return pl.pallas_call(
        kernel,
        in_specs=[ANY] * len(args),
        out_specs=[ANY] * len(out_shape) if many else ANY,
        out_shape=out_shape,
        scratch_shapes=scratch,
        compiler_params=pltpu.CompilerParams(vmem_limit_bytes=VMEM, **extra),
        cost_estimate=pl.CostEstimate(flops=int(flops), bytes_accessed=int(moved), transcendentals=0),
    )(*args)


def _pieces(pieces, a_s):
    at, pairs = 0, []
    for p in pieces:
        pairs.append((p, a_s.at[pl.ds(at, p.shape[0]), :]))
        at += p.shape[0]
    return pairs


def _places(chunk, ref, s):
    return [(ref.at[pl.ds(pl.multiple_of(at, HALF), HALF), :], s.at[pl.ds(m * HALF, HALF), :]) for m, at in enumerate(_starts(chunk))]


def _forward(piece, a_s, f_ref, sems):
    rows = piece.shape[0]
    under = a_s.at[pl.ds(rows, rows), :]
    return _to_sibling(piece, under, sems.at[0], sems.at[1]), pltpu.make_async_copy(under, f_ref, sems.at[2])


def _project(*refs, n, chunk):
    pieces, (wq_ref, wk_ref, wv_ref, c_ref, s_ref, q_ref, k_ref, v_ref), refs = refs[:n], refs[n : n + 8], refs[n + 8 :]
    f_ref, refs = (None, refs) if chunk == "near" else (refs[0], refs[1:])
    a_s, w_s, c_s, s_s, q_s, k_s, v_s, sem, w_sem, out_sem, kv_sem, f_sem = refs
    steps, wide = w_s.shape[0] - 1, w_s.shape[2]
    pairs = _pieces(pieces, a_s) + _places(chunk, c_ref, c_s) + _places(chunk, s_ref, s_s)
    ready = _copies(pairs, sem)
    columns = lambda ref, i: ref.at[:, pl.ds(pl.multiple_of(i * wide, wide), wide)]
    tile = lambda i: pltpu.make_async_copy(columns(wq_ref, i), w_s.at[i], w_sem.at[i])
    kv = [pltpu.make_async_copy(w, w_s.at[steps, :, pl.ds(m * HEAD, HEAD)], kv_sem.at[m]) for m, w in enumerate((wk_ref, wv_ref))]
    for copy in ready + [tile(0)]:
        copy.start()
    if f_ref is not None:
        _meet()
        forward, keep = _forward(pieces[0], a_s, f_ref, f_sem)
        forward.start()
    for copy in ready:
        copy.wait()
    for i in range(1, AHEAD):
        tile(i).start()
    if f_ref is not None:
        forward.wait()
        keep.start()

    def turn(t):
        t = t.astype(BF16).astype(F32)
        return (t * c_s[...] + pltpu.roll(t, HEAD // 2, 1) * s_s[...]).astype(BF16)

    out = lambda i, slot: pltpu.make_async_copy(q_s.at[slot], columns(q_ref, i), out_sem.at[slot])

    def step(i, _):
        slot = lax.rem(i, 2)
        tile(i).wait()

        @pl.when(i + AHEAD < steps)
        def _():
            tile(i + AHEAD).start()

        @pl.when(i + AHEAD == steps)
        def _():
            for copy in kv:
                copy.start()

        t = _dot(a_s[...], w_s[i], 1, 0)

        @pl.when(i >= 2)
        def _():
            out(i - 2, slot).wait()

        for m in range(wide // HEAD):
            q_s[slot, :, m * HEAD : (m + 1) * HEAD] = turn(t[:, m * HEAD : (m + 1) * HEAD])
        out(i, slot).start()

    lax.fori_loop(0, steps, step, None)
    for copy in kv:
        copy.wait()
    t = _dot(a_s[...], w_s[steps], 1, 0)
    k_s[...] = turn(t[:, :HEAD])
    v_s[...] = t[:, HEAD:].astype(BF16)
    last = _copies([(k_s, k_ref), (v_s, v_ref)], kv_sem)
    for copy in last:
        copy.start()
    for copy in last + [out(steps - 2 + m, (steps + m) % 2) for m in range(2)]:
        copy.wait()
    if f_ref is not None:
        keep.wait()


def project(chunk, pieces, wq, wk, wv, cos, sin, meeting=None):
    d, width = wq.shape
    n, rows = len(pieces), sum(p.shape[0] for p in pieces)
    more = [] if meeting is None else [_sds((rows, d))]
    rows *= 1 + len(more)
    wide = 256
    steps = width // wide
    vmem, dma = pltpu.VMEM, pltpu.SemaphoreType.DMA
    return _all(
        functools.partial(_project, n=n, chunk=chunk),
        [_sds((rows, width)), _sds((rows, HEAD)), _sds((rows, HEAD)), *more],
        [vmem((rows, d), BF16), vmem((steps + 1, d, wide), BF16), vmem((rows, HEAD), F32), vmem((rows, HEAD), F32), vmem((2, rows, wide), BF16),
         vmem((rows, HEAD), BF16), vmem((rows, HEAD), BF16), dma((n + 2 * rows // HALF,)), dma((steps,)), dma((2,)), dma((2,)), dma((3,))],
        2 * rows * d * (width + 2 * HEAD), 2 * (d * (width + 256) + rows * (d + width)), *pieces, wq, wk, wv, cos, sin, meeting=meeting)


def _into(*refs, n, forwards):
    pieces, w_ref, o_ref, refs = refs[:n], refs[n], refs[n + 1], refs[n + 2 :]
    f_ref, refs = (refs[0], refs[1:]) if forwards else (None, refs)
    a_s, w_s, o_s, sem, w_sem, out_sem, f_sem = refs
    steps, wide = w_s.shape[:2]
    ready = _copies(_pieces(pieces, a_s), sem)
    tile = lambda i: pltpu.make_async_copy(w_ref.at[pl.ds(pl.multiple_of(i * wide, wide), wide), :], w_s.at[i], w_sem.at[i])
    for copy in ready + [tile(0)]:
        copy.start()
    if forwards:
        _meet()
        forward, keep = _forward(pieces[0], a_s, f_ref, f_sem)
        forward.start()
    for copy in ready:
        copy.wait()
    for i in range(1, AHEAD):
        tile(i).start()
    if forwards:
        forward.wait()
        keep.start()
    out = lambda i, slot: pltpu.make_async_copy(o_s.at[slot], o_ref.at[:, pl.ds(pl.multiple_of(i * wide, wide), wide)], out_sem.at[slot])

    def step(i, _):
        slot = lax.rem(i, 2)
        tile(i).wait()

        @pl.when(i + AHEAD < steps)
        def _():
            tile(i + AHEAD).start()

        t = _dot(a_s[...], w_s[i], 1, 1).astype(BF16)

        @pl.when(i >= 2)
        def _():
            out(i - 2, slot).wait()

        o_s[slot] = t
        out(i, slot).start()

    lax.fori_loop(0, steps, step, None)
    for m in range(2):
        out(steps - 2 + m, (steps + m) % 2).wait()
    if forwards:
        keep.wait()


def into(pieces, wo, meeting=None):
    width, d = wo.shape
    n, rows = len(pieces), sum(p.shape[0] for p in pieces)
    more = [] if meeting is None else [_sds((rows, d))]
    rows *= 1 + len(more)
    result = _sds((rows, width))
    wide = 256
    steps = width // wide
    vmem, dma = pltpu.VMEM, pltpu.SemaphoreType.DMA
    return _all(
        functools.partial(_into, n=n, forwards=bool(more)), [result, *more] if more else result,
        [vmem((rows, d), BF16), vmem((steps, wide, d), BF16), vmem((2, rows, wide), BF16), dma((n,)), dma((steps,)), dma((2,)), dma((3,))],
        2 * rows * d * width, 2 * (d * width + rows * (d + width)), *pieces, wo, meeting=meeting)


def _near(a_ref, b_ref, dy_ref, wq_ref, wk_ref, wv_ref, wo_ref, c_ref, s_ref, q_ref, k_ref, v_ref, o_ref, e_ref, dh_ref, dl_ref,
          a_s, d_s, w_s, wo_s, c_s, s_s, q_s, k_s, v_s, o_s, sem, w_sem, wo_sem, out_sem, kv_sem, d_sem, e_sem):
    steps, wide = w_s.shape[0] - 1, w_s.shape[2]
    core = _here()[1]
    ready = _copies(_pieces((a_ref, b_ref), a_s) + _places("near", c_ref, c_s) + _places("near", s_ref, s_s), sem)
    columns = lambda ref, i: ref.at[:, pl.ds(pl.multiple_of(i * wide, wide), wide)]
    tile = lambda i: pltpu.make_async_copy(columns(wq_ref, i), w_s.at[i], w_sem.at[i])
    wo_tile = lambda i: pltpu.make_async_copy(wo_ref.at[pl.ds(pl.multiple_of(i * wide, wide), wide), :], wo_s.at[i], wo_sem.at[i])
    kv = [pltpu.make_async_copy(w, w_s.at[steps, :, pl.ds(m * HEAD, HEAD)], kv_sem.at[m]) for m, w in enumerate((wk_ref, wv_ref))]
    for copy in ready + [tile(0)]:
        copy.start()
    _meet()
    for copy in ready:
        copy.wait()
    tile(1).start()
    sib = d_s.at[pl.ds(BLOCK, BLOCK), :]
    swap = _to_sibling(dy_ref, sib, d_sem.at[0], d_sem.at[1])
    swap.start()
    d_get = pltpu.make_async_copy(dy_ref, d_s.at[pl.ds(0, BLOCK), :], d_sem.at[2])
    piece = lambda at: d_s.at[pl.ds(pl.multiple_of(at * HALF, HALF), HALF), :]
    given = [pltpu.make_async_copy(src, dst, e_sem.at[m])
             for m, (src, dst) in enumerate(((sib, e_ref), (piece(2 - core), dh_ref), (piece(3 * core), dl_ref)))]

    def turn(t):
        t = t.astype(BF16).astype(F32)
        return (t * c_s[...] + pltpu.roll(t, HEAD // 2, 1) * s_s[...]).astype(BF16)

    out = lambda s, ref, i, slot: pltpu.make_async_copy(s.at[slot], columns(ref, i), out_sem.at[slot])

    def step(i, _):
        slot = lax.rem(i, 2)
        tile(i).wait()

        @pl.when(i + AHEAD < steps)
        def _():
            tile(i + AHEAD).start()

        @pl.when(i + AHEAD == steps)
        def _():
            for copy in kv:
                copy.start()

        @pl.when(i == 2)
        def _():
            d_get.start()

        @pl.when(i + 1 == steps)
        def _():
            wo_tile(0).start()

        t = _dot(a_s[...], w_s[i], 1, 0)

        @pl.when(i >= 2)
        def _():
            out(q_s, q_ref, i - 2, slot).wait()

        for m in range(wide // HEAD):
            q_s[slot, :, m * HEAD : (m + 1) * HEAD] = turn(t[:, m * HEAD : (m + 1) * HEAD])
        out(q_s, q_ref, i, slot).start()

    lax.fori_loop(0, steps, step, None)
    for copy in kv:
        copy.wait()
    wo_tile(1).start()
    t = _dot(a_s[...], w_s[steps], 1, 0)
    k_s[...] = turn(t[:, :HEAD])
    v_s[...] = t[:, HEAD:].astype(BF16)
    last = _copies([(k_s, k_ref), (v_s, v_ref)], kv_sem)
    for copy in last:
        copy.start()
    for m in range(2):
        out(q_s, q_ref, steps - 2 + m, (steps + m) % 2).wait()
    swap.wait()
    d_get.wait()
    for copy in given:
        copy.start()

    def wo_step(i, _):
        slot = lax.rem(i, 2)
        wo_tile(i).wait()

        @pl.when(i + AHEAD < steps)
        def _():
            wo_tile(i + AHEAD).start()

        t = _dot(d_s[...], wo_s[i], 1, 1).astype(BF16)

        @pl.when(i >= 2)
        def _():
            out(o_s, o_ref, i - 2, slot).wait()

        o_s[slot] = t
        out(o_s, o_ref, i, slot).start()

    lax.fori_loop(0, steps, wo_step, None)
    for copy in last + [out(o_s, o_ref, steps - 2 + m, (steps + m) % 2) for m in range(2)] + given:
        copy.wait()


def near(a, b, dy, wq, wk, wv, wo, cos, sin, meeting):
    d, width = wq.shape
    rows = 2 * BLOCK
    wide = 256
    steps = width // wide
    vmem, dma = pltpu.VMEM, pltpu.SemaphoreType.DMA
    line = _sds((rows, HEAD))
    return _all(
        _near, [_sds((rows, width)), line, line, _sds((rows, width)), _sds((BLOCK, d)), _sds((HALF, d)), _sds((HALF, d))],
        [vmem((rows, d), BF16), vmem((rows, d), BF16), vmem((steps + 1, d, wide), BF16), vmem((steps, wide, d), BF16),
         vmem((rows, HEAD), F32), vmem((rows, HEAD), F32), vmem((2, rows, wide), BF16), vmem((rows, HEAD), BF16), vmem((rows, HEAD), BF16),
         vmem((2, rows, wide), BF16), dma((2 + 2 * rows // HALF,)), dma((steps,)), dma((steps,)), dma((2,)), dma((2,)), dma((3,)), dma((3,))],
        2 * rows * d * (2 * width + 2 * HEAD), 4 * d * (width + rows), a, b, dy, wq, wk, wv, wo, cos, sin, meeting=meeting)


def _attend(pos_ref, q_ref, do_ref, kl_ref, kh_ref, kr_ref, vl_ref, vh_ref, vr_ref, c_ref, s_ref, *rest, first, hp, added):
    dk_in, dv_in = rest[:2] if added else (None, None)
    seen_ref, dq_ref, dk_ref, dv_ref, k_s, v_s, kt_s, vt_s, s_s, dp_s, o_s, dq_s, dk_s, dv_s = rest[-14:]
    iq, ih = pl.program_id(0), pl.program_id(1)
    wide = hp * BLOCK
    e = HEAD**-0.5 * LOG2E

    @pl.when((iq == 0) & (ih == 0))
    def _():
        at = 0
        for kc, vc in ((kl_ref, vl_ref), (kh_ref, vh_ref), (kr_ref, vr_ref)):
            for m in range(kc.shape[0] // HALF):
                here = pl.ds(pl.multiple_of(pos_ref[at], HALF), HALF)
                k_s[here, :] = kc[m * HALF : (m + 1) * HALF, :]
                v_s[here, :] = vc[m * HALF : (m + 1) * HALF, :]
                at += 1
        kt_s[...] = k_s[...].T
        vt_s[...] = v_s[...].T
        dk_s[...] = dk_in[...] if added else jnp.zeros_like(dk_s)
        dv_s[...] = dv_in[...] if added else jnp.zeros_like(dv_s)

    place = pos_ref[first + 2 * iq]
    own = lax.div(place, BLOCK)
    turned = lax.rem(place, BLOCK)
    q2 = jnp.concatenate([q_ref[:, m * HEAD : (m + 1) * HEAD] for m in range(hp)], axis=0)
    do2 = jnp.concatenate([do_ref[:, m * HEAD : (m + 1) * HEAD] for m in range(hp)], axis=0)

    def rows(j):
        return pl.ds(pl.multiple_of(j * BLOCK, BLOCK), BLOCK)

    here = rows(own)
    s = _dot(k_s[here, :], q2, 1, 1)
    query = lax.rem(lax.broadcasted_iota(jnp.int32, s.shape, 1) + turned, BLOCK)
    s = jnp.where(lax.broadcasted_iota(jnp.int32, s.shape, 0) <= query, s, HIDDEN)
    s_s[here, :] = s

    def scores(j, top):
        s = _dot(k_s[rows(j), :], q2, 1, 1)
        s_s[rows(j), :] = s
        return jnp.maximum(top, s.max(axis=0, keepdims=True))

    top = lax.fori_loop(0, own, scores, s.max(axis=0, keepdims=True))
    o_s[...] = jnp.zeros_like(o_s)
    dq_s[...] = jnp.zeros_like(dq_s)

    def weigh(j, sums):
        total, delta = sums
        dp = _dot(v_s[rows(j), :], do2, 1, 1)
        dp_s[rows(j), :] = dp
        p = jnp.exp2((s_s[rows(j), :] - top) * e)
        s_s[rows(j), :] = p
        o_s[...] += _dot(vt_s[:, rows(j)], p.astype(BF16), 1, 0)
        return total + p.sum(axis=0, keepdims=True), delta + (p * dp).sum(axis=0, keepdims=True)

    zero = jnp.zeros((1, wide), F32)
    total, delta = lax.fori_loop(0, own + 1, weigh, (zero, zero))
    inv = 1 / total
    delta = delta * inv

    def grads(j, _):
        p = s_s[rows(j), :] * inv
        ds = (p * (dp_s[rows(j), :] - delta)).astype(BF16)
        dv_s[rows(j), :] += _dot(p.astype(BF16), do2, 1, 0)
        dk_s[rows(j), :] += _dot(ds, q2, 1, 0)
        dq_s[...] += _dot(kt_s[:, rows(j)], ds, 1, 0)

    lax.fori_loop(0, own + 1, grads, None)
    cos, sin = _table(c_ref, pos_ref, first + 2 * iq, 2), _table(s_ref, pos_ref, first + 2 * iq, 2)
    o = (o_s[...] * inv).astype(BF16)
    for m in range(hp):
        seen_ref[m * HEAD : (m + 1) * HEAD, :] = o[:, m * BLOCK : (m + 1) * BLOCK]
        g = (dq_s[:, m * BLOCK : (m + 1) * BLOCK] * HEAD**-0.5).T.astype(BF16).astype(F32)
        dq_ref[:, m * HEAD : (m + 1) * HEAD] = (g * cos - pltpu.roll(g, HEAD // 2, 1) * sin).astype(BF16)

    @pl.when((iq == pl.num_programs(0) - 1) & (ih == pl.num_programs(1) - 1))
    def _():
        dk_ref[...] = dk_s[...]
        dv_ref[...] = dv_s[...]


def attend(pos, first, q, do, ks, vs, cos, sin, sums=None):
    rows, width = q.shape
    hp = 6
    sk = sum(k.shape[0] for k in ks)
    tile = pl.BlockSpec((BLOCK, hp * HEAD), lambda i, h, _: (i, h))
    whole = lambda a: pl.BlockSpec(a.shape, lambda i, h, _: (0, 0))
    keys = _sds((sk, HEAD), F32)
    given = (*ks, *vs, cos, sin, *(sums or ()))
    wide = hp * BLOCK
    vmem = lambda *shape, t=F32: pltpu.VMEM(shape, t)
    return _call(
        functools.partial(_attend, first=first, hp=hp, added=sums is not None), (rows // BLOCK, width // (hp * HEAD)),
        [tile, tile, *map(whole, given)],
        [pl.BlockSpec((hp * HEAD, BLOCK), lambda i, h, _: (h, i)), tile, whole(keys), whole(keys)],
        [_sds((width, rows)), _sds((rows, width)), keys, keys],
        [vmem(sk, HEAD, t=BF16), vmem(sk, HEAD, t=BF16), vmem(HEAD, sk, t=BF16), vmem(HEAD, sk, t=BF16), vmem(sk, wide), vmem(sk, wide),
         vmem(HEAD, wide), vmem(HEAD, wide), vmem(sk, HEAD), vmem(sk, HEAD)],
        2 * 6 * 2 * rows * sk * width * 0.6, 8 * rows * width, (pos, q, do, *given))


def _back(dq_ref, dk_ref, dv_ref, c_ref, s_ref, wq_ref, wk_ref, wv_ref, sum_ref, g_ref,
          g_s, dk_s, dv_s, c_s, s_s, w_s, keep_s, send_s, came_s, sum_s, sem, w_sem, out_sem, g_sem, send_sem, recv_sem, *, chunk):
    rows, width = dq_ref.shape
    half = rows // 2
    steps, wide = w_s.shape[:2]
    pairs = [(dq_ref, g_s.at[:, pl.ds(0, width)])]
    for ref, s in ((dk_ref, dk_s), (dv_ref, dv_s), (c_ref, c_s), (s_ref, s_s)):
        pairs += _places(chunk, ref, s)
    ready = _copies(pairs, sem)
    lines = lambda ref, i: ref.at[pl.ds(pl.multiple_of(i * wide, wide), wide), :]
    parts = ((wq_ref, 0, width), (wk_ref, width, HEAD), (wv_ref, width + HEAD, HEAD))
    tile = lambda i: [pltpu.make_async_copy(lines(w, i), w_s.at[i, :, pl.ds(at, size)], w_sem.at[i, m]) for m, (w, at, size) in enumerate(parts)]
    for copy in ready + tile(0) + tile(1):
        copy.start()
    _meet()
    for copy in ready:
        copy.wait()
    for copy in tile(2):
        copy.start()
    g = (dk_s[...] * HEAD**-0.5).astype(BF16).astype(F32)
    g_s[:, width : width + HEAD] = (g * c_s[...] - pltpu.roll(g, HEAD // 2, 1) * s_s[...]).astype(BF16)
    g_s[:, width + HEAD :] = dv_s[...].astype(BF16)
    g_out = pltpu.make_async_copy(g_s, g_ref, g_sem.at[0])
    g_out.start()
    swap = lambda i: _to_sibling(send_s.at[i], came_s.at[i], send_sem.at[i], recv_sem.at[i])
    out = lambda i: pltpu.make_async_copy(sum_s.at[i], sum_ref.at[:, pl.ds(pl.multiple_of(i * wide, wide), wide)], out_sem.at[i])

    def add(i):
        swap(i).wait_recv()
        sum_s[i] = (keep_s[i] + came_s[i].astype(F32)).astype(sum_s.dtype)
        out(i).start()

    def step(i, _):
        for copy in tile(i):
            copy.wait()

        @pl.when(i + 3 < steps)
        def _():
            for copy in tile(i + 3):
                copy.start()

        t = _dot(g_s[...], w_s[i], 1, 1)
        keep_s[i] = t[:half]
        send_s[i] = t[half:].astype(BF16)
        swap(i).start()

        @pl.when(i >= LAG)
        def _():
            add(i - LAG)

    lax.fori_loop(0, steps, step, None)
    lax.fori_loop(steps - LAG, steps, lambda i, _: add(i), None)

    def done(i, _):
        swap(i).wait_send()
        out(i).wait()

    lax.fori_loop(0, steps, done, None)
    g_out.wait()


def back(chunk, dtype, dq, dk, dv, wq, wk, wv, cos, sin, meeting):
    d, width = wq.shape
    rows = dq.shape[0]
    wide = 512
    steps = d // wide
    full = width + 2 * HEAD
    vmem, dma = pltpu.VMEM, pltpu.SemaphoreType.DMA
    line = vmem((rows, HEAD), F32)
    tiles = lambda t: vmem((steps, rows // 2, wide), t)
    return _all(
        functools.partial(_back, chunk=chunk), [_sds((rows // 2, d), dtype), _sds((rows, full))],
        [vmem((rows, full), BF16), line, line, line, line, vmem((steps, wide, full), BF16), tiles(F32), tiles(BF16), tiles(BF16), tiles(dtype),
         dma((1 + 4 * rows // HALF,)), dma((steps, 3)), dma((steps,)), dma((1,)), dma((steps,)), dma((steps,))],
        2 * rows * d * full, 2 * (d * full + rows * (2 * d + width)), dq, dk, dv, cos, sin, wq, wk, wv, meeting=meeting)


def _weights(_, *refs, n, ng):
    pieces, gs, (wq_ref, wk_ref, wv_ref, g_s, sem) = refs[:n], refs[n : n + ng], refs[n + ng :]

    @pl.when(pl.program_id(0) == 0)
    def _():
        at, pairs = 0, []
        for g in gs:
            pairs.append((g, g_s.at[pl.ds(at, g.shape[0]), :]))
            at += g.shape[0]
        _fetch(pairs, sem)

    a = jnp.concatenate([p[...] for p in pieces], axis=0)
    t = _dot(a, g_s[...], 0, 0).astype(BF16)
    width = wq_ref.shape[1]
    wq_ref[...] = t[:, :width]
    wk_ref[...] = t[:, width : width + HEAD]
    wv_ref[...] = t[:, width + HEAD :]


def weights(pos, pieces, gs):
    d = pieces[0].shape[1]
    full = gs[0].shape[1]
    width = full - 2 * HEAD
    rows = sum(g.shape[0] for g in gs)
    wide = 1024
    tile = lambda n: pl.BlockSpec((wide, n), lambda i, _: (i, 0))
    return _call(
        functools.partial(_weights, n=len(pieces), ng=len(gs)), (d // wide,),
        [pl.BlockSpec((p.shape[0], wide), lambda i, _: (0, i)) for p in pieces] + [ANY] * len(gs),
        [tile(width), tile(HEAD), tile(HEAD)], [_sds((d, width)), _sds((d, HEAD)), _sds((d, HEAD))],
        [pltpu.VMEM((rows, full), BF16), pltpu.SemaphoreType.DMA((len(gs),))],
        2 * rows * d * full, 2 * (rows * (d + full) + d * full), (pos, *pieces, *gs))


def _out_weights(*refs, n, ns):
    pieces, seen, (dx_ref, o_ref, x_ref, s_s, x_s, sem, x_sem) = refs[:n], refs[n : n + ns], refs[n + ns :]
    i = pl.program_id(0)
    last = pl.num_programs(0) - 1
    get, put = pltpu.make_async_copy(dx_ref, x_s, x_sem.at[0]), pltpu.make_async_copy(x_s, x_ref, x_sem.at[1])

    @pl.when(i == 0)
    def _():
        at, pairs = 0, []
        for s in seen:
            pairs.append((s, s_s.at[:, pl.ds(at, s.shape[1])]))
            at += s.shape[1]
        _fetch(pairs, sem)
        get.start()

    @pl.when(i == last - 1)
    def _():
        get.wait()
        put.start()

    o_ref[...] = _dot(s_s[...], jnp.concatenate([p[...] for p in pieces], axis=0), 1, 0).astype(BF16)

    @pl.when(i == last)
    def _():
        put.wait()


def out_weights(pieces, seen, dx):
    d = pieces[0].shape[1]
    width = seen[0].shape[0]
    rows = sum(s.shape[1] for s in seen)
    wide = 1024
    return pl.pallas_call(
        functools.partial(_out_weights, n=len(pieces), ns=len(seen)),
        name="out_weights",
        grid=(d // wide,),
        in_specs=[pl.BlockSpec((p.shape[0], wide), lambda i: (0, i)) for p in pieces] + [ANY] * (len(seen) + 1),
        out_specs=[pl.BlockSpec((width, wide), lambda i: (0, i)), ANY],
        out_shape=[_sds((width, d)), _sds(dx.shape)],
        scratch_shapes=[pltpu.VMEM((width, rows), BF16), pltpu.VMEM(dx.shape, BF16), pltpu.SemaphoreType.DMA((len(seen),)),
                        pltpu.SemaphoreType.DMA((2,))],
        compiler_params=pltpu.CompilerParams(dimension_semantics=("arbitrary",), vmem_limit_bytes=VMEM),
        cost_estimate=pl.CostEstimate(flops=2 * rows * d * width, bytes_accessed=2 * (rows * (d + width) + d * width), transcendentals=0),
    )(*pieces, *seen, dx)


def _finish(own_ref, rh_ref, rl_ref, x_ref, dy_ref, gain_ref, dx_ref, dg_ref,
            own_s, far_s, x_s, dy_s, gain_s, dx_s, dg_s, sem, out_sem, far_sem):
    n, rows = x_s.shape[:2]
    part = lambda ref, i: ref.at[pl.ds(pl.multiple_of(i * rows, rows), rows), :]
    core = _here()[1]
    half = n // 2
    there = far_s.at[pl.ds(pl.multiple_of(core * HALF, HALF), HALF), :]
    mine = lambda ref: pltpu.make_async_copy(ref, there, far_sem.at[0])
    hand = lambda ref: _to_sibling(ref, there, far_sem.at[1], far_sem.at[2])
    rest = ((own_ref, own_s), (x_ref, x_s), (dy_ref, dy_s))
    row = lambda i: lax.rem(i + core * half, n)

    def get(i):
        return [pltpu.make_async_copy(part(ref, row(i)), s.at[i], sem.at[i, k]) for k, (ref, s) in enumerate(rest)]

    get_gain = pltpu.make_async_copy(gain_ref, gain_s, out_sem.at[n])
    get_gain.start()
    _meet()
    for which, here, give in ((0, rl_ref, rh_ref), (1, rh_ref, rl_ref)):

        @pl.when(core == which)
        def _():
            mine(here).start()
            hand(give).start()

    for i in range(AHEAD):
        for copy in get(i):
            copy.start()
    get_gain.wait()
    mine(rh_ref).wait()
    dg_s[...] = jnp.zeros_like(dg_s)

    def step(i, _):
        @pl.when(i + AHEAD < n)
        def _():
            for copy in get(i + AHEAD):
                copy.start()

        @pl.when(i == half)
        def _():
            hand(rh_ref).wait_recv()

        for copy in get(i):
            copy.wait()
        far = far_s[pl.ds(pl.multiple_of(row(i) * rows, rows), rows), :]
        da = own_s[i] + far.astype(F32)
        x = x_s[i].astype(F32)
        scale = lax.rsqrt(jnp.mean(x * x, -1, keepdims=True) + 1e-6)
        h = x * scale
        dg_s[...] += jnp.sum(da * h, axis=0, keepdims=True)
        dh = da * gain_s[...].astype(F32)
        dx = scale * (dh - h * jnp.mean(dh * h, -1, keepdims=True))
        dx_s[i] = (dy_s[i].astype(F32) + dx).astype(BF16)
        pltpu.make_async_copy(dx_s.at[i], part(dx_ref, row(i)), out_sem.at[i]).start()

    lax.fori_loop(0, n, step, None)
    last = pltpu.make_async_copy(dg_s, dg_ref, out_sem.at[n])
    last.start()
    for copy in _copies([(dx_s.at[i], part(dx_ref, i)) for i in range(n)], out_sem) + [last]:
        copy.wait()
    hand(rh_ref).wait_send()


def finish(own, rh, rl, x, dy, gain, meeting):
    rows, d = x.shape
    n = 8
    block = (n, rows // n, d)
    vmem, dma = pltpu.VMEM, pltpu.SemaphoreType.DMA
    return _all(
        _finish, [_sds((rows, d)), _sds((1, d), F32)],
        [vmem(block, F32), vmem((rows, d), BF16), vmem(block, BF16), vmem(block, BF16), vmem((1, d), BF16), vmem(block, BF16),
         vmem((1, d), F32), dma((n, 3)), dma((n + 1,)), dma((3,))],
        3 * 10**9, 12 * rows * d, own, rh, rl, x, dy, gain, meeting=meeting)


def tables(rows):
    half = HEAD // 2
    angle = jnp.arange(rows).astype(F32)[:, None] * THETA ** (-jnp.arange(half, dtype=F32) / half)
    cos, sin = jnp.cos(angle), jnp.sin(angle)
    return jnp.concatenate([cos, cos], -1), jnp.concatenate([-sin, sin], -1)


SIBLING = [(0, 1), (1, 0), (2, 3), (3, 2)]
PARTNER = [(0, 2), (2, 0), (1, 3), (3, 1)]
ACROSS = [(0, 3), (3, 0), (1, 2), (2, 1)]


def solution(mesh):
    def move(t, pairs):
        return lax.ppermute(t, "tp", pairs)

    def work(x, dy, gain, wq, wk, wv, wo):
        me = lax.axis_index("tp")
        core = lax.rem(me, 2)
        gain = gain[None]
        start = lambda block, half: block * BLOCK + half * HALF
        sib, far = me + 1 - 2 * core, 2 * (1 - lax.div(me, 2))
        pos = jnp.stack([start(me, 0), start(me, 1), start(sib, 0), start(sib, 1), start(far + 1, core), start(far + 1, 1 - core),
                         start(far, core), start(far, 1 - core)]).astype(jnp.int32)
        cos, sin = tables(4 * BLOCK)

        def after(t, *others):
            return lax.optimization_barrier((t, *others))[0]

        a, b, a_high, a_low = head(x, gain, 7)
        ah = move(a_high, PARTNER)
        al = move(a_low, PARTNER)
        w = (wq, wk, wv)
        turns = (cos, sin)
        q_n, k_n, v_n, do_n, e, d_high, d_low = near(a, b, dy, *w, wo, *turns, meeting=9)
        dh = move(d_high, PARTNER)
        dl = move(d_low, PARTNER)
        ah = after(ah, do_n)
        q_h, k_h, v_h, ah2 = project("high", (ah,), *w, *turns, meeting=0)
        al = after(al, q_h)
        q_l, k_l, v_l, al2 = project("low", (al,), *w, *turns, meeting=1)
        keys = ((k_n, k_h, k_l), (v_n, v_h, v_l), *turns)
        seen_n, dq_n, dk, dv = attend(pos, 0, q_n, do_n, *keys)
        dh = after(dh, dq_n)
        do_h, dh2 = into((dh,), wo, meeting=2)
        seen_h, dq_h, dk, dv = attend(pos, 4, q_h, do_h, *keys, sums=(dk, dv))
        sum_h, g_h = back("high", BF16, dq_h, dk, dv, *w, *turns, meeting=3)
        dl = after(dl, sum_h)
        do_l, dl2 = into((dl,), wo, meeting=4)
        seen_l, dq_l, dk, dv = attend(pos, 6, q_l, do_l, *keys, sums=(dk, dv))
        r_h = move(after(sum_h, dq_l), PARTNER)
        sum_l, g_l = back("low", BF16, dq_l, dk, dv, *w, *turns, meeting=5)
        r_l = move(sum_l, PARTNER)
        own, g_n = back("near", F32, after(dq_n, sum_l), dk, dv, *w, *turns, meeting=6)
        by_wq, by_wk, by_wv = weights(pos, (a, b, ah, ah2, al, al2), (after(g_n, own), g_h, g_l))
        dx, part = finish(own, after(r_h, by_wq), after(r_l, by_wq), x, dy, gain, 8)
        by_wo, by_x = out_weights((dy, e, dh, dh2, dl, dl2), (seen_n, seen_h, seen_l), dx)
        by_gain = (part + move(part, SIBLING)) + (move(part, PARTNER) + move(part, ACROSS))
        return by_x, by_gain, by_wq, by_wk, by_wv, by_wo

    tokens, columns = P(("dp", "tp"), None), P(None, "tp")
    return jax.shard_map(
        work,
        mesh=mesh,
        in_specs=(tokens, tokens, P(None), columns, columns, columns, P("tp", None)),
        out_specs=(tokens, P("dp", None), P("dp", "tp"), P("dp", "tp"), P("dp", "tp"), P(("dp", "tp"), None)),
        check_vma=False,
    )
```

```python
import functools

import jax
import jax.numpy as jnp
from jax import lax
from jax.experimental import pallas as pl
from jax.experimental.pallas import tpu as pltpu
from jax.sharding import PartitionSpec as P


HEAD = 128
THETA = 10000
HIDDEN = -2e30
LOG2E = 1.4426950408889634
VMEM = 63 * 2**20
HALF = 128
BLOCK = 256
LAG = 3
AHEAD = 2
F32, BF16 = jnp.float32, jnp.bfloat16
ANY = pl.BlockSpec(memory_space=pl.ANY)


def _dot(a, b, ca, cb):
    return lax.dot_general(a, b, (((ca,), (cb,)), ((), ())), preferred_element_type=F32)


def _call(kernel, grid, in_specs, out_specs, out_shape, scratch, flops, moved, args, scalars=1):
    return pl.pallas_call(
        kernel,
        grid_spec=pltpu.PrefetchScalarGridSpec(
            num_scalar_prefetch=scalars, grid=grid, in_specs=in_specs, out_specs=out_specs, scratch_shapes=scratch),
        out_shape=out_shape,
        compiler_params=pltpu.CompilerParams(dimension_semantics=("arbitrary",) * len(grid), vmem_limit_bytes=VMEM),
        cost_estimate=pl.CostEstimate(flops=int(flops), bytes_accessed=int(moved), transcendentals=0),
    )(*args)


def _here():
    me = lax.axis_index("tp")
    core = lax.rem(me, 2)
    return me, core, me + 1 - 2 * core, 2 * (1 - lax.div(me, 2))


def _starts(chunk):
    me, core, sib, far = _here()
    at = lambda block, half: block * BLOCK + half * HALF
    if chunk == "near":
        return [at(me, 0), at(me, 1), at(sib, 0), at(sib, 1)]
    block = far + (chunk == "high")
    return [at(block, core), at(block, 1 - core)]


def _meet():
    barrier = pltpu.get_barrier_semaphore()
    pl.semaphore_signal(barrier, inc=1, device_id={"tp": _here()[2]}, device_id_type=pl.DeviceIdType.MESH)
    pl.semaphore_wait(barrier, 1)


def _to_sibling(src, dst, send_sem, recv_sem):
    return pltpu.make_async_remote_copy(src_ref=src, dst_ref=dst, send_sem=send_sem, recv_sem=recv_sem, device_id={"tp": _here()[2]},
                                        device_id_type=pl.DeviceIdType.MESH)


def _sds(shape, dtype=BF16):
    return jax.ShapeDtypeStruct(shape, dtype)


def _head(x_ref, gain_ref, a_ref, b_ref, ah_ref, al_ref, x_s, a_s, b_s, gain_s, sem, out_sem, part_sem, send_sem, recv_sem, b_sem, far_sem, gain_sem):
    n, rows = x_s.shape[:2]
    half = n // 2
    core = _here()[1]
    part = lambda ref, i: ref.at[pl.ds(pl.multiple_of(i * rows, rows), rows), :]
    get = lambda i: pltpu.make_async_copy(part(x_ref, i), x_s.at[i], sem.at[i])
    put = lambda i: pltpu.make_async_copy(a_s.at[i], part(a_ref, i), out_sem.at[i])
    give = lambda i: _to_sibling(a_s.at[i], b_s.at[i], send_sem.at[i], recv_sem.at[i])
    b_put = lambda i: pltpu.make_async_copy(b_s.at[i], part(b_ref, i), b_sem.at[i])
    keep = lambda to, i: pltpu.make_async_copy(a_s.at[i], part(to, lax.rem(i, half)), part_sem.at[i])
    b_keep = lambda to, i: pltpu.make_async_copy(b_s.at[i], part(to, lax.rem(i, half)), far_sem.at[i])
    ways = ((0, al_ref, ah_ref), (1, ah_ref, al_ref))
    gain_copy = pltpu.make_async_copy(gain_ref, gain_s, gain_sem.at[0])
    gain_copy.start()
    for i in range(AHEAD + 1):
        get(i).start()
    _meet()
    gain_copy.wait()

    def parts(i, do):
        for which, own, sib in ways:

            @pl.when((core == which) & (lax.div(i, half) == which))
            def _():
                do(own, sib)

    def step(i, _):
        get(i).wait()

        @pl.when(i + AHEAD + 1 < n)
        def _():
            get(i + AHEAD + 1).start()

        x = x_s[i].astype(F32)
        scale = lax.rsqrt(jnp.mean(x * x, -1, keepdims=True) + 1e-6)
        a_s[i] = (x * scale * gain_s[...].astype(F32)).astype(BF16)
        give(i).start()
        put(i).start()
        parts(i, lambda own, sib: keep(own, i).start())

    lax.fori_loop(0, n, step, None)

    def came(i, _):
        give(i).wait_recv()
        b_put(i).start()
        parts(i, lambda own, sib: b_keep(sib, i).start())

    lax.fori_loop(0, n, came, None)

    def done(i, _):
        put(i).wait()
        give(i).wait_send()
        b_put(i).wait()

        def both(own, sib):
            keep(own, i).wait()
            b_keep(sib, i).wait()

        parts(i, both)

    lax.fori_loop(0, n, done, None)


def head(x, gain, meeting):
    rows, d = x.shape
    n = 8
    block = (n, rows // n, d)
    vmem, dma = pltpu.VMEM, pltpu.SemaphoreType.DMA
    full, half = _sds((rows, d)), _sds((rows // 2, d))
    return _all(
        _head, [full, full, half, half],
        [vmem(block, BF16), vmem(block, BF16), vmem(block, BF16), vmem((1, d), BF16), *[dma((n,))] * 7, dma((1,))],
        10**9, 12 * rows * d, x, gain, meeting=meeting)


def _copies(pairs, sem, base=0):
    return [pltpu.make_async_copy(src, dst, sem.at[base + n]) for n, (src, dst) in enumerate(pairs)]


def _all(kernel, out_shape, scratch, flops, moved, *args, meeting=None):
    many = isinstance(out_shape, list)
    extra = {} if meeting is None else dict(collective_id=meeting, has_side_effects=True)
    return pl.pallas_call(
        kernel,
        in_specs=[ANY] * len(args),
        out_specs=[ANY] * len(out_shape) if many else ANY,
        out_shape=out_shape,
        scratch_shapes=scratch,
        compiler_params=pltpu.CompilerParams(vmem_limit_bytes=VMEM, **extra),
        cost_estimate=pl.CostEstimate(flops=int(flops), bytes_accessed=int(moved), transcendentals=0),
    )(*args)


def _pieces(pieces, a_s):
    at, pairs = 0, []
    for p in pieces:
        pairs.append((p, a_s.at[pl.ds(at, p.shape[0]), :]))
        at += p.shape[0]
    return pairs


def _places(chunk, ref, s):
    return [(ref.at[pl.ds(pl.multiple_of(at, HALF), HALF), :], s.at[pl.ds(m * HALF, HALF), :]) for m, at in enumerate(_starts(chunk))]


def _forward(piece, a_s, f_ref, sems):
    rows = piece.shape[0]
    under = a_s.at[pl.ds(rows, rows), :]
    return _to_sibling(piece, under, sems.at[0], sems.at[1]), pltpu.make_async_copy(under, f_ref, sems.at[2])


def _project(*refs, n, chunk):
    pieces, (wq_ref, wk_ref, wv_ref, c_ref, s_ref, q_ref, k_ref, v_ref), refs = refs[:n], refs[n : n + 8], refs[n + 8 :]
    f_ref, refs = (None, refs) if chunk == "near" else (refs[0], refs[1:])
    a_s, w_s, c_s, s_s, q_s, k_s, v_s, sem, w_sem, out_sem, kv_sem, f_sem = refs
    steps, wide = w_s.shape[0] - 1, w_s.shape[2]
    pairs = _pieces(pieces, a_s) + _places(chunk, c_ref, c_s) + _places(chunk, s_ref, s_s)
    ready = _copies(pairs, sem)
    columns = lambda ref, i: ref.at[:, pl.ds(pl.multiple_of(i * wide, wide), wide)]
    tile = lambda i: pltpu.make_async_copy(columns(wq_ref, i), w_s.at[i], w_sem.at[i])
    kv = [pltpu.make_async_copy(w, w_s.at[steps, :, pl.ds(m * HEAD, HEAD)], kv_sem.at[m]) for m, w in enumerate((wk_ref, wv_ref))]
    for copy in ready + [tile(0)]:
        copy.start()
    if f_ref is not None:
        _meet()
        forward, keep = _forward(pieces[0], a_s, f_ref, f_sem)
        forward.start()
    for copy in ready:
        copy.wait()
    for i in range(1, AHEAD):
        tile(i).start()
    if f_ref is not None:
        forward.wait()
        keep.start()

    def turn(t):
        t = t.astype(BF16).astype(F32)
        return (t * c_s[...] + pltpu.roll(t, HEAD // 2, 1) * s_s[...]).astype(BF16)

    out = lambda i, slot: pltpu.make_async_copy(q_s.at[slot], columns(q_ref, i), out_sem.at[slot])

    def step(i, _):
        slot = lax.rem(i, 2)
        tile(i).wait()

        @pl.when(i + AHEAD < steps)
        def _():
            tile(i + AHEAD).start()

        @pl.when(i + AHEAD == steps)
        def _():
            for copy in kv:
                copy.start()

        t = _dot(a_s[...], w_s[i], 1, 0)

        @pl.when(i >= 2)
        def _():
            out(i - 2, slot).wait()

        for m in range(wide // HEAD):
            q_s[slot, :, m * HEAD : (m + 1) * HEAD] = turn(t[:, m * HEAD : (m + 1) * HEAD])
        out(i, slot).start()

    lax.fori_loop(0, steps, step, None)
    for copy in kv:
        copy.wait()
    t = _dot(a_s[...], w_s[steps], 1, 0)
    k_s[...] = turn(t[:, :HEAD])
    v_s[...] = t[:, HEAD:].astype(BF16)
    last = _copies([(k_s, k_ref), (v_s, v_ref)], kv_sem)
    for copy in last:
        copy.start()
    for copy in last + [out(steps - 2 + m, (steps + m) % 2) for m in range(2)]:
        copy.wait()
    if f_ref is not None:
        keep.wait()


def project(chunk, pieces, wq, wk, wv, cos, sin, meeting=None):
    d, width = wq.shape
    n, rows = len(pieces), sum(p.shape[0] for p in pieces)
    more = [] if meeting is None else [_sds((rows, d))]
    rows *= 1 + len(more)
    wide = 256
    steps = width // wide
    vmem, dma = pltpu.VMEM, pltpu.SemaphoreType.DMA
    return _all(
        functools.partial(_project, n=n, chunk=chunk),
        [_sds((rows, width)), _sds((rows, HEAD)), _sds((rows, HEAD)), *more],
        [vmem((rows, d), BF16), vmem((steps + 1, d, wide), BF16), vmem((rows, HEAD), F32), vmem((rows, HEAD), F32), vmem((2, rows, wide), BF16),
         vmem((rows, HEAD), BF16), vmem((rows, HEAD), BF16), dma((n + 2 * rows // HALF,)), dma((steps,)), dma((2,)), dma((2,)), dma((3,))],
        2 * rows * d * (width + 2 * HEAD), 2 * (d * (width + 256) + rows * (d + width)), *pieces, wq, wk, wv, cos, sin, meeting=meeting)


def _into(*refs, n, forwards):
    pieces, w_ref, o_ref, refs = refs[:n], refs[n], refs[n + 1], refs[n + 2 :]
    f_ref, refs = (refs[0], refs[1:]) if forwards else (None, refs)
    a_s, w_s, o_s, sem, w_sem, out_sem, f_sem = refs
    steps, wide = w_s.shape[:2]
    ready = _copies(_pieces(pieces, a_s), sem)
    tile = lambda i: pltpu.make_async_copy(w_ref.at[pl.ds(pl.multiple_of(i * wide, wide), wide), :], w_s.at[i], w_sem.at[i])
    for copy in ready + [tile(0)]:
        copy.start()
    if forwards:
        _meet()
        forward, keep = _forward(pieces[0], a_s, f_ref, f_sem)
        forward.start()
    for copy in ready:
        copy.wait()
    for i in range(1, AHEAD):
        tile(i).start()
    if forwards:
        forward.wait()
        keep.start()
    out = lambda i, slot: pltpu.make_async_copy(o_s.at[slot], o_ref.at[:, pl.ds(pl.multiple_of(i * wide, wide), wide)], out_sem.at[slot])

    def step(i, _):
        slot = lax.rem(i, 2)
        tile(i).wait()

        @pl.when(i + AHEAD < steps)
        def _():
            tile(i + AHEAD).start()

        t = _dot(a_s[...], w_s[i], 1, 1).astype(BF16)

        @pl.when(i >= 2)
        def _():
            out(i - 2, slot).wait()

        o_s[slot] = t
        out(i, slot).start()

    lax.fori_loop(0, steps, step, None)
    for m in range(2):
        out(steps - 2 + m, (steps + m) % 2).wait()
    if forwards:
        keep.wait()


def into(pieces, wo, meeting=None):
    width, d = wo.shape
    n, rows = len(pieces), sum(p.shape[0] for p in pieces)
    more = [] if meeting is None else [_sds((rows, d))]
    rows *= 1 + len(more)
    result = _sds((rows, width))
    wide = 256
    steps = width // wide
    vmem, dma = pltpu.VMEM, pltpu.SemaphoreType.DMA
    return _all(
        functools.partial(_into, n=n, forwards=bool(more)), [result, *more] if more else result,
        [vmem((rows, d), BF16), vmem((steps, wide, d), BF16), vmem((2, rows, wide), BF16), dma((n,)), dma((steps,)), dma((2,)), dma((3,))],
        2 * rows * d * width, 2 * (d * width + rows * (d + width)), *pieces, wo, meeting=meeting)


def _near(a_ref, b_ref, dy_ref, wq_ref, wk_ref, wv_ref, wo_ref, c_ref, s_ref, q_ref, k_ref, v_ref, o_ref, e_ref, dh_ref, dl_ref,
          a_s, d_s, w_s, wo_s, c_s, s_s, q_s, k_s, v_s, o_s, sem, w_sem, wo_sem, out_sem, kv_sem, d_sem, e_sem):
    steps, wide = w_s.shape[0] - 1, w_s.shape[2]
    core = _here()[1]
    ready = _copies(_pieces((a_ref, b_ref), a_s) + _places("near", c_ref, c_s) + _places("near", s_ref, s_s), sem)
    columns = lambda ref, i: ref.at[:, pl.ds(pl.multiple_of(i * wide, wide), wide)]
    tile = lambda i: pltpu.make_async_copy(columns(wq_ref, i), w_s.at[i], w_sem.at[i])
    wo_tile = lambda i: pltpu.make_async_copy(wo_ref.at[pl.ds(pl.multiple_of(i * wide, wide), wide), :], wo_s.at[i], wo_sem.at[i])
    kv = [pltpu.make_async_copy(w, w_s.at[steps, :, pl.ds(m * HEAD, HEAD)], kv_sem.at[m]) for m, w in enumerate((wk_ref, wv_ref))]
    for copy in ready + [tile(0)]:
        copy.start()
    _meet()
    for copy in ready:
        copy.wait()
    tile(1).start()
    sib = d_s.at[pl.ds(BLOCK, BLOCK), :]
    swap = _to_sibling(dy_ref, sib, d_sem.at[0], d_sem.at[1])
    swap.start()
    d_get = pltpu.make_async_copy(dy_ref, d_s.at[pl.ds(0, BLOCK), :], d_sem.at[2])
    piece = lambda at: d_s.at[pl.ds(pl.multiple_of(at * HALF, HALF), HALF), :]
    given = [pltpu.make_async_copy(src, dst, e_sem.at[m])
             for m, (src, dst) in enumerate(((sib, e_ref), (piece(2 - core), dh_ref), (piece(3 * core), dl_ref)))]

    def turn(t):
        t = t.astype(BF16).astype(F32)
        return (t * c_s[...] + pltpu.roll(t, HEAD // 2, 1) * s_s[...]).astype(BF16)

    out = lambda s, ref, i, slot: pltpu.make_async_copy(s.at[slot], columns(ref, i), out_sem.at[slot])

    def step(i, _):
        slot = lax.rem(i, 2)
        tile(i).wait()

        @pl.when(i + AHEAD < steps)
        def _():
            tile(i + AHEAD).start()

        @pl.when(i + AHEAD == steps)
        def _():
            for copy in kv:
                copy.start()

        @pl.when(i == 2)
        def _():
            d_get.start()

        @pl.when(i + 1 == steps)
        def _():
            wo_tile(0).start()

        t = _dot(a_s[...], w_s[i], 1, 0)

        @pl.when(i >= 2)
        def _():
            out(q_s, q_ref, i - 2, slot).wait()

        for m in range(wide // HEAD):
            q_s[slot, :, m * HEAD : (m + 1) * HEAD] = turn(t[:, m * HEAD : (m + 1) * HEAD])
        out(q_s, q_ref, i, slot).start()

    lax.fori_loop(0, steps, step, None)
    for copy in kv:
        copy.wait()
    wo_tile(1).start()
    t = _dot(a_s[...], w_s[steps], 1, 0)
    k_s[...] = turn(t[:, :HEAD])
    v_s[...] = t[:, HEAD:].astype(BF16)
    last = _copies([(k_s, k_ref), (v_s, v_ref)], kv_sem)
    for copy in last:
        copy.start()
    for m in range(2):
        out(q_s, q_ref, steps - 2 + m, (steps + m) % 2).wait()
    swap.wait()
    d_get.wait()
    for copy in given:
        copy.start()

    def wo_step(i, _):
        slot = lax.rem(i, 2)
        wo_tile(i).wait()

        @pl.when(i + AHEAD < steps)
        def _():
            wo_tile(i + AHEAD).start()

        t = _dot(d_s[...], wo_s[i], 1, 1).astype(BF16)

        @pl.when(i >= 2)
        def _():
            out(o_s, o_ref, i - 2, slot).wait()

        o_s[slot] = t
        out(o_s, o_ref, i, slot).start()

    lax.fori_loop(0, steps, wo_step, None)
    for copy in last + [out(o_s, o_ref, steps - 2 + m, (steps + m) % 2) for m in range(2)] + given:
        copy.wait()


def near(a, b, dy, wq, wk, wv, wo, cos, sin, meeting):
    d, width = wq.shape
    rows = 2 * BLOCK
    wide = 256
    steps = width // wide
    vmem, dma = pltpu.VMEM, pltpu.SemaphoreType.DMA
    line = _sds((rows, HEAD))
    return _all(
        _near, [_sds((rows, width)), line, line, _sds((rows, width)), _sds((BLOCK, d)), _sds((HALF, d)), _sds((HALF, d))],
        [vmem((rows, d), BF16), vmem((rows, d), BF16), vmem((steps + 1, d, wide), BF16), vmem((steps, wide, d), BF16),
         vmem((rows, HEAD), F32), vmem((rows, HEAD), F32), vmem((2, rows, wide), BF16), vmem((rows, HEAD), BF16), vmem((rows, HEAD), BF16),
         vmem((2, rows, wide), BF16), dma((2 + 2 * rows // HALF,)), dma((steps,)), dma((steps,)), dma((2,)), dma((2,)), dma((3,)), dma((3,))],
        2 * rows * d * (2 * width + 2 * HEAD), 4 * d * (width + rows), a, b, dy, wq, wk, wv, wo, cos, sin, meeting=meeting)


def _attend(pos_ref, q_ref, do_ref, kl_ref, kh_ref, kr_ref, vl_ref, vh_ref, vr_ref, c_ref, s_ref, *rest, first, hp, added):
    dk_in, dv_in = rest[:2] if added else (None, None)
    seen_ref, dq_ref, dk_ref, dv_ref, k_s, v_s, kt_s, vt_s, s_s, dp_s, o_s, dq_s, dk_s, dv_s, c_s, t_s, sem = rest[-17:]
    iq, ih = pl.program_id(0), pl.program_id(1)
    wide = hp * BLOCK
    e = HEAD**-0.5 * LOG2E

    n = c_s.shape[0] // HALF
    later = [(ref.at[pl.ds(pl.multiple_of(pos_ref[first + m], HALF), HALF), :], s.at[pl.ds(m * HALF, HALF), :])
             for ref, s in ((c_ref, c_s), (s_ref, t_s)) for m in range(n)]
    later = _copies(later + ([(dk_in, dk_s), (dv_in, dv_s)] if added else []), sem)
    starts = (iq == 0) & (ih == 0)

    @pl.when(starts)
    def _():
        for copy in later:
            copy.start()
        at = 0
        for kc, vc in ((kl_ref, vl_ref), (kh_ref, vh_ref), (kr_ref, vr_ref)):
            for m in range(kc.shape[0] // HALF):
                here = pl.ds(pl.multiple_of(pos_ref[at], HALF), HALF)
                k_s[here, :] = kc[m * HALF : (m + 1) * HALF, :]
                v_s[here, :] = vc[m * HALF : (m + 1) * HALF, :]
                at += 1
        kt_s[...] = k_s[...].T
        vt_s[...] = v_s[...].T
        if not added:
            dk_s[...] = jnp.zeros_like(dk_s)
            dv_s[...] = jnp.zeros_like(dv_s)

    place = pos_ref[first + 2 * iq]
    own = lax.div(place, BLOCK)
    turned = lax.rem(place, BLOCK)
    q2 = jnp.concatenate([q_ref[:, m * HEAD : (m + 1) * HEAD] for m in range(hp)], axis=0)
    do2 = jnp.concatenate([do_ref[:, m * HEAD : (m + 1) * HEAD] for m in range(hp)], axis=0)

    def rows(j):
        return pl.ds(pl.multiple_of(j * BLOCK, BLOCK), BLOCK)

    here = rows(own)
    s = _dot(k_s[here, :], q2, 1, 1)
    query = lax.rem(lax.broadcasted_iota(jnp.int32, s.shape, 1) + turned, BLOCK)
    s = jnp.where(lax.broadcasted_iota(jnp.int32, s.shape, 0) <= query, s, HIDDEN)
    s_s[here, :] = s

    def scores(j, top):
        s = _dot(k_s[rows(j), :], q2, 1, 1)
        s_s[rows(j), :] = s
        return jnp.maximum(top, s.max(axis=0, keepdims=True))

    top = lax.fori_loop(0, own, scores, s.max(axis=0, keepdims=True))
    o_s[...] = jnp.zeros_like(o_s)
    dq_s[...] = jnp.zeros_like(dq_s)

    def weigh(j, sums):
        total, delta = sums
        dp = _dot(v_s[rows(j), :], do2, 1, 1)
        dp_s[rows(j), :] = dp
        p = jnp.exp2((s_s[rows(j), :] - top) * e)
        s_s[rows(j), :] = p
        o_s[...] += _dot(vt_s[:, rows(j)], p.astype(BF16), 1, 0)
        return total + p.sum(axis=0, keepdims=True), delta + (p * dp).sum(axis=0, keepdims=True)

    zero = jnp.zeros((1, wide), F32)
    total, delta = lax.fori_loop(0, own + 1, weigh, (zero, zero))
    inv = 1 / total
    delta = delta * inv

    @pl.when(starts)
    def _():
        for copy in later:
            copy.wait()

    def grads(j, _):
        p = s_s[rows(j), :] * inv
        ds = (p * (dp_s[rows(j), :] - delta)).astype(BF16)
        dv_s[rows(j), :] += _dot(p.astype(BF16), do2, 1, 0)
        dk_s[rows(j), :] += _dot(ds, q2, 1, 0)
        dq_s[...] += _dot(kt_s[:, rows(j)], ds, 1, 0)

    lax.fori_loop(0, own + 1, grads, None)
    these = pl.ds(pl.multiple_of(iq * BLOCK, BLOCK), BLOCK)
    cos, sin = c_s[these, :], t_s[these, :]
    o = (o_s[...] * inv).astype(BF16)
    for m in range(hp):
        seen_ref[m * HEAD : (m + 1) * HEAD, :] = o[:, m * BLOCK : (m + 1) * BLOCK]
        g = (dq_s[:, m * BLOCK : (m + 1) * BLOCK] * HEAD**-0.5).T.astype(BF16).astype(F32)
        dq_ref[:, m * HEAD : (m + 1) * HEAD] = (g * cos - pltpu.roll(g, HEAD // 2, 1) * sin).astype(BF16)

    @pl.when((iq == pl.num_programs(0) - 1) & (ih == pl.num_programs(1) - 1))
    def _():
        dk_ref[...] = dk_s[...]
        dv_ref[...] = dv_s[...]


def attend(pos, first, q, do, ks, vs, cos, sin, sums=None):
    rows, width = q.shape
    hp = 6
    sk = sum(k.shape[0] for k in ks)
    tile = pl.BlockSpec((BLOCK, hp * HEAD), lambda i, h, _: (i, h))
    whole = lambda a: pl.BlockSpec(a.shape, lambda i, h, _: (0, 0))
    keys = _sds((sk, HEAD), F32)
    given, other = (*ks, *vs), (cos, sin, *(sums or ()))
    wide = hp * BLOCK
    vmem = lambda *shape, t=F32: pltpu.VMEM(shape, t)
    return _call(
        functools.partial(_attend, first=first, hp=hp, added=sums is not None), (rows // BLOCK, width // (hp * HEAD)),
        [tile, tile, *map(whole, given), *[ANY] * len(other)],
        [pl.BlockSpec((hp * HEAD, BLOCK), lambda i, h, _: (h, i)), tile, whole(keys), whole(keys)],
        [_sds((width, rows)), _sds((rows, width)), keys, keys],
        [vmem(sk, HEAD, t=BF16), vmem(sk, HEAD, t=BF16), vmem(HEAD, sk, t=BF16), vmem(HEAD, sk, t=BF16), vmem(sk, wide), vmem(sk, wide),
         vmem(HEAD, wide), vmem(HEAD, wide), vmem(sk, HEAD), vmem(sk, HEAD), vmem(rows, HEAD), vmem(rows, HEAD),
         pltpu.SemaphoreType.DMA((2 * rows // HALF + 2,))],
        2 * 6 * 2 * rows * sk * width * 0.6, 8 * rows * width, (pos, q, do, *given, *other))


def _back(*refs, chunks):
    n = len(chunks)
    dqs, (dk_ref, dv_ref, c_ref, s_ref, wq_ref, wk_ref, wv_ref), refs = refs[:n], refs[n : n + 7], refs[n + 7 :]
    sums, g_ref, refs = refs[:n], refs[n], refs[n + 1 :]
    sum_ss, (g_s, dk_s, dv_s, c_s, s_s, w_s, keep_s, send_s, came_s, sem, w_sem, out_sem, g_sem, send_sem, recv_sem) = refs[:n], refs[n:]
    width = dqs[0].shape[1]
    steps, wide = keep_s.shape[0], keep_s.shape[2]
    slots = w_s.shape[0]
    pairs, at = [], 0
    for dq, chunk in zip(dqs, chunks):
        rows = pl.ds(at, dq.shape[0])
        pairs.append((dq, g_s.at[rows, pl.ds(0, width)]))
        for ref, s in ((dk_ref, dk_s), (dv_ref, dv_s), (c_ref, c_s), (s_ref, s_s)):
            pairs += _places(chunk, ref, s.at[rows, :])
        at += dq.shape[0]
    ready = _copies(pairs, sem)
    lines = lambda ref, i: ref.at[pl.ds(pl.multiple_of(i * wide, wide), wide), :]
    parts = ((wq_ref, 0, width), (wk_ref, width, HEAD), (wv_ref, width + HEAD, HEAD))

    def tile(i):
        slot = lax.rem(i, slots)
        return [pltpu.make_async_copy(lines(w, i), w_s.at[slot, :, pl.ds(at, size)], w_sem.at[slot, m]) for m, (w, at, size) in enumerate(parts)]

    for copy in ready + tile(0) + tile(1):
        copy.start()
    _meet()
    for copy in ready:
        copy.wait()
    for copy in tile(2):
        copy.start()
    g = (dk_s[...] * HEAD**-0.5).astype(BF16).astype(F32)
    g_s[:, width : width + HEAD] = (g * c_s[...] - pltpu.roll(g, HEAD // 2, 1) * s_s[...]).astype(BF16)
    g_s[:, width + HEAD :] = dv_s[...].astype(BF16)
    g_out = pltpu.make_async_copy(g_s, g_ref, g_sem.at[0])
    g_out.start()
    swap = lambda i: _to_sibling(send_s.at[i], came_s.at[i], send_sem.at[i], recv_sem.at[i])
    columns = lambda i: pl.ds(pl.multiple_of(i * wide, wide), wide)
    out = lambda i: [pltpu.make_async_copy(s.at[i], ref.at[:, columns(i)], out_sem.at[i, m]) for m, (s, ref) in enumerate(zip(sum_ss, sums))]

    def add(i):
        swap(i).wait_recv()
        at = 0
        for s in sum_ss:
            rows = slice(at, at + s.shape[1])
            s[i] = (keep_s[i, rows, :] + came_s[i, rows, :].astype(F32)).astype(s.dtype)
            at += s.shape[1]
        for copy in out(i):
            copy.start()

    def step(i, _):
        for copy in tile(i):
            copy.wait()

        @pl.when(i + 3 < steps)
        def _():
            for copy in tile(i + 3):
                copy.start()

        t = _dot(g_s[...], w_s[lax.rem(i, slots)], 1, 1)
        at = 0
        for s in sum_ss:
            half = s.shape[1]
            keep_s[i, at : at + half, :] = t[2 * at : 2 * at + half]
            send_s[i, at : at + half, :] = t[2 * at + half : 2 * at + 2 * half].astype(BF16)
            at += half
        swap(i).start()

        @pl.when(i >= LAG)
        def _():
            add(i - LAG)

    lax.fori_loop(0, steps, step, None)
    lax.fori_loop(steps - LAG, steps, lambda i, _: add(i), None)

    def done(i, _):
        swap(i).wait_send()
        for copy in out(i):
            copy.wait()

    lax.fori_loop(0, steps, done, None)
    g_out.wait()


def back(chunks, dqs, dk, dv, wq, wk, wv, cos, sin, meeting):
    d, width = wq.shape
    each = [dq.shape[0] for dq in dqs]
    rows = sum(each)
    wide = 512
    steps = d // wide
    full = width + 2 * HEAD
    vmem, dma = pltpu.VMEM, pltpu.SemaphoreType.DMA
    line = vmem((rows, HEAD), F32)
    tiles = lambda t, n=rows: vmem((steps, n // 2, wide), t)
    return _all(
        functools.partial(_back, chunks=[name for name, _ in chunks]),
        [*[_sds((n // 2, d), t) for n, (_, t) in zip(each, chunks)], _sds((rows, full))],
        [*[tiles(t, n) for n, (_, t) in zip(each, chunks)], vmem((rows, full), BF16), line, line, line, line, vmem((5, wide, full), BF16),
         tiles(F32), tiles(BF16), tiles(BF16), dma((len(each) + 4 * rows // HALF,)), dma((5, 3)), dma((steps, len(each))), dma((1,)),
         dma((steps,)), dma((steps,))],
        2 * rows * d * full, 2 * (d * full + rows * (2 * d + width)), *dqs, dk, dv, cos, sin, wq, wk, wv, meeting=meeting)


def _tiles(pieces, a_s, sem, wide):
    def tile(i):
        slot, at, copies = lax.rem(i, 4), 0, []
        for m, p in enumerate(pieces):
            columns = pl.ds(pl.multiple_of(i * wide, wide), wide)
            copies.append(pltpu.make_async_copy(p.at[:, columns], a_s.at[slot, pl.ds(at, p.shape[0]), :], sem.at[slot, m]))
            at += p.shape[0]
        return copies

    return tile


def _go(copies):
    for copy in copies:
        copy.start()


def _wait(copies):
    for copy in copies:
        copy.wait()


def _stream(steps, tile, ready, out, work):
    _go(ready + tile(0))
    _go(tile(1))
    _wait(ready)

    def step(i, _):
        slot = lax.rem(i, 2)
        _wait(tile(i))

        @pl.when(i + 2 < steps)
        def _():
            _go(tile(i + 2))

        @pl.when(i >= 2)
        def _():
            _wait(out(i - 2, slot))

        work(i, slot)
        _go(out(i, slot))

    lax.fori_loop(0, steps, step, None)
    for m in range(2):
        _wait(out(steps - 2 + m, (steps + m) % 2))


def _weights(*refs, n, ng):
    pieces, gs, (wq_ref, wk_ref, wv_ref, a_s, g_s, o_s, a_sem, g_sem, o_sem) = refs[:n], refs[n : n + ng], refs[n + ng :]
    width, wide = wq_ref.shape[1], a_s.shape[2]
    parts = ((wq_ref, 0, width), (wk_ref, width, HEAD), (wv_ref, width + HEAD, HEAD))

    def out(i, slot):
        rows = pl.ds(pl.multiple_of(i * wide, wide), wide)
        return _copies([(o_s.at[slot, :, pl.ds(at, size)], ref.at[rows, :]) for ref, at, size in parts], o_sem.at[slot])

    def work(i, slot):
        o_s[slot] = _dot(a_s[lax.rem(i, 4)], g_s[...], 0, 0).astype(BF16)

    _stream(wq_ref.shape[0] // wide, _tiles(pieces, a_s, a_sem, wide), _copies(_pieces(gs, g_s), g_sem), out, work)


def weights(pieces, gs):
    d = pieces[0].shape[1]
    full = gs[0].shape[1]
    width = full - 2 * HEAD
    rows = sum(g.shape[0] for g in gs)
    wide = 512
    vmem, dma = pltpu.VMEM, pltpu.SemaphoreType.DMA
    return _all(
        functools.partial(_weights, n=len(pieces), ng=len(gs)), [_sds((d, width)), _sds((d, HEAD)), _sds((d, HEAD))],
        [vmem((4, rows, wide), BF16), vmem((rows, full), BF16), vmem((2, wide, full), BF16), dma((4, len(pieces))), dma((len(gs),)), dma((2, 3))],
        2 * rows * d * full, 2 * (rows * (d + full) + d * full), *pieces, *gs)


def _out_weights(*refs, n, ns):
    pieces, seen, (dx_ref, o_ref, x_ref, a_s, s_s, o_s, x_s, a_sem, s_sem, o_sem, x_sem) = refs[:n], refs[n : n + ns], refs[n + ns :]
    wide = a_s.shape[2]
    steps = o_ref.shape[1] // wide
    get, put = pltpu.make_async_copy(dx_ref, x_s, x_sem.at[0]), pltpu.make_async_copy(x_s, x_ref, x_sem.at[1])
    pairs, at = [], 0
    for s in seen:
        pairs.append((s, s_s.at[:, pl.ds(at, s.shape[1])]))
        at += s.shape[1]
    out = lambda i, slot: [pltpu.make_async_copy(o_s.at[slot], o_ref.at[:, pl.ds(pl.multiple_of(i * wide, wide), wide)], o_sem.at[slot])]

    def work(i, slot):
        @pl.when(i == 2)
        def _():
            get.start()

        @pl.when(i == steps // 2)
        def _():
            get.wait()
            put.start()

        o_s[slot] = _dot(s_s[...], a_s[lax.rem(i, 4)], 1, 0).astype(BF16)

    _stream(steps, _tiles(pieces, a_s, a_sem, wide), _copies(pairs, s_sem), out, work)
    put.wait()


def out_weights(pieces, seen, dx):
    d = pieces[0].shape[1]
    width = seen[0].shape[0]
    rows = sum(s.shape[1] for s in seen)
    wide = 512
    vmem, dma = pltpu.VMEM, pltpu.SemaphoreType.DMA
    return _all(
        functools.partial(_out_weights, n=len(pieces), ns=len(seen)), [_sds((width, d)), _sds(dx.shape)],
        [vmem((4, rows, wide), BF16), vmem((width, rows), BF16), vmem((2, width, wide), BF16), vmem(dx.shape, BF16),
         dma((4, len(pieces))), dma((len(seen),)), dma((2,)), dma((2,))],
        2 * rows * d * width, 2 * (rows * (d + width) + d * width), *pieces, *seen, dx)


def _finish(own_ref, rh_ref, rl_ref, x_ref, dy_ref, gain_ref, dx_ref, dg_ref,
            own_s, far_s, x_s, dy_s, gain_s, dx_s, dg_s, sem, out_sem, far_sem):
    n, rows = x_s.shape[:2]
    part = lambda ref, i: ref.at[pl.ds(pl.multiple_of(i * rows, rows), rows), :]
    core = _here()[1]
    half = n // 2
    there = far_s.at[pl.ds(pl.multiple_of(core * HALF, HALF), HALF), :]
    mine = lambda ref: pltpu.make_async_copy(ref, there, far_sem.at[0])
    hand = lambda ref: _to_sibling(ref, there, far_sem.at[1], far_sem.at[2])
    rest = ((own_ref, own_s), (x_ref, x_s), (dy_ref, dy_s))
    row = lambda i: lax.rem(i + core * half, n)

    def get(i):
        return [pltpu.make_async_copy(part(ref, row(i)), s.at[i], sem.at[i, k]) for k, (ref, s) in enumerate(rest)]

    get_gain = pltpu.make_async_copy(gain_ref, gain_s, out_sem.at[n])
    get_gain.start()
    _meet()
    for which, here, give in ((0, rl_ref, rh_ref), (1, rh_ref, rl_ref)):

        @pl.when(core == which)
        def _():
            mine(here).start()
            hand(give).start()

    for i in range(AHEAD):
        for copy in get(i):
            copy.start()
    get_gain.wait()
    mine(rh_ref).wait()
    dg_s[...] = jnp.zeros_like(dg_s)

    def step(i, _):
        @pl.when(i + AHEAD < n)
        def _():
            for copy in get(i + AHEAD):
                copy.start()

        @pl.when(i == half)
        def _():
            hand(rh_ref).wait_recv()

        for copy in get(i):
            copy.wait()
        far = far_s[pl.ds(pl.multiple_of(row(i) * rows, rows), rows), :]
        da = own_s[i] + far.astype(F32)
        x = x_s[i].astype(F32)
        scale = lax.rsqrt(jnp.mean(x * x, -1, keepdims=True) + 1e-6)
        h = x * scale
        dg_s[...] += jnp.sum(da * h, axis=0, keepdims=True)
        dh = da * gain_s[...].astype(F32)
        dx = scale * (dh - h * jnp.mean(dh * h, -1, keepdims=True))
        dx_s[i] = (dy_s[i].astype(F32) + dx).astype(BF16)
        pltpu.make_async_copy(dx_s.at[i], part(dx_ref, row(i)), out_sem.at[i]).start()

    lax.fori_loop(0, n, step, None)
    last = pltpu.make_async_copy(dg_s, dg_ref, out_sem.at[n])
    last.start()
    for copy in _copies([(dx_s.at[i], part(dx_ref, i)) for i in range(n)], out_sem) + [last]:
        copy.wait()
    hand(rh_ref).wait_send()


def finish(own, rh, rl, x, dy, gain, meeting):
    rows, d = x.shape
    n = 8
    block = (n, rows // n, d)
    vmem, dma = pltpu.VMEM, pltpu.SemaphoreType.DMA
    return _all(
        _finish, [_sds((rows, d)), _sds((1, d), F32)],
        [vmem(block, F32), vmem((rows, d), BF16), vmem(block, BF16), vmem(block, BF16), vmem((1, d), BF16), vmem(block, BF16),
         vmem((1, d), F32), dma((n, 3)), dma((n + 1,)), dma((3,))],
        3 * 10**9, 12 * rows * d, own, rh, rl, x, dy, gain, meeting=meeting)


def tables(rows):
    half = HEAD // 2
    angle = jnp.arange(rows).astype(F32)[:, None] * THETA ** (-jnp.arange(half, dtype=F32) / half)
    cos, sin = jnp.cos(angle), jnp.sin(angle)
    return jnp.concatenate([cos, cos], -1), jnp.concatenate([-sin, sin], -1)


SIBLING = [(0, 1), (1, 0), (2, 3), (3, 2)]
PARTNER = [(0, 2), (2, 0), (1, 3), (3, 1)]
ACROSS = [(0, 3), (3, 0), (1, 2), (2, 1)]


def solution(mesh):
    def move(t, pairs):
        return lax.ppermute(t, "tp", pairs)

    def work(x, dy, gain, wq, wk, wv, wo):
        me = lax.axis_index("tp")
        core = lax.rem(me, 2)
        gain = gain[None]
        start = lambda block, half: block * BLOCK + half * HALF
        sib, far = me + 1 - 2 * core, 2 * (1 - lax.div(me, 2))
        pos = jnp.stack([start(me, 0), start(me, 1), start(sib, 0), start(sib, 1), start(far + 1, core), start(far + 1, 1 - core),
                         start(far, core), start(far, 1 - core)]).astype(jnp.int32)
        cos, sin = tables(4 * BLOCK)

        def after(t, *others):
            return lax.optimization_barrier((t, *others))[0]

        a, b, a_high, a_low = head(x, gain, 7)
        ah = move(a_high, PARTNER)
        al = move(a_low, PARTNER)
        w = (wq, wk, wv)
        turns = (cos, sin)
        q_n, k_n, v_n, do_n, e, d_high, d_low = near(a, b, dy, *w, wo, *turns, meeting=9)
        dh = move(d_high, PARTNER)
        dl = move(d_low, PARTNER)
        ah = after(ah, do_n)
        q_h, k_h, v_h, ah2 = project("high", (ah,), *w, *turns, meeting=0)
        al = after(al, q_h)
        q_l, k_l, v_l, al2 = project("low", (al,), *w, *turns, meeting=1)
        keys = ((k_n, k_h, k_l), (v_n, v_h, v_l), *turns)
        seen_n, dq_n, dk, dv = attend(pos, 0, q_n, do_n, *keys)
        dh = after(dh, dq_n)
        do_h, dh2 = into((dh,), wo, meeting=2)
        seen_h, dq_h, dk, dv = attend(pos, 4, q_h, do_h, *keys, sums=(dk, dv))
        sum_h, g_h = back((("high", BF16),), (dq_h,), dk, dv, *w, *turns, meeting=3)
        r_h = move(sum_h, PARTNER)
        dl = after(dl, sum_h)
        do_l, dl2 = into((dl,), wo, meeting=4)
        seen_l, dq_l, dk, dv = attend(pos, 6, q_l, do_l, *keys, sums=(dk, dv))
        sum_l, own, g = back((("low", BF16), ("near", F32)), (dq_l, dq_n), dk, dv, *w, *turns, meeting=5)
        r_l = move(sum_l, PARTNER)
        by_wq, by_wk, by_wv = weights((ah, ah2, al, al2, a, b), (g_h, after(g, sum_l)))
        dx, part = finish(own, after(r_h, by_wq), after(r_l, by_wq), x, dy, gain, 8)
        by_wo, by_x = out_weights((dy, e, dh, dh2, dl, dl2), (seen_n, seen_h, seen_l), dx)
        by_gain = (part + move(part, SIBLING)) + (move(part, PARTNER) + move(part, ACROSS))
        return by_x, by_gain, by_wq, by_wk, by_wv, by_wo

    tokens, columns = P(("dp", "tp"), None), P(None, "tp")
    return jax.shard_map(
        work,
        mesh=mesh,
        in_specs=(tokens, tokens, P(None), columns, columns, columns, P("tp", None)),
        out_specs=(tokens, P("dp", None), P("dp", "tp"), P("dp", "tp"), P("dp", "tp"), P(("dp", "tp"), None)),
        check_vma=False,
    )
```

```python
import functools

import jax
import jax.numpy as jnp
from jax import lax
from jax.experimental import pallas as pl
from jax.experimental.pallas import tpu as pltpu
from jax.sharding import PartitionSpec as P


HEAD = 128
THETA = 10000
HIDDEN = -2e30
LOG2E = 1.4426950408889634
VMEM = 63 * 2**20
HALF = 128
BLOCK = 256
LAG = 3
AHEAD = 2
F32, BF16 = jnp.float32, jnp.bfloat16
ANY = pl.BlockSpec(memory_space=pl.ANY)


def _dot(a, b, ca, cb):
    return lax.dot_general(a, b, (((ca,), (cb,)), ((), ())), preferred_element_type=F32)


def _call(kernel, grid, in_specs, out_specs, out_shape, scratch, flops, moved, args, scalars=1):
    return pl.pallas_call(
        kernel,
        grid_spec=pltpu.PrefetchScalarGridSpec(
            num_scalar_prefetch=scalars, grid=grid, in_specs=in_specs, out_specs=out_specs, scratch_shapes=scratch),
        out_shape=out_shape,
        compiler_params=pltpu.CompilerParams(dimension_semantics=("arbitrary",) * len(grid), vmem_limit_bytes=VMEM),
        cost_estimate=pl.CostEstimate(flops=int(flops), bytes_accessed=int(moved), transcendentals=0),
    )(*args)


def _here():
    me = lax.axis_index("tp")
    core = lax.rem(me, 2)
    return me, core, me + 1 - 2 * core, 2 * (1 - lax.div(me, 2))


def _starts(chunk):
    me, core, sib, far = _here()
    at = lambda block, half: block * BLOCK + half * HALF
    if chunk == "near":
        return [at(me, 0), at(me, 1), at(sib, 0), at(sib, 1)]
    block = far + (chunk == "high")
    return [at(block, core), at(block, 1 - core)]


def _meet():
    barrier = pltpu.get_barrier_semaphore()
    pl.semaphore_signal(barrier, inc=1, device_id={"tp": _here()[2]}, device_id_type=pl.DeviceIdType.MESH)
    pl.semaphore_wait(barrier, 1)


def _to_sibling(src, dst, send_sem, recv_sem):
    return pltpu.make_async_remote_copy(src_ref=src, dst_ref=dst, send_sem=send_sem, recv_sem=recv_sem, device_id={"tp": _here()[2]},
                                        device_id_type=pl.DeviceIdType.MESH)


def _sds(shape, dtype=BF16):
    return jax.ShapeDtypeStruct(shape, dtype)


def _head(x_ref, gain_ref, a_ref, b_ref, ah_ref, al_ref, x_s, a_s, b_s, gain_s, sem, out_sem, part_sem, send_sem, recv_sem, b_sem, far_sem, gain_sem):
    n, rows = x_s.shape[:2]
    half = n // 2
    core = _here()[1]
    part = lambda ref, i: ref.at[pl.ds(pl.multiple_of(i * rows, rows), rows), :]
    get = lambda i: pltpu.make_async_copy(part(x_ref, i), x_s.at[i], sem.at[i])
    put = lambda i: pltpu.make_async_copy(a_s.at[i], part(a_ref, i), out_sem.at[i])
    give = lambda i: _to_sibling(a_s.at[i], b_s.at[i], send_sem.at[i], recv_sem.at[i])
    b_put = lambda i: pltpu.make_async_copy(b_s.at[i], part(b_ref, i), b_sem.at[i])
    keep = lambda to, i: pltpu.make_async_copy(a_s.at[i], part(to, lax.rem(i, half)), part_sem.at[i])
    b_keep = lambda to, i: pltpu.make_async_copy(b_s.at[i], part(to, lax.rem(i, half)), far_sem.at[i])
    ways = ((0, al_ref, ah_ref), (1, ah_ref, al_ref))
    gain_copy = pltpu.make_async_copy(gain_ref, gain_s, gain_sem.at[0])
    gain_copy.start()
    for i in range(AHEAD + 1):
        get(i).start()
    _meet()
    gain_copy.wait()

    def parts(i, do):
        for which, own, sib in ways:

            @pl.when((core == which) & (lax.div(i, half) == which))
            def _():
                do(own, sib)

    def step(i, _):
        get(i).wait()

        @pl.when(i + AHEAD + 1 < n)
        def _():
            get(i + AHEAD + 1).start()

        x = x_s[i].astype(F32)
        scale = lax.rsqrt(jnp.mean(x * x, -1, keepdims=True) + 1e-6)
        a_s[i] = (x * scale * gain_s[...].astype(F32)).astype(BF16)
        give(i).start()
        put(i).start()
        parts(i, lambda own, sib: keep(own, i).start())

    lax.fori_loop(0, n, step, None)

    def came(i, _):
        give(i).wait_recv()
        b_put(i).start()
        parts(i, lambda own, sib: b_keep(sib, i).start())

    lax.fori_loop(0, n, came, None)

    def done(i, _):
        put(i).wait()
        give(i).wait_send()
        b_put(i).wait()

        def both(own, sib):
            keep(own, i).wait()
            b_keep(sib, i).wait()

        parts(i, both)

    lax.fori_loop(0, n, done, None)


def head(x, gain, meeting):
    rows, d = x.shape
    n = 8
    block = (n, rows // n, d)
    vmem, dma = pltpu.VMEM, pltpu.SemaphoreType.DMA
    full, half = _sds((rows, d)), _sds((rows // 2, d))
    return _all(
        _head, [full, full, half, half],
        [vmem(block, BF16), vmem(block, BF16), vmem(block, BF16), vmem((1, d), BF16), *[dma((n,))] * 7, dma((1,))],
        10**9, 12 * rows * d, x, gain, meeting=meeting)


def _copies(pairs, sem, base=0):
    return [pltpu.make_async_copy(src, dst, sem.at[base + n]) for n, (src, dst) in enumerate(pairs)]


def _all(kernel, out_shape, scratch, flops, moved, *args, meeting=None, aliases=None):
    many = isinstance(out_shape, list)
    extra = {} if meeting is None else dict(collective_id=meeting, has_side_effects=True)
    return pl.pallas_call(
        kernel,
        in_specs=[ANY] * len(args),
        out_specs=[ANY] * len(out_shape) if many else ANY,
        out_shape=out_shape,
        scratch_shapes=scratch,
        input_output_aliases=aliases or {},
        compiler_params=pltpu.CompilerParams(vmem_limit_bytes=VMEM, **extra),
        cost_estimate=pl.CostEstimate(flops=int(flops), bytes_accessed=int(moved), transcendentals=0),
    )(*args)


def _pieces(pieces, a_s):
    at, pairs = 0, []
    for p in pieces:
        pairs.append((p, a_s.at[pl.ds(at, p.shape[0]), :]))
        at += p.shape[0]
    return pairs


def _places(chunk, ref, s):
    return [(ref.at[pl.ds(pl.multiple_of(at, HALF), HALF), :], s.at[pl.ds(m * HALF, HALF), :]) for m, at in enumerate(_starts(chunk))]


def _forward(piece, a_s, f_ref, sems):
    rows = piece.shape[0]
    under = a_s.at[pl.ds(rows, rows), :]
    return _to_sibling(piece, under, sems.at[0], sems.at[1]), pltpu.make_async_copy(under, f_ref, sems.at[2])


def _project(*refs, n, chunk):
    pieces, (wq_ref, wk_ref, wv_ref, c_ref, s_ref, q_ref, k_ref, v_ref), refs = refs[:n], refs[n : n + 8], refs[n + 8 :]
    f_ref, refs = (None, refs) if chunk == "near" else (refs[0], refs[1:])
    a_s, w_s, c_s, s_s, q_s, k_s, v_s, sem, w_sem, out_sem, kv_sem, f_sem = refs
    steps, wide = w_s.shape[0] - 1, w_s.shape[2]
    pairs = _pieces(pieces, a_s) + _places(chunk, c_ref, c_s) + _places(chunk, s_ref, s_s)
    ready = _copies(pairs, sem)
    columns = lambda ref, i: ref.at[:, pl.ds(pl.multiple_of(i * wide, wide), wide)]
    tile = lambda i: pltpu.make_async_copy(columns(wq_ref, i), w_s.at[i], w_sem.at[i])
    kv = [pltpu.make_async_copy(w, w_s.at[steps, :, pl.ds(m * HEAD, HEAD)], kv_sem.at[m]) for m, w in enumerate((wk_ref, wv_ref))]
    for copy in ready + [tile(0)]:
        copy.start()
    if f_ref is not None:
        _meet()
        forward, keep = _forward(pieces[0], a_s, f_ref, f_sem)
        forward.start()
    for copy in ready:
        copy.wait()
    for i in range(1, AHEAD):
        tile(i).start()
    if f_ref is not None:
        forward.wait()
        keep.start()

    def turn(t):
        t = t.astype(BF16).astype(F32)
        return (t * c_s[...] + pltpu.roll(t, HEAD // 2, 1) * s_s[...]).astype(BF16)

    out = lambda i, slot: pltpu.make_async_copy(q_s.at[slot], columns(q_ref, i), out_sem.at[slot])

    def step(i, _):
        slot = lax.rem(i, 2)
        tile(i).wait()

        @pl.when(i + AHEAD < steps)
        def _():
            tile(i + AHEAD).start()

        @pl.when(i + AHEAD == steps)
        def _():
            for copy in kv:
                copy.start()

        t = _dot(a_s[...], w_s[i], 1, 0)

        @pl.when(i >= 2)
        def _():
            out(i - 2, slot).wait()

        for m in range(wide // HEAD):
            q_s[slot, :, m * HEAD : (m + 1) * HEAD] = turn(t[:, m * HEAD : (m + 1) * HEAD])
        out(i, slot).start()

    lax.fori_loop(0, steps, step, None)
    for copy in kv:
        copy.wait()
    t = _dot(a_s[...], w_s[steps], 1, 0)
    k_s[...] = turn(t[:, :HEAD])
    v_s[...] = t[:, HEAD:].astype(BF16)
    last = _copies([(k_s, k_ref), (v_s, v_ref)], kv_sem)
    for copy in last:
        copy.start()
    for copy in last + [out(steps - 2 + m, (steps + m) % 2) for m in range(2)]:
        copy.wait()
    if f_ref is not None:
        keep.wait()


def project(chunk, pieces, wq, wk, wv, cos, sin, meeting=None):
    d, width = wq.shape
    n, rows = len(pieces), sum(p.shape[0] for p in pieces)
    more = [] if meeting is None else [_sds((rows, d))]
    rows *= 1 + len(more)
    wide = 256
    steps = width // wide
    vmem, dma = pltpu.VMEM, pltpu.SemaphoreType.DMA
    return _all(
        functools.partial(_project, n=n, chunk=chunk),
        [_sds((rows, width)), _sds((rows, HEAD)), _sds((rows, HEAD)), *more],
        [vmem((rows, d), BF16), vmem((steps + 1, d, wide), BF16), vmem((rows, HEAD), F32), vmem((rows, HEAD), F32), vmem((2, rows, wide), BF16),
         vmem((rows, HEAD), BF16), vmem((rows, HEAD), BF16), dma((n + 2 * rows // HALF,)), dma((steps,)), dma((2,)), dma((2,)), dma((3,))],
        2 * rows * d * (width + 2 * HEAD), 2 * (d * (width + 256) + rows * (d + width)), *pieces, wq, wk, wv, cos, sin, meeting=meeting)


def _into(*refs, n, forwards):
    pieces, w_ref, o_ref, refs = refs[:n], refs[n], refs[n + 1], refs[n + 2 :]
    f_ref, refs = (refs[0], refs[1:]) if forwards else (None, refs)
    a_s, w_s, o_s, sem, w_sem, out_sem, f_sem = refs
    steps, wide = w_s.shape[:2]
    ready = _copies(_pieces(pieces, a_s), sem)
    tile = lambda i: pltpu.make_async_copy(w_ref.at[pl.ds(pl.multiple_of(i * wide, wide), wide), :], w_s.at[i], w_sem.at[i])
    for copy in ready + [tile(0)]:
        copy.start()
    if forwards:
        _meet()
        forward, keep = _forward(pieces[0], a_s, f_ref, f_sem)
        forward.start()
    for copy in ready:
        copy.wait()
    for i in range(1, AHEAD):
        tile(i).start()
    if forwards:
        forward.wait()
        keep.start()
    out = lambda i, slot: pltpu.make_async_copy(o_s.at[slot], o_ref.at[:, pl.ds(pl.multiple_of(i * wide, wide), wide)], out_sem.at[slot])

    def step(i, _):
        slot = lax.rem(i, 2)
        tile(i).wait()

        @pl.when(i + AHEAD < steps)
        def _():
            tile(i + AHEAD).start()

        t = _dot(a_s[...], w_s[i], 1, 1).astype(BF16)

        @pl.when(i >= 2)
        def _():
            out(i - 2, slot).wait()

        o_s[slot] = t
        out(i, slot).start()

    lax.fori_loop(0, steps, step, None)
    for m in range(2):
        out(steps - 2 + m, (steps + m) % 2).wait()
    if forwards:
        keep.wait()


def into(pieces, wo, meeting=None):
    width, d = wo.shape
    n, rows = len(pieces), sum(p.shape[0] for p in pieces)
    more = [] if meeting is None else [_sds((rows, d))]
    rows *= 1 + len(more)
    result = _sds((rows, width))
    wide = 256
    steps = width // wide
    vmem, dma = pltpu.VMEM, pltpu.SemaphoreType.DMA
    return _all(
        functools.partial(_into, n=n, forwards=bool(more)), [result, *more] if more else result,
        [vmem((rows, d), BF16), vmem((steps, wide, d), BF16), vmem((2, rows, wide), BF16), dma((n,)), dma((steps,)), dma((2,)), dma((3,))],
        2 * rows * d * width, 2 * (d * width + rows * (d + width)), *pieces, wo, meeting=meeting)


def _near(a_ref, b_ref, dy_ref, wq_ref, wk_ref, wv_ref, wo_ref, c_ref, s_ref, q_ref, k_ref, v_ref, o_ref, e_ref, dh_ref, dl_ref,
          a_s, d_s, w_s, wo_s, c_s, s_s, q_s, k_s, v_s, o_s, sem, w_sem, wo_sem, out_sem, kv_sem, d_sem, e_sem):
    steps, wide = w_s.shape[0] - 1, w_s.shape[2]
    core = _here()[1]
    ready = _copies(_pieces((a_ref, b_ref), a_s) + _places("near", c_ref, c_s) + _places("near", s_ref, s_s), sem)
    columns = lambda ref, i: ref.at[:, pl.ds(pl.multiple_of(i * wide, wide), wide)]
    tile = lambda i: pltpu.make_async_copy(columns(wq_ref, i), w_s.at[i], w_sem.at[i])
    wo_tile = lambda i: pltpu.make_async_copy(wo_ref.at[pl.ds(pl.multiple_of(i * wide, wide), wide), :], wo_s.at[i], wo_sem.at[i])
    kv = [pltpu.make_async_copy(w, w_s.at[steps, :, pl.ds(m * HEAD, HEAD)], kv_sem.at[m]) for m, w in enumerate((wk_ref, wv_ref))]
    for copy in ready + [tile(0)]:
        copy.start()
    _meet()
    for copy in ready:
        copy.wait()
    tile(1).start()
    sib = d_s.at[pl.ds(BLOCK, BLOCK), :]
    swap = _to_sibling(dy_ref, sib, d_sem.at[0], d_sem.at[1])
    swap.start()
    d_get = pltpu.make_async_copy(dy_ref, d_s.at[pl.ds(0, BLOCK), :], d_sem.at[2])
    piece = lambda at: d_s.at[pl.ds(pl.multiple_of(at * HALF, HALF), HALF), :]
    given = [pltpu.make_async_copy(src, dst, e_sem.at[m])
             for m, (src, dst) in enumerate(((sib, e_ref), (piece(2 - core), dh_ref), (piece(3 * core), dl_ref)))]

    def turn(t):
        t = t.astype(BF16).astype(F32)
        return (t * c_s[...] + pltpu.roll(t, HEAD // 2, 1) * s_s[...]).astype(BF16)

    out = lambda s, ref, i, slot: pltpu.make_async_copy(s.at[slot], columns(ref, i), out_sem.at[slot])

    def step(i, _):
        slot = lax.rem(i, 2)
        tile(i).wait()

        @pl.when(i + AHEAD < steps)
        def _():
            tile(i + AHEAD).start()

        @pl.when(i + AHEAD == steps)
        def _():
            for copy in kv:
                copy.start()

        @pl.when(i == 2)
        def _():
            d_get.start()

        @pl.when(i + 1 == steps)
        def _():
            wo_tile(0).start()

        t = _dot(a_s[...], w_s[i], 1, 0)

        @pl.when(i >= 2)
        def _():
            out(q_s, q_ref, i - 2, slot).wait()

        for m in range(wide // HEAD):
            q_s[slot, :, m * HEAD : (m + 1) * HEAD] = turn(t[:, m * HEAD : (m + 1) * HEAD])
        out(q_s, q_ref, i, slot).start()

    lax.fori_loop(0, steps, step, None)
    for copy in kv:
        copy.wait()
    wo_tile(1).start()
    t = _dot(a_s[...], w_s[steps], 1, 0)
    k_s[...] = turn(t[:, :HEAD])
    v_s[...] = t[:, HEAD:].astype(BF16)
    last = _copies([(k_s, k_ref), (v_s, v_ref)], kv_sem)
    for copy in last:
        copy.start()
    for m in range(2):
        out(q_s, q_ref, steps - 2 + m, (steps + m) % 2).wait()
    swap.wait()
    d_get.wait()
    for copy in given:
        copy.start()

    def wo_step(i, _):
        slot = lax.rem(i, 2)
        wo_tile(i).wait()

        @pl.when(i + AHEAD < steps)
        def _():
            wo_tile(i + AHEAD).start()

        t = _dot(d_s[...], wo_s[i], 1, 1).astype(BF16)

        @pl.when(i >= 2)
        def _():
            out(o_s, o_ref, i - 2, slot).wait()

        o_s[slot] = t
        out(o_s, o_ref, i, slot).start()

    lax.fori_loop(0, steps, wo_step, None)
    for copy in last + [out(o_s, o_ref, steps - 2 + m, (steps + m) % 2) for m in range(2)] + given:
        copy.wait()


def near(a, b, dy, wq, wk, wv, wo, cos, sin, meeting):
    d, width = wq.shape
    rows = 2 * BLOCK
    wide = 256
    steps = width // wide
    vmem, dma = pltpu.VMEM, pltpu.SemaphoreType.DMA
    line = _sds((rows, HEAD))
    return _all(
        _near, [_sds((rows, width)), line, line, _sds((rows, width)), _sds((BLOCK, d)), _sds((HALF, d)), _sds((HALF, d))],
        [vmem((rows, d), BF16), vmem((rows, d), BF16), vmem((steps + 1, d, wide), BF16), vmem((steps, wide, d), BF16),
         vmem((rows, HEAD), F32), vmem((rows, HEAD), F32), vmem((2, rows, wide), BF16), vmem((rows, HEAD), BF16), vmem((rows, HEAD), BF16),
         vmem((2, rows, wide), BF16), dma((2 + 2 * rows // HALF,)), dma((steps,)), dma((steps,)), dma((2,)), dma((2,)), dma((3,)), dma((3,))],
        2 * rows * d * (2 * width + 2 * HEAD), 4 * d * (width + rows), a, b, dy, wq, wk, wv, wo, cos, sin, meeting=meeting)


def _attend(pos_ref, q_ref, do_ref, kl_ref, kh_ref, kr_ref, vl_ref, vh_ref, vr_ref, c_ref, s_ref, *rest, first, hp, added):
    dk_in, dv_in = rest[:2] if added else (None, None)
    seen_ref, dq_ref, dk_ref, dv_ref, k_s, v_s, kt_s, vt_s, s_s, dp_s, o_s, dq_s, dk_s, dv_s, c_s, t_s, sem = rest[-17:]
    iq, ih = pl.program_id(0), pl.program_id(1)
    wide = hp * BLOCK
    e = HEAD**-0.5 * LOG2E

    n = c_s.shape[0] // HALF
    later = [(ref.at[pl.ds(pl.multiple_of(pos_ref[first + m], HALF), HALF), :], s.at[pl.ds(m * HALF, HALF), :])
             for ref, s in ((c_ref, c_s), (s_ref, t_s)) for m in range(n)]
    later = _copies(later + ([(dk_in, dk_s), (dv_in, dv_s)] if added else []), sem)
    starts = (iq == 0) & (ih == 0)

    @pl.when(starts)
    def _():
        for copy in later:
            copy.start()
        at = 0
        for kc, vc in ((kl_ref, vl_ref), (kh_ref, vh_ref), (kr_ref, vr_ref)):
            for m in range(kc.shape[0] // HALF):
                here = pl.ds(pl.multiple_of(pos_ref[at], HALF), HALF)
                k_s[here, :] = kc[m * HALF : (m + 1) * HALF, :]
                v_s[here, :] = vc[m * HALF : (m + 1) * HALF, :]
                at += 1
        kt_s[...] = k_s[...].T
        vt_s[...] = v_s[...].T
        if not added:
            dk_s[...] = jnp.zeros_like(dk_s)
            dv_s[...] = jnp.zeros_like(dv_s)

    place = pos_ref[first + 2 * iq]
    own = lax.div(place, BLOCK)
    turned = lax.rem(place, BLOCK)
    q2 = jnp.concatenate([q_ref[:, m * HEAD : (m + 1) * HEAD] for m in range(hp)], axis=0)
    do2 = jnp.concatenate([do_ref[:, m * HEAD : (m + 1) * HEAD] for m in range(hp)], axis=0)

    def rows(j):
        return pl.ds(pl.multiple_of(j * BLOCK, BLOCK), BLOCK)

    here = rows(own)
    s = _dot(k_s[here, :], q2, 1, 1)
    query = lax.rem(lax.broadcasted_iota(jnp.int32, s.shape, 1) + turned, BLOCK)
    s = jnp.where(lax.broadcasted_iota(jnp.int32, s.shape, 0) <= query, s, HIDDEN)
    s_s[here, :] = s

    def scores(j, top):
        s = _dot(k_s[rows(j), :], q2, 1, 1)
        s_s[rows(j), :] = s
        return jnp.maximum(top, s.max(axis=0, keepdims=True))

    top = lax.fori_loop(0, own, scores, s.max(axis=0, keepdims=True))
    o_s[...] = jnp.zeros_like(o_s)
    dq_s[...] = jnp.zeros_like(dq_s)

    def weigh(j, sums):
        total, delta = sums
        dp = _dot(v_s[rows(j), :], do2, 1, 1)
        dp_s[rows(j), :] = dp
        p = jnp.exp2((s_s[rows(j), :] - top) * e)
        s_s[rows(j), :] = p
        o_s[...] += _dot(vt_s[:, rows(j)], p.astype(BF16), 1, 0)
        return total + p.sum(axis=0, keepdims=True), delta + (p * dp).sum(axis=0, keepdims=True)

    zero = jnp.zeros((1, wide), F32)
    total, delta = lax.fori_loop(0, own + 1, weigh, (zero, zero))
    inv = 1 / total
    delta = delta * inv

    @pl.when(starts)
    def _():
        for copy in later:
            copy.wait()

    def grads(j, _):
        p = s_s[rows(j), :] * inv
        ds = (p * (dp_s[rows(j), :] - delta)).astype(BF16)
        dv_s[rows(j), :] += _dot(p.astype(BF16), do2, 1, 0)
        dk_s[rows(j), :] += _dot(ds, q2, 1, 0)
        dq_s[...] += _dot(kt_s[:, rows(j)], ds, 1, 0)

    lax.fori_loop(0, own + 1, grads, None)
    these = pl.ds(pl.multiple_of(iq * BLOCK, BLOCK), BLOCK)
    cos, sin = c_s[these, :], t_s[these, :]
    o = (o_s[...] * inv).astype(BF16)
    for m in range(hp):
        seen_ref[m * HEAD : (m + 1) * HEAD, :] = o[:, m * BLOCK : (m + 1) * BLOCK]
        g = (dq_s[:, m * BLOCK : (m + 1) * BLOCK] * HEAD**-0.5).T.astype(BF16).astype(F32)
        dq_ref[:, m * HEAD : (m + 1) * HEAD] = (g * cos - pltpu.roll(g, HEAD // 2, 1) * sin).astype(BF16)

    @pl.when((iq == pl.num_programs(0) - 1) & (ih == pl.num_programs(1) - 1))
    def _():
        dk_ref[...] = dk_s[...]
        dv_ref[...] = dv_s[...]


def attend(pos, first, q, do, ks, vs, cos, sin, sums=None):
    rows, width = q.shape
    hp = 6
    sk = sum(k.shape[0] for k in ks)
    tile = pl.BlockSpec((BLOCK, hp * HEAD), lambda i, h, _: (i, h))
    whole = lambda a: pl.BlockSpec(a.shape, lambda i, h, _: (0, 0))
    keys = _sds((sk, HEAD), F32)
    given, other = (*ks, *vs), (cos, sin, *(sums or ()))
    wide = hp * BLOCK
    vmem = lambda *shape, t=F32: pltpu.VMEM(shape, t)
    return _call(
        functools.partial(_attend, first=first, hp=hp, added=sums is not None), (rows // BLOCK, width // (hp * HEAD)),
        [tile, tile, *map(whole, given), *[ANY] * len(other)],
        [pl.BlockSpec((hp * HEAD, BLOCK), lambda i, h, _: (h, i)), tile, whole(keys), whole(keys)],
        [_sds((width, rows)), _sds((rows, width)), keys, keys],
        [vmem(sk, HEAD, t=BF16), vmem(sk, HEAD, t=BF16), vmem(HEAD, sk, t=BF16), vmem(HEAD, sk, t=BF16), vmem(sk, wide), vmem(sk, wide),
         vmem(HEAD, wide), vmem(HEAD, wide), vmem(sk, HEAD), vmem(sk, HEAD), vmem(rows, HEAD), vmem(rows, HEAD),
         pltpu.SemaphoreType.DMA((2 * rows // HALF + 2,))],
        2 * 6 * 2 * rows * sk * width * 0.6, 8 * rows * width, (pos, q, do, *given, *other))


def _back(*refs, chunks):
    n = len(chunks)
    dqs, (dk_ref, dv_ref, c_ref, s_ref, wq_ref, wk_ref, wv_ref), refs = refs[:n], refs[n : n + 7], refs[n + 7 :]
    sums, g_ref, refs = refs[:n], refs[n], refs[n + 1 :]
    sum_ss, (g_s, dk_s, dv_s, c_s, s_s, w_s, keep_s, send_s, came_s, sem, w_sem, out_sem, g_sem, send_sem, recv_sem) = refs[:n], refs[n:]
    width = dqs[0].shape[1]
    steps, wide = keep_s.shape[0], keep_s.shape[2]
    slots = w_s.shape[0]
    pairs, at = [], 0
    for dq, chunk in zip(dqs, chunks):
        rows = pl.ds(at, dq.shape[0])
        pairs.append((dq, g_s.at[rows, pl.ds(0, width)]))
        for ref, s in ((dk_ref, dk_s), (dv_ref, dv_s), (c_ref, c_s), (s_ref, s_s)):
            pairs += _places(chunk, ref, s.at[rows, :])
        at += dq.shape[0]
    ready = _copies(pairs, sem)
    lines = lambda ref, i: ref.at[pl.ds(pl.multiple_of(i * wide, wide), wide), :]
    parts = ((wq_ref, 0, width), (wk_ref, width, HEAD), (wv_ref, width + HEAD, HEAD))

    def tile(i):
        slot = lax.rem(i, slots)
        return [pltpu.make_async_copy(lines(w, i), w_s.at[slot, :, pl.ds(at, size)], w_sem.at[slot, m]) for m, (w, at, size) in enumerate(parts)]

    for copy in ready + tile(0) + tile(1):
        copy.start()
    _meet()
    for copy in ready:
        copy.wait()
    for copy in tile(2):
        copy.start()
    g = (dk_s[...] * HEAD**-0.5).astype(BF16).astype(F32)
    g_s[:, width : width + HEAD] = (g * c_s[...] - pltpu.roll(g, HEAD // 2, 1) * s_s[...]).astype(BF16)
    g_s[:, width + HEAD :] = dv_s[...].astype(BF16)
    g_out = pltpu.make_async_copy(g_s, g_ref, g_sem.at[0])
    g_out.start()
    swap = lambda i: _to_sibling(send_s.at[i], came_s.at[i], send_sem.at[i], recv_sem.at[i])
    columns = lambda i: pl.ds(pl.multiple_of(i * wide, wide), wide)
    out = lambda i: [pltpu.make_async_copy(s.at[i], ref.at[:, columns(i)], out_sem.at[i, m]) for m, (s, ref) in enumerate(zip(sum_ss, sums))]

    def add(i):
        swap(i).wait_recv()
        at = 0
        for s in sum_ss:
            rows = slice(at, at + s.shape[1])
            s[i] = (keep_s[i, rows, :] + came_s[i, rows, :].astype(F32)).astype(s.dtype)
            at += s.shape[1]
        for copy in out(i):
            copy.start()

    def step(i, _):
        for copy in tile(i):
            copy.wait()

        @pl.when(i + 3 < steps)
        def _():
            for copy in tile(i + 3):
                copy.start()

        t = _dot(g_s[...], w_s[lax.rem(i, slots)], 1, 1)
        at = 0
        for s in sum_ss:
            half = s.shape[1]
            keep_s[i, at : at + half, :] = t[2 * at : 2 * at + half]
            send_s[i, at : at + half, :] = t[2 * at + half : 2 * at + 2 * half].astype(BF16)
            at += half
        swap(i).start()

        @pl.when(i >= LAG)
        def _():
            add(i - LAG)

    lax.fori_loop(0, steps, step, None)
    lax.fori_loop(steps - LAG, steps, lambda i, _: add(i), None)

    def done(i, _):
        swap(i).wait_send()
        for copy in out(i):
            copy.wait()

    lax.fori_loop(0, steps, done, None)
    g_out.wait()


def back(chunks, dqs, dk, dv, wq, wk, wv, cos, sin, meeting):
    d, width = wq.shape
    each = [dq.shape[0] for dq in dqs]
    rows = sum(each)
    wide = 512
    steps = d // wide
    full = width + 2 * HEAD
    vmem, dma = pltpu.VMEM, pltpu.SemaphoreType.DMA
    line = vmem((rows, HEAD), F32)
    tiles = lambda t, n=rows: vmem((steps, n // 2, wide), t)
    return _all(
        functools.partial(_back, chunks=[name for name, _ in chunks]),
        [*[_sds((n // 2, d), t) for n, (_, t) in zip(each, chunks)], _sds((rows, full))],
        [*[tiles(t, n) for n, (_, t) in zip(each, chunks)], vmem((rows, full), BF16), line, line, line, line, vmem((5, wide, full), BF16),
         tiles(F32), tiles(BF16), tiles(BF16), dma((len(each) + 4 * rows // HALF,)), dma((5, 3)), dma((steps, len(each))), dma((1,)),
         dma((steps,)), dma((steps,))],
        2 * rows * d * full, 2 * (d * full + rows * (2 * d + width)), *dqs, dk, dv, cos, sin, wq, wk, wv, meeting=meeting)


def _tiles(pieces, a_s, sem, wide, base=0):
    def tile(i):
        slot, at, copies = lax.rem(i, 4), 0, []
        for m, p in enumerate(pieces):
            columns = pl.ds(pl.multiple_of((base + i) * wide, wide), wide)
            copies.append(pltpu.make_async_copy(p.at[:, columns], a_s.at[slot, pl.ds(at, p.shape[0]), :], sem.at[slot, m]))
            at += p.shape[0]
        return copies

    return tile


def _go(copies):
    for copy in copies:
        copy.start()


def _wait(copies):
    for copy in copies:
        copy.wait()


def _stream(steps, tile, ready, out, work):
    _go(ready + tile(0))
    _go(tile(1))
    _wait(ready)

    def step(i, _):
        slot = lax.rem(i, 2)
        _wait(tile(i))

        @pl.when(i + 2 < steps)
        def _():
            _go(tile(i + 2))

        @pl.when(i >= 2)
        def _():
            _wait(out(i - 2, slot))

        work(i, slot)
        _go(out(i, slot))

    lax.fori_loop(0, steps, step, None)
    for m in range(2):
        _wait(out(steps - 2 + m, (steps + m) % 2))


def _weights(*refs, n, ng):
    pieces, gs, (wq_ref, wk_ref, wv_ref, a_s, g_s, o_s, a_sem, g_sem, o_sem) = refs[:n], refs[n : n + ng], refs[n + ng :]
    width, wide = wq_ref.shape[1], a_s.shape[2]
    parts = ((wq_ref, 0, width), (wk_ref, width, HEAD), (wv_ref, width + HEAD, HEAD))

    def out(i, slot):
        rows = pl.ds(pl.multiple_of(i * wide, wide), wide)
        return _copies([(o_s.at[slot, :, pl.ds(at, size)], ref.at[rows, :]) for ref, at, size in parts], o_sem.at[slot])

    def work(i, slot):
        o_s[slot] = _dot(a_s[lax.rem(i, 4)], g_s[...], 0, 0).astype(BF16)

    _stream(wq_ref.shape[0] // wide, _tiles(pieces, a_s, a_sem, wide), _copies(_pieces(gs, g_s), g_sem), out, work)


def weights(pieces, gs):
    d = pieces[0].shape[1]
    full = gs[0].shape[1]
    width = full - 2 * HEAD
    rows = sum(g.shape[0] for g in gs)
    wide = 512
    vmem, dma = pltpu.VMEM, pltpu.SemaphoreType.DMA
    return _all(
        functools.partial(_weights, n=len(pieces), ng=len(gs)), [_sds((d, width)), _sds((d, HEAD)), _sds((d, HEAD))],
        [vmem((4, rows, wide), BF16), vmem((rows, full), BF16), vmem((2, wide, full), BF16), dma((4, len(pieces))), dma((len(gs),)), dma((2, 3))],
        2 * rows * d * full, 2 * (rows * (d + full) + d * full), *pieces, *gs)


def _out_weights(*refs, n, ns, late):
    pieces, seen, refs = refs[:n], refs[n : n + ns], refs[n + ns :]
    if late:
        dx_ref, _, o_ref, x_ref, a_s, s_s, o_s, a_sem, s_sem, o_sem, x_s, x_sem = refs
        get, put = pltpu.make_async_copy(dx_ref, x_s, x_sem.at[0]), pltpu.make_async_copy(x_s, x_ref, x_sem.at[1])
    else:
        o_ref, a_s, s_s, o_s, a_sem, s_sem, o_sem = refs
    wide = a_s.shape[2]
    steps = o_ref.shape[1] // wide // 2
    base = steps if late else 0
    pairs, at = [], 0
    for s in seen:
        pairs.append((s, s_s.at[:, pl.ds(at, s.shape[1])]))
        at += s.shape[1]
    columns = lambda i: pl.ds(pl.multiple_of((base + i) * wide, wide), wide)
    out = lambda i, slot: [pltpu.make_async_copy(o_s.at[slot], o_ref.at[:, columns(i)], o_sem.at[slot])]

    def work(i, slot):
        if late:

            @pl.when(i == 1)
            def _():
                get.start()

            @pl.when(i == steps - 2)
            def _():
                get.wait()
                put.start()

        o_s[slot] = _dot(s_s[...], a_s[lax.rem(i, 4)], 1, 0).astype(BF16)

    _stream(steps, _tiles(pieces, a_s, a_sem, wide, base), _copies(pairs, s_sem), out, work)
    if late:
        put.wait()


def out_weights(pieces, seen, early=None, dx=None):
    d = pieces[0].shape[1]
    width = seen[0].shape[0]
    rows = sum(s.shape[1] for s in seen)
    wide = 512
    vmem, dma = pltpu.VMEM, pltpu.SemaphoreType.DMA
    late = early is not None
    out = _sds((width, d))
    more = ([vmem(dx.shape, BF16), dma((2,))], (dx, early), {"aliases": {len(pieces) + len(seen) + 1: 0}}) if late else ([], (), {})
    return _all(
        functools.partial(_out_weights, n=len(pieces), ns=len(seen), late=late), [out, _sds(dx.shape)] if late else out,
        [vmem((4, rows, wide), BF16), vmem((width, rows), BF16), vmem((2, width, wide), BF16), dma((4, len(pieces))), dma((len(seen),)),
         dma((2,)), *more[0]],
        rows * d * width, rows * (d + width) + d * width, *pieces, *seen, *more[1], **more[2])


def _finish(own_ref, rh_ref, rl_ref, x_ref, dy_ref, gain_ref, dx_ref, dg_ref,
            own_s, far_s, x_s, dy_s, gain_s, dx_s, dg_s, sem, out_sem, far_sem):
    n, rows = x_s.shape[:2]
    part = lambda ref, i: ref.at[pl.ds(pl.multiple_of(i * rows, rows), rows), :]
    core = _here()[1]
    half = n // 2
    there = far_s.at[pl.ds(pl.multiple_of(core * HALF, HALF), HALF), :]
    mine = lambda ref: pltpu.make_async_copy(ref, there, far_sem.at[0])
    hand = lambda ref: _to_sibling(ref, there, far_sem.at[1], far_sem.at[2])
    rest = ((own_ref, own_s), (x_ref, x_s), (dy_ref, dy_s))
    row = lambda i: lax.rem(i + core * half, n)

    def get(i):
        return [pltpu.make_async_copy(part(ref, row(i)), s.at[i], sem.at[i, k]) for k, (ref, s) in enumerate(rest)]

    get_gain = pltpu.make_async_copy(gain_ref, gain_s, out_sem.at[n])
    get_gain.start()
    _meet()
    for which, here, give in ((0, rl_ref, rh_ref), (1, rh_ref, rl_ref)):

        @pl.when(core == which)
        def _():
            mine(here).start()
            hand(give).start()

    for i in range(AHEAD):
        for copy in get(i):
            copy.start()
    get_gain.wait()
    mine(rh_ref).wait()
    dg_s[...] = jnp.zeros_like(dg_s)

    def step(i, _):
        @pl.when(i + AHEAD < n)
        def _():
            for copy in get(i + AHEAD):
                copy.start()

        @pl.when(i == half)
        def _():
            hand(rh_ref).wait_recv()

        for copy in get(i):
            copy.wait()
        far = far_s[pl.ds(pl.multiple_of(row(i) * rows, rows), rows), :]
        da = own_s[i] + far.astype(F32)
        x = x_s[i].astype(F32)
        scale = lax.rsqrt(jnp.mean(x * x, -1, keepdims=True) + 1e-6)
        h = x * scale
        dg_s[...] += jnp.sum(da * h, axis=0, keepdims=True)
        dh = da * gain_s[...].astype(F32)
        dx = scale * (dh - h * jnp.mean(dh * h, -1, keepdims=True))
        dx_s[i] = (dy_s[i].astype(F32) + dx).astype(BF16)
        pltpu.make_async_copy(dx_s.at[i], part(dx_ref, row(i)), out_sem.at[i]).start()

    lax.fori_loop(0, n, step, None)
    last = pltpu.make_async_copy(dg_s, dg_ref, out_sem.at[n])
    last.start()
    for copy in _copies([(dx_s.at[i], part(dx_ref, i)) for i in range(n)], out_sem) + [last]:
        copy.wait()
    hand(rh_ref).wait_send()


def finish(own, rh, rl, x, dy, gain, meeting):
    rows, d = x.shape
    n = 8
    block = (n, rows // n, d)
    vmem, dma = pltpu.VMEM, pltpu.SemaphoreType.DMA
    return _all(
        _finish, [_sds((rows, d)), _sds((1, d), F32)],
        [vmem(block, F32), vmem((rows, d), BF16), vmem(block, BF16), vmem(block, BF16), vmem((1, d), BF16), vmem(block, BF16),
         vmem((1, d), F32), dma((n, 3)), dma((n + 1,)), dma((3,))],
        3 * 10**9, 12 * rows * d, own, rh, rl, x, dy, gain, meeting=meeting)


def tables(rows):
    half = HEAD // 2
    angle = jnp.arange(rows).astype(F32)[:, None] * THETA ** (-jnp.arange(half, dtype=F32) / half)
    cos, sin = jnp.cos(angle), jnp.sin(angle)
    return jnp.concatenate([cos, cos], -1), jnp.concatenate([-sin, sin], -1)


SIBLING = [(0, 1), (1, 0), (2, 3), (3, 2)]
PARTNER = [(0, 2), (2, 0), (1, 3), (3, 1)]
ACROSS = [(0, 3), (3, 0), (1, 2), (2, 1)]


def solution(mesh):
    def move(t, pairs):
        return lax.ppermute(t, "tp", pairs)

    def work(x, dy, gain, wq, wk, wv, wo):
        me = lax.axis_index("tp")
        core = lax.rem(me, 2)
        gain = gain[None]
        start = lambda block, half: block * BLOCK + half * HALF
        sib, far = me + 1 - 2 * core, 2 * (1 - lax.div(me, 2))
        pos = jnp.stack([start(me, 0), start(me, 1), start(sib, 0), start(sib, 1), start(far + 1, core), start(far + 1, 1 - core),
                         start(far, core), start(far, 1 - core)]).astype(jnp.int32)
        cos, sin = tables(4 * BLOCK)

        def after(t, *others):
            return lax.optimization_barrier((t, *others))[0]

        a, b, a_high, a_low = head(x, gain, 7)
        ah = move(a_high, PARTNER)
        al = move(a_low, PARTNER)
        w = (wq, wk, wv)
        turns = (cos, sin)
        q_n, k_n, v_n, do_n, e, d_high, d_low = near(a, b, dy, *w, wo, *turns, meeting=9)
        dh = move(d_high, PARTNER)
        dl = move(d_low, PARTNER)
        ah = after(ah, do_n)
        q_h, k_h, v_h, ah2 = project("high", (ah,), *w, *turns, meeting=0)
        al = after(al, q_h)
        q_l, k_l, v_l, al2 = project("low", (al,), *w, *turns, meeting=1)
        keys = ((k_n, k_h, k_l), (v_n, v_h, v_l), *turns)
        seen_n, dq_n, dk, dv = attend(pos, 0, q_n, do_n, *keys)
        dh = after(dh, dq_n)
        do_h, dh2 = into((dh,), wo, meeting=2)
        seen_h, dq_h, dk, dv = attend(pos, 4, q_h, do_h, *keys, sums=(dk, dv))
        sum_h, g_h = back((("high", BF16),), (dq_h,), dk, dv, *w, *turns, meeting=3)
        dl = after(dl, sum_h)
        do_l, dl2 = into((dl,), wo, meeting=4)
        seen_l, dq_l, dk, dv = attend(pos, 6, q_l, do_l, *keys, sums=(dk, dv))
        r_h = move(after(sum_h, dq_l), PARTNER)
        sum_l, own, g = back((("low", BF16), ("near", F32)), (dq_l, dq_n), dk, dv, *w, *turns, meeting=5)
        r_l = move(sum_l, PARTNER)
        by_wq, by_wk, by_wv = weights((ah, ah2, al, al2, a, b), (g_h, after(g, sum_l)))
        rows, seen = (dy, e, dh, dh2, dl, dl2), (seen_n, seen_h, seen_l)
        early = out_weights(rows, (seen_n, seen_h, after(seen_l, by_wq)))
        dx, part = finish(own, after(r_h, early), after(r_l, early), x, dy, gain, 8)
        by_wo, by_x = out_weights(rows, seen, early, dx)
        by_gain = (part + move(part, SIBLING)) + (move(part, PARTNER) + move(part, ACROSS))
        return by_x, by_gain, by_wq, by_wk, by_wv, by_wo

    tokens, columns = P(("dp", "tp"), None), P(None, "tp")
    return jax.shard_map(
        work,
        mesh=mesh,
        in_specs=(tokens, tokens, P(None), columns, columns, columns, P("tp", None)),
        out_specs=(tokens, P("dp", None), P("dp", "tp"), P("dp", "tp"), P("dp", "tp"), P(("dp", "tp"), None)),
        check_vma=False,
    )
```
